256 devices in a mesh: ep: 32 (over z_lo, y, x), dp: 8 (over z_hi, core).
Axes of the slice: x: 4, y: 4, z: 8 (z_hi: 4, z_lo: 2; z = z_hi * 2 + z_lo), core: 2. Of those that a mesh axis runs over, the one named last changes fastest.
Arguments:
- tokens: bfloat16 [16384, 2048], P(('dp', 'ep')), parts along dimension 0, may hold values from -6 to 6
- expert_ids: int32 [16384, 8], P(('dp', 'ep')), parts along dimension 0, may hold values from 0 to 31, all different within a row; in each aligned block of 64 rows (0 to 63, 64 to 127, ...) at most 32 rows name the same one
- gate_probs: float32 [16384, 8], P(('dp', 'ep')), parts along dimension 0, may hold values from 0.05 to 1
- w_gate: bfloat16 [32, 2048, 768], P('ep'), may hold values from -0.125 to 0.125
- w_up: bfloat16 [32, 2048, 768], P('ep'), may hold values from -0.125 to 0.125
- w_down: bfloat16 [32, 768, 2048], P('ep'), may hold values from -0.21875 to 0.21875
Outputs:
- combined: bfloat16 [16384, 2048], P(('dp', 'ep')), parts along dimension 0
The draws below stay inside these ranges and needn't reach their ends.
There are 8 independent parts, one for each index of `dp`. The reference program is written for one: setup_inputs(seed, part) draws one part's arguments, and reference() takes and returns one part's arrays. A program takes and returns all parts, laid end to end along the dimension named above; an argument that names none is the same for every part. Nothing has to cross between parts.
Inputs may be any that keep to these rules, and one draw needn't show every extreme that they name: `expert_ids`: each row names 8 different experts. Among the rows of one index of ep (aligned blocks of 64 rows) no expert is named by more than 32 rows, and in every draw some expert is named by exactly 32 rows of some block. Expert popularity is skewed.
All inputs are finite; a program needn't handle non-finite values.
Results may differ from the reference program's by a relative error of at most 0.0085.
Values may be sent and summed in bfloat16 or wider, within the bound.
A program may use at most 64 MiB of HBM per device.

```python
import math
import jax
import jax.numpy as jnp
import numpy as np
from jax import lax

D = 2048
FF = 768
TOP = 8
TOK_DEV = 64
EXPERTS = 32
TOKENS = 2048
MOST = 32
N_EP = 32


def levels(key, extent, cuts, least, top_value):
    factor_of, own = 1.0, jax.random.fold_in(key, 6)
    for dim, blocks in cuts:
        steps = jnp.exp(jax.random.uniform(jax.random.fold_in(own, dim), (blocks,), jnp.float32, least / len(cuts), top_value / len(cuts)))
        factor_of = factor_of * jnp.repeat(steps, extent[dim] // blocks).reshape([-1 if axis == dim else 1 for axis in range(len(extent))])
    return factor_of


def deal_out(own_key, own, number, rows, count, top, reach, lean):
    sequence = jax.random.permutation(own_key, count)
    crowded, usual = shares(count, rows * top, reach, lean, True), shares(count, rows * top, reach, lean, False)
    places = jnp.arange(count)

    def named(lengths, offset_by):
        used = int((lengths > 0).sum())
        fixed = max(1, used // 4)
        passed = fixed + (places - fixed + offset_by * (used - fixed)) % max(1, count - fixed)
        return jnp.zeros((count,), jnp.int32).at[sequence[jnp.where(places < fixed, places, passed)]].set(jnp.asarray(lengths, jnp.int32))

    lengths = jnp.where(number % 4 == 0, named(crowded, number // 4), named(usual, number - number // 4 - 1))
    mixed = jax.random.permutation(jax.random.fold_in(own, 3), count)
    source_of, receiver = mixed[0:count // 2 * 2:2], mixed[1:count // 2 * 2:2]
    margin = jnp.minimum(lengths[source_of] - 1, reach - lengths[receiver]) // 2
    margin = jnp.where((source_of == sequence[0]) | (receiver == sequence[0]) | (lengths[receiver] == 0), 0, jnp.maximum(margin, 0))
    passed = jax.random.randint(jax.random.fold_in(own, 4), (count // 2,), 0, 1 << 20) % (margin + 1)
    lengths = lengths.at[source_of].add(-passed).at[receiver].add(passed)
    labels = jnp.searchsorted(jnp.cumsum(lengths), jnp.arange(rows * top), side="right").astype(jnp.int32)
    grid = labels.reshape(top, rows).T
    grid = grid[jax.random.permutation(jax.random.fold_in(own, 1), rows)]
    offset_by = jax.random.randint(jax.random.fold_in(own, 2), (rows, 1), 0, top)
    return jnp.take_along_axis(grid, (jnp.arange(top)[None, :] + offset_by) % top, axis=1)


def shares(amount, total, limit, skew, full):
    loads = [(1 << 20) // math.isqrt(standing ** skew) + 1 for standing in range(1, amount + 1)]
    largest = limit if full else min(limit, max(-(-total // amount), total * loads[0] // sum(loads)))
    least = 1 if total - largest >= amount - 1 else 0
    given, rest = [largest] + [least] * (amount - 1), total - largest - least * (amount - 1)
    while rest > 0:
        movable = [i for i in range(1, amount) if given[i] < largest] or [i for i in range(1, amount) if given[i] < limit]
        mass, left = sum([loads[i] for i in movable]), rest
        for i in movable:
            extra = min(limit - given[i], max(1, left * loads[i] // mass), rest)
            given[i] = given[i] + extra
            rest = rest - extra
    return np.array(given)


def gaussian(own_key, shape, deviation, limit, cuts=(), kind=jnp.bfloat16):
    level = levels(own_key, shape, cuts, -0.22, 0.18) if cuts else 1.0
    values = jax.random.normal(own_key, shape, jnp.float32) * deviation * level
    return jnp.minimum(jnp.maximum(values, -limit), limit).astype(kind)


def setup_inputs(seed: int = 0, part: int = 0) -> dict:
    arg_keys = jax.random.split(jax.random.key(seed), 7)
    part_keys = jax.random.split(jax.random.fold_in(arg_keys[6], part), 7)
    tokens = gaussian(part_keys[0], (TOKENS, D), 1.0, 6.0, ((0, 32),))
    expert_ids_keys = jax.random.split(jax.random.fold_in(part_keys[1], 1), TOKENS // TOK_DEV)
    expert_ids_turns = jax.random.permutation(jax.random.fold_in(part_keys[1], 3), TOKENS // TOK_DEV)
    expert_ids = jax.vmap(lambda own, number: deal_out(jax.random.fold_in(part_keys[1], 2), own, number, TOK_DEV, EXPERTS, TOP, MOST, 2))(expert_ids_keys, expert_ids_turns).reshape((TOKENS, TOP))
    gate_probs = jnp.clip(0.05 + 0.95 * jax.random.uniform(part_keys[2], (TOKENS, TOP), jnp.float32) ** levels(part_keys[2], (TOKENS, TOP), ((0, 32),), -0.2, 0.2), 0.05, 1.0)
    w_gate = gaussian(arg_keys[3], (EXPERTS, D, FF), D ** -0.5, 0.125, ((0, 32),))
    w_up = gaussian(arg_keys[4], (EXPERTS, D, FF), D ** -0.5, 0.125, ((0, 32),))
    w_down = gaussian(arg_keys[5], (EXPERTS, FF, D), FF ** -0.5, 0.21875, ((0, 32),))
    return dict(tokens=tokens, expert_ids=expert_ids, gate_probs=gate_probs, w_gate=w_gate, w_up=w_up, w_down=w_down)


def expert_ffn(row_block, gate_matrix, up_matrix, down_matrix):
    gate_act = jnp.dot(row_block, gate_matrix, preferred_element_type=jnp.float32)
    up_act = jnp.dot(row_block, up_matrix, preferred_element_type=jnp.float32)
    hidden = (jax.nn.silu(gate_act) * up_act).astype(jnp.bfloat16)
    return jnp.dot(hidden, down_matrix, preferred_element_type=jnp.float32).astype(jnp.bfloat16)


def reference(tokens, expert_ids, gate_probs, w_gate, w_up, w_down):
    experts = w_gate.shape[0]
    capacity = N_EP * MOST
    flat_ids = expert_ids.reshape(-1).astype(jnp.int32)
    owners = (jnp.arange(flat_ids.shape[0], dtype=jnp.int32) // TOP).astype(jnp.int32)
    onehot = (flat_ids[:, None] == jnp.arange(experts, dtype=jnp.int32)[None, :]).astype(jnp.int32)
    within_rank = jnp.sum((jnp.cumsum(onehot, axis=0) - onehot) * onehot, axis=1).astype(jnp.int32)
    slot_index = (flat_ids * capacity + within_rank).astype(jnp.int32)
    slot_token = jnp.zeros((experts * capacity,), jnp.int32).at[slot_index].set(owners)
    filled = jnp.zeros((experts * capacity,), jnp.bool_).at[slot_index].set(True)

    def per_expert(expert_index):
        row_start = (expert_index * capacity).astype(jnp.int32)
        chosen = lax.dynamic_slice_in_dim(slot_token, row_start, capacity, 0)
        present = lax.dynamic_slice_in_dim(filled, row_start, capacity, 0)
        row_block = jnp.where(present[:, None], tokens[chosen], jnp.zeros((), jnp.bfloat16))
        return expert_ffn(row_block, w_gate[expert_index], w_up[expert_index], w_down[expert_index])

    outputs = lax.map(per_expert, jnp.arange(experts, dtype=jnp.int32))
    picked = outputs.reshape(-1, tokens.shape[1])[slot_index].astype(jnp.float32)
    picked = picked.reshape(tokens.shape[0], TOP, tokens.shape[1])
    weights = gate_probs / jnp.sum(gate_probs, axis=1, keepdims=True)
    combined = jnp.sum(picked * weights[:, :, None], axis=1)
    return combined.astype(jnp.bfloat16)
```

```python
import functools

import jax
import jax.numpy as jnp
from jax import lax
from jax.experimental import pallas as pl
from jax.experimental.pallas import tpu as pltpu
from jax.sharding import PartitionSpec as P

MESH = pl.DeviceIdType.MESH
F32, BF16 = jnp.float32, jnp.bfloat16
OPPOSITE = {"xp": "xm", "xm": "xp", "yp": "ym", "ym": "yp", "zp": "zm", "zm": "zp"}

ORDER = [
    (0, 0), (1, 0), (3, 0), (0, 1), (0, 3), (1, 1), (1, 3), (3, 1),
    (3, 3), (0, 2), (2, 0), (1, 2), (3, 2), (2, 1), (2, 3), (2, 2),
]
PLACE = {slot: place for place, slot in enumerate(ORDER)}
CHUNKS = 4
MAX_COPIES = 176


def kernel(
    sizes, tok_hbm, ids_ref, probs_ref, wg_hbm, wu_hbm, wd_hbm, out_ref,
    gath, meta, comb, xown, zsend, zrecv, hown, hz, wg, wu, wd, zout, both, part,
    y1p, y1m, x1p, x1m, y2p, y2m, x2p, x2m, x4p, x4m, y4p, y4m, x5p, x5m, y5p, y5m,
    send_sem, recv_sem, local_sem,
):
    n_hi, tok, width, hid, most = sizes
    half, quarter = width // 2, width // 4
    ep, dp = lax.axis_index("ep"), lax.axis_index("dp")
    x, y, z_lo = lax.rem(ep, 4), lax.rem(ep // 4, 4), ep // 16
    z_hi, core = dp // 2, lax.rem(dp, 2)

    def at(xx, yy, zz):
        return zz * 16 + yy * 4 + xx

    z_up = lax.rem(z_hi + z_lo, n_hi) * 2 + core
    z_down = lax.rem(z_hi + z_lo + n_hi - 1, n_hi) * 2 + core
    target = {
        "xp": {"ep": at(lax.rem(x + 1, 4), y, z_lo), "dp": dp},
        "xm": {"ep": at(lax.rem(x + 3, 4), y, z_lo), "dp": dp},
        "yp": {"ep": at(x, lax.rem(y + 1, 4), z_lo), "dp": dp},
        "ym": {"ep": at(x, lax.rem(y + 3, 4), z_lo), "dp": dp},
        "zp": {"ep": at(x, y, 1 - z_lo), "dp": z_up},
        "zm": {"ep": at(x, y, 1 - z_lo), "dp": z_down},
    }
    other = at(x, y, 1 - z_lo)

    copies = {}

    def send(name, way, src, dst):
        index = len(copies)
        copy = pltpu.make_async_remote_copy(
            src_ref=src, dst_ref=dst, send_sem=send_sem.at[index], recv_sem=recv_sem.at[index],
            device_id=target[way], device_id_type=MESH,
        )
        copy.start()
        copies[name] = copy

    def wait(*names):
        for name in names:
            copies[name].wait_recv()

    load_tok = pltpu.make_async_copy(tok_hbm, gath.at[0, 0], local_sem.at[0])
    load_tok.start()
    loads = [
        pltpu.make_async_copy(src.at[0], dst, local_sem.at[1 + i])
        for i, (src, dst) in enumerate(((wg_hbm, wg), (wu_hbm, wu), (wd_hbm, wd)))
    ]
    for load in loads:
        load.start()

    barrier = pltpu.get_barrier_semaphore()
    for way in target:
        pl.semaphore_signal(barrier, inc=1, device_id=target[way], device_id_type=MESH)

    ids = ids_ref[...].astype(F32)
    probs = probs_ref[...]
    weights = probs / jnp.sum(probs, axis=0, keepdims=True)
    experts = lax.broadcasted_iota(jnp.int32, (32, tok), 0).astype(F32)
    named = jnp.zeros((32, tok), F32)
    for k in range(8):
        named = named + jnp.where(ids[k:k + 1, :] == experts, 1.0, 0.0)
    before = lax.broadcasted_iota(jnp.int32, (tok, tok), 0) < lax.broadcasted_iota(jnp.int32, (tok, tok), 1)
    ranks = jnp.dot(named.astype(BF16), before.astype(F32).astype(BF16), preferred_element_type=F32)
    for k in range(8):
        rank = jnp.sum(jnp.where(ids[k:k + 1, :] == experts, ranks, 0.0), axis=0, keepdims=True)
        meta[0, 0, k:k + 1, 0:tok] = ids[k:k + 1, :] * float(most) + rank
    meta[0, 0, 8:16, 0:tok] = weights

    pl.semaphore_wait(barrier, 6)
    load_tok.wait()

    first, second = pl.ds(0, half), pl.ds(half, half)
    quarters = [pl.ds(q * quarter, quarter) for q in range(4)]

    def move(tag, way, slot, cols, with_meta=False):
        dx, dy = slot
        shift = {"xp": (3, 0), "xm": (1, 0), "yp": (0, 3), "ym": (0, 1)}[way]
        to = ((dx + shift[0]) % 4, (dy + shift[1]) % 4)
        send((tag, way, to), way, gath.at[dx, dy, :, cols], gath.at[to[0], to[1], :, cols])
        if with_meta:
            send(("m" + tag, way, to), way, meta.at[dx, dy], meta.at[to[0], to[1]])

    def x_own():
        move("a", "xp", (0, 0), first, True)
        move("a", "xm", (0, 0), first, True)

    def y_own():
        move("b", "yp", (0, 0), second)
        move("b", "ym", (0, 0), second)

    def y_pass(dx):
        move("c", "yp", (dx, 0), first, True)
        move("c", "ym", (dx, 0), first, True)

    def x_pass(dy):
        move("d", "xp", (0, dy), second)
        move("d", "xm", (0, dy), second)

    def x_relay():
        move("e", "xp", (3, 0), quarters[0], True)
        move("e", "xm", (1, 0), quarters[1])

    def y_relay():
        move("f", "yp", (0, 3), quarters[2])
        move("f", "ym", (0, 1), quarters[3])

    def y_pass_relay(dx):
        move("g", "yp", (dx, 3), quarters[0], True)
        move("g", "ym", (dx, 1), quarters[1])

    def x_pass_relay(dy):
        move("h", "xp", (3, dy), quarters[2])
        move("h", "xm", (1, dy), quarters[3])

    def got_y_pass(dx):
        wait(("c", "yp", (dx, 3)), ("mc", "yp", (dx, 3)), ("c", "ym", (dx, 1)), ("mc", "ym", (dx, 1)))

    def got_x_pass(dy):
        wait(("d", "xp", (3, dy)), ("d", "xm", (1, dy)))

    def got_y_pass_relay(dx):
        wait(("g", "yp", (dx, 2)), ("mg", "yp", (dx, 2)), ("g", "ym", (dx, 2)))

    def got_x_pass_relay(dy):
        wait(("h", "xp", (2, dy)), ("h", "xm", (2, dy)))

    place_row = lax.broadcasted_iota(jnp.int32, (2 * most, tok), 0)
    wanted = jnp.where(place_row < most, ep * most + place_row, (other - 1) * most + place_row).astype(F32)

    def select(dx, dy):
        place = PLACE[dx, dy]
        one, scaled = jnp.zeros((2 * most, tok), F32), jnp.zeros((2 * most, tok), F32)
        for k in range(8):
            hit = meta[dx, dy, k:k + 1, 0:tok] == wanted
            one = one + jnp.where(hit, 1.0, 0.0)
            scaled = scaled + jnp.where(hit, meta[dx, dy, 8 + k:9 + k, 0:tok], 0.0)
        comb[place] = scaled.T.astype(BF16)
        pick = one.astype(BF16)

        @pl.loop(0, 4)
        def _(q):
            cols = pl.ds(pl.multiple_of(q * quarter, quarter), quarter)
            rows = jnp.dot(pick, gath[dx, dy, :, cols], preferred_element_type=F32).astype(BF16)
            xown[place, :, cols] = rows[:most]
            zsend[place, :, cols] = rows[most:]

        send(("z", place), "zm" if place % 2 else "zp", zsend.at[place], zrecv.at[place])

    def gate_up(rows_ref, group, hidden):
        rows = 8 * most
        tile = 256

        @pl.loop(0, hid // tile)
        def _(n):
            cols = pl.ds(pl.multiple_of(n * tile, tile), tile)
            block = rows_ref[8 * group:8 * group + 8].reshape(rows, width)
            gate = jnp.dot(block, wg[:, cols], preferred_element_type=F32)
            up = jnp.dot(block, wu[:, cols], preferred_element_type=F32)
            hidden[rows * group:rows * (group + 1), cols] = (gate / (1.0 + jnp.exp(-gate)) * up).astype(BF16)

    x_own()
    y_own()
    y_pass(0)
    x_pass(0)
    select(0, 0)
    wait(("a", "xp", (3, 0)), ("ma", "xp", (3, 0)), ("a", "xm", (1, 0)), ("ma", "xm", (1, 0)))
    wait(("b", "yp", (0, 3)), ("b", "ym", (0, 1)))
    x_relay()
    y_relay()
    for d in (1, 3):
        y_pass(d)
        x_pass(d)
    got_y_pass(0)
    got_x_pass(0)
    y_pass_relay(0)
    x_pass_relay(0)
    for slot in ORDER[1:5]:
        select(*slot)
    wait(("e", "xp", (2, 0)), ("me", "xp", (2, 0)), ("e", "xm", (2, 0)))
    wait(("f", "yp", (0, 2)), ("f", "ym", (0, 2)))
    y_pass(2)
    x_pass(2)
    for d in (1, 3):
        got_y_pass(d)
        got_x_pass(d)
        y_pass_relay(d)
        x_pass_relay(d)
    for slot in ORDER[5:9]:
        select(*slot)
    got_y_pass_relay(0)
    got_x_pass_relay(0)
    for slot in ORDER[9:11]:
        select(*slot)
    got_y_pass(2)
    got_x_pass(2)
    y_pass_relay(2)
    x_pass_relay(2)
    loads[0].wait()
    loads[1].wait()
    gate_up(xown, 0, hown)
    for d in (1, 3):
        got_y_pass_relay(d)
        got_x_pass_relay(d)
    for slot in ORDER[11:15]:
        select(*slot)
    got_y_pass_relay(2)
    got_x_pass_relay(2)
    select(2, 2)

    def chunk_cols(c):
        return pl.ds(c * (width // CHUNKS), width // CHUNKS)

    def down_z(group, c):
        rows = 8 * most
        out = jnp.dot(hz[rows * group:rows * (group + 1), :], wd[:, chunk_cols(c)], preferred_element_type=F32)
        zout[4 * group:4 * group + 4, :, :, chunk_cols(c)] = out.astype(BF16).reshape(4, 2, most, width // CHUNKS)
        for side, way in ((0, "zm"), (1, "zp")):
            send(
                ("r", group, c, side), way,
                zout.at[pl.ds(4 * group, 4), side, :, chunk_cols(c)],
                both.at[pl.ds(4 * group, 4), side, pl.ds(most, most), chunk_cols(c)],
            )

    def down_own(c):
        out = jnp.dot(hown[...], wd[:, chunk_cols(c)], preferred_element_type=F32)
        both[:, :, 0:most, chunk_cols(c)] = out.astype(BF16).reshape(8, 2, most, width // CHUNKS)

    for place in range(8):
        wait(("z", place))
    gate_up(zrecv, 0, hz)
    loads[2].wait()
    down_z(0, 0)
    down_z(0, 1)
    gate_up(xown, 1, hown)
    for place in range(8, 16):
        wait(("z", place))
    gate_up(zrecv, 1, hz)
    down_z(1, 0)
    down_z(1, 1)
    for c in (2, 3):
        down_z(0, c)
        down_z(1, c)
    for c in range(CHUNKS):
        down_own(c)

    unit = width // CHUNKS // 4

    def cols_of(c, start, count=1):
        return pl.ds((4 * c + start) * unit, count * unit)

    def expand(c):
        cols = chunk_cols(c)
        for group in (0, 1):
            wait(("r", group, c, 0), ("r", group, c, 1))

        def fill(dx, dy):
            place = PLACE[dx, dy]
            part[dx, dy, :, cols] = jnp.dot(
                comb[place], both[place // 2, place % 2, :, cols], preferred_element_type=F32
            ).astype(BF16)

        far = [slot for slot in ORDER if 2 in slot]
        for slot in far:
            fill(*slot)
        send(("1", c, "yp"), "yp", part.at[:, 2, :, cols_of(c, 0)], y1p.at[c])
        send(("1", c, "ym"), "ym", part.at[:, 2, :, cols_of(c, 1)], y1m.at[c])
        send(("1", c, "xp"), "xp", part.at[2, :, :, cols_of(c, 2)], x1p.at[c])
        send(("1", c, "xm"), "xm", part.at[2, :, :, cols_of(c, 3)], x1m.at[c])
        for slot in ORDER:
            if slot not in far:
                fill(*slot)

    def add(dx, dy, cols, *refs):
        total = part[dx, dy, :, cols].astype(F32)
        for ref in refs:
            total = total + ref[...].astype(F32)
        part[dx, dy, :, cols] = total.astype(BF16)

    def step_two(c):
        for way in ("yp", "ym", "xp", "xm"):
            wait(("1", c, way))
        for d in range(4):
            add(d, 1, cols_of(c, 0), y1p.at[c, d])
            add(d, 3, cols_of(c, 1), y1m.at[c, d])
            add(1, d, cols_of(c, 2), x1p.at[c, d])
            add(3, d, cols_of(c, 3), x1m.at[c, d])
        send(("2", c, "yp"), "yp", part.at[:, 1, :, cols_of(c, 0, 2)], y2p.at[c])
        send(("2", c, "ym"), "ym", part.at[:, 3, :, cols_of(c, 0, 2)], y2m.at[c])
        send(("2", c, "xp"), "xp", part.at[1, :, :, cols_of(c, 2, 2)], x2p.at[c])
        send(("2", c, "xm"), "xm", part.at[3, :, :, cols_of(c, 2, 2)], x2m.at[c])

    def step_three(c):
        for way in ("yp", "ym", "xp", "xm"):
            wait(("2", c, way))
        for d in (2, 1, 3, 0):
            add(d, 0, cols_of(c, 0, 2), y2p.at[c, d], y2m.at[c, d])
            add(0, d, cols_of(c, 2, 2), x2p.at[c, d], x2m.at[c, d])
            if d == 2:
                send(("4", c, "xp"), "xp", part.at[2, 0, :, cols_of(c, 0)], x4p.at[c])
                send(("4", c, "xm"), "xm", part.at[2, 0, :, cols_of(c, 1)], x4m.at[c])
                send(("4", c, "yp"), "yp", part.at[0, 2, :, cols_of(c, 2)], y4p.at[c])
                send(("4", c, "ym"), "ym", part.at[0, 2, :, cols_of(c, 3)], y4m.at[c])

    def step_four(c):
        for way in ("xp", "xm", "yp", "ym"):
            wait(("4", c, way))
        add(1, 0, cols_of(c, 0), x4p.at[c])
        add(3, 0, cols_of(c, 1), x4m.at[c])
        add(0, 1, cols_of(c, 2), y4p.at[c])
        add(0, 3, cols_of(c, 3), y4m.at[c])
        send(("5", c, "xp"), "xp", part.at[1, 0, :, cols_of(c, 0, 2)], x5p.at[c])
        send(("5", c, "xm"), "xm", part.at[3, 0, :, cols_of(c, 0, 2)], x5m.at[c])
        send(("5", c, "yp"), "yp", part.at[0, 1, :, cols_of(c, 2, 2)], y5p.at[c])
        send(("5", c, "ym"), "ym", part.at[0, 3, :, cols_of(c, 2, 2)], y5m.at[c])

    def step_five(c):
        for way in ("xp", "xm", "yp", "ym"):
            wait(("5", c, way))
        for start, plus, minus in ((0, x5p, x5m), (2, y5p, y5m)):
            cols = cols_of(c, start, 2)
            total = part[0, 0, :, cols].astype(F32) + plus[c].astype(F32) + minus[c].astype(F32)
            out_ref[:, cols] = total.astype(BF16)

    expand(0)
    step_two(0)
    expand(1)
    step_three(0)
    step_two(1)
    step_four(0)
    expand(2)
    step_three(1)
    step_two(2)
    step_five(0)
    step_four(1)
    expand(3)
    step_three(2)
    step_two(3)
    step_five(1)
    step_four(2)
    step_three(3)
    step_five(2)
    step_four(3)
    step_five(3)
    for copy in copies.values():
        copy.wait_send()


def shards(n_hi, tokens, expert_ids, gate_probs, w_gate, w_up, w_down):
    tok, width = tokens.shape
    hid = w_gate.shape[2]
    most = 32
    unit = width // CHUNKS // 4
    vmem = pl.BlockSpec(memory_space=pltpu.VMEM)
    hbm = pl.BlockSpec(memory_space=pl.ANY)
    wide = [pltpu.VMEM((CHUNKS, 4, tok, unit), BF16)] * 4 + [pltpu.VMEM((CHUNKS, 4, tok, 2 * unit), BF16)] * 4
    thin = [pltpu.VMEM((CHUNKS, tok, unit), BF16)] * 4 + [pltpu.VMEM((CHUNKS, tok, 2 * unit), BF16)] * 4
    return pl.pallas_call(
        functools.partial(kernel, (n_hi, tok, width, hid, most)),
        out_shape=jax.ShapeDtypeStruct((tok, width), BF16),
        in_specs=[hbm, vmem, vmem, hbm, hbm, hbm],
        out_specs=vmem,
        scratch_shapes=[
            pltpu.VMEM((4, 4, tok, width), BF16),
            pltpu.VMEM((4, 4, 16, 128), F32),
            pltpu.VMEM((16, tok, 2 * most), BF16),
            pltpu.VMEM((16, most, width), BF16),
            pltpu.VMEM((16, most, width), BF16),
            pltpu.VMEM((16, most, width), BF16),
            pltpu.VMEM((16 * most, hid), BF16),
            pltpu.VMEM((16 * most, hid), BF16),
            pltpu.VMEM((width, hid), BF16),
            pltpu.VMEM((width, hid), BF16),
            pltpu.VMEM((hid, width), BF16),
            pltpu.VMEM((8, 2, most, width), BF16),
            pltpu.VMEM((8, 2, 2 * most, width), BF16),
            pltpu.VMEM((4, 4, tok, width), BF16),
            *wide,
            *thin,
            pltpu.SemaphoreType.DMA((MAX_COPIES,)),
            pltpu.SemaphoreType.DMA((MAX_COPIES,)),
            pltpu.SemaphoreType.DMA((4,)),
        ],
        compiler_params=pltpu.CompilerParams(
            collective_id=0, has_side_effects=True, vmem_limit_bytes=60 * 1024 * 1024
        ),
        name="routed_experts",
    )(tokens, expert_ids.T, gate_probs.T, w_gate, w_up, w_down)


def solution(mesh):
    placed = (
        P(("dp", "ep"), None),
        P(("dp", "ep"), None),
        P(("dp", "ep"), None),
        P("ep", None, None),
        P("ep", None, None),
        P("ep", None, None),
    )
    return jax.shard_map(
        functools.partial(shards, mesh.shape["dp"] // 2), mesh=mesh, in_specs=placed,
        out_specs=P(("dp", "ep"), None), check_vma=False,
    )
```

```python
import functools

import jax
import jax.numpy as jnp
from jax import lax
from jax.experimental import pallas as pl
from jax.experimental.pallas import tpu as pltpu
from jax.sharding import PartitionSpec as P

MESH = pl.DeviceIdType.MESH
F32, BF16 = jnp.float32, jnp.bfloat16
OPPOSITE = {"xp": "xm", "xm": "xp", "yp": "ym", "ym": "yp", "zp": "zm", "zm": "zp"}

ORDER = [
    (0, 0), (1, 0), (3, 0), (0, 1), (0, 3), (1, 1), (1, 3), (3, 1),
    (3, 3), (0, 2), (2, 0), (1, 2), (3, 2), (2, 1), (2, 3), (2, 2),
]
PLACE = {slot: place for place, slot in enumerate(ORDER)}
PARTS = (2, 2, 2, 1, 1)
STEPS = (
    "E0", "E1", "A0", "A1", "E2", "B0", "B1", "E3", "A2", "E4", "C0", "C1", "A3", "B2", "A4", "D0", "D1", "B3", "C2", "B4",
    "C3", "D2", "C4", "D3", "D4",
)
MAX_SEMS = 64


def kernel(
    sizes, tok_hbm, ids_ref, probs_ref, wg_hbm, wu_hbm, wd_hbm, out_hbm,
    gath, meta, comb, xown, zsend, zrecv, hown, hz, wg, wu, wd, zout, both, part, picks,
    r1p, r1m, r2p, r2m, r4p, r4m, r5p, r5m, outv,
    send_sem, recv_sem, local_sem,
):
    n_hi, tok, width, hid, most = sizes
    half, quarter = width // 2, width // 4
    ep, dp = lax.axis_index("ep"), lax.axis_index("dp")
    x, y, z_lo = lax.rem(ep, 4), lax.rem(ep // 4, 4), ep // 16
    z_hi, core = dp // 2, lax.rem(dp, 2)

    def at(xx, yy, zz):
        return zz * 16 + yy * 4 + xx

    cross = 1 - core
    here = z_hi * 2 + cross
    z_up = lax.rem(z_hi + z_lo, n_hi) * 2 + cross
    z_down = lax.rem(z_hi + z_lo + n_hi - 1, n_hi) * 2 + cross
    target = {
        "xp": {"ep": at(lax.rem(x + 1, 4), y, z_lo), "dp": here},
        "xm": {"ep": at(lax.rem(x + 3, 4), y, z_lo), "dp": here},
        "yp": {"ep": at(x, lax.rem(y + 1, 4), z_lo), "dp": here},
        "ym": {"ep": at(x, lax.rem(y + 3, 4), z_lo), "dp": here},
        "zp": {"ep": at(x, y, 1 - z_lo), "dp": z_up},
        "zm": {"ep": at(x, y, 1 - z_lo), "dp": z_down},
    }
    other = at(x, y, 1 - z_lo)

    sems = {}

    def sem(array, kind):
        return array.at[sems.setdefault(kind, len(sems))]

    def send(way, src, dst, leaves, lands):
        pltpu.make_async_remote_copy(
            src_ref=src, dst_ref=dst, send_sem=sem(send_sem, leaves), recv_sem=sem(recv_sem, lands),
            device_id=target[way], device_id_type=MESH,
        ).start()

    def wait(lands, *like):
        pltpu.make_async_copy(*like, *like, sem(recv_sem, lands)).wait()

    def drain(leaves, like):
        pltpu.make_async_copy(like, like, sem(send_sem, leaves)).wait()

    load_tok = pltpu.make_async_copy(tok_hbm, gath.at[0, 0], local_sem.at[0])
    load_tok.start()
    loads = [
        pltpu.make_async_copy(src.at[0], dst, local_sem.at[1 + i])
        for i, (src, dst) in enumerate(((wg_hbm, wg), (wu_hbm, wu), (wd_hbm, wd)))
    ]
    for load in loads:
        load.start()

    barrier = pltpu.get_barrier_semaphore()
    for way in target:
        pl.semaphore_signal(barrier, inc=1, device_id=target[way], device_id_type=MESH)

    ids = ids_ref[...].astype(F32)
    probs = probs_ref[...]
    weights = probs / jnp.sum(probs, axis=0, keepdims=True)
    experts = lax.broadcasted_iota(jnp.int32, (32, tok), 0).astype(F32)
    named = jnp.zeros((32, tok), F32)
    for k in range(8):
        named = named + jnp.where(ids[k:k + 1, :] == experts, 1.0, 0.0)
    before = lax.broadcasted_iota(jnp.int32, (tok, tok), 0) < lax.broadcasted_iota(jnp.int32, (tok, tok), 1)
    ranks = jnp.dot(named.astype(BF16), before.astype(F32).astype(BF16), preferred_element_type=F32)
    for k in range(8):
        rank = jnp.sum(jnp.where(ids[k:k + 1, :] == experts, ranks, 0.0), axis=0, keepdims=True)
        meta[0, 0, k:k + 1, 0:tok] = ids[k:k + 1, :] * float(most) + rank
    meta[0, 0, 8:16, 0:tok] = weights

    pl.semaphore_wait(barrier, 6)
    load_tok.wait()

    first, second = pl.ds(0, half), pl.ds(half, half)
    quarters = [pl.ds(q * quarter, quarter) for q in range(4)]

    def move(kind, leaves, way, slot, cols, with_meta=None):
        dx, dy = slot
        shift = {"xp": (3, 0), "xm": (1, 0), "yp": (0, 3), "ym": (0, 1)}[way]
        to = ((dx + shift[0]) % 4, (dy + shift[1]) % 4)
        send(way, gath.at[dx, dy, :, cols], gath.at[to[0], to[1], :, cols], leaves, kind)
        if with_meta:
            send(way, meta.at[dx, dy], meta.at[to[0], to[1]], with_meta, "m" + kind)

    def own_first():
        for way in ("xp", "xm"):
            move("own", "own", way, (0, 0), first, "m12")
        for way in ("yp", "ym"):
            move("own", "own", way, (0, 0), second, "m3")

    def own_second():
        for way in ("yp", "ym"):
            move("pass0", "own", way, (0, 0), first)
        for way in ("xp", "xm"):
            move("pass0", "own", way, (0, 0), second)

    def own_relay():
        move("far", "pass", "xp", (3, 0), quarters[0], "m12")
        move("far", "pass", "xm", (1, 0), quarters[1])
        move("far", "pass", "yp", (0, 3), quarters[2], "m3")
        move("far", "pass", "ym", (0, 1), quarters[3])

    def passes(d):
        move(f"pass{d}", "pass", "yp", (d, 0), first, "m12")
        move(f"pass{d}", "pass", "ym", (d, 0), first, "m12")
        move(f"pass{d}", "second", "xp", (0, d), second)
        move(f"pass{d}", "second", "xm", (0, d), second)

    def relays(d):
        move(f"relay{d}", "relay", "yp", (d, 3), quarters[0], "m12" if d else None)
        move(f"relay{d}", "relay", "ym", (d, 1), quarters[1])
        move(f"relay{d}", "relay", "xp", (3, d), quarters[2])
        move(f"relay{d}", "relay", "xm", (1, d), quarters[3])

    def got_own():
        wait("own", gath.at[0, 0:2])
        wait("mown", meta.at[0])

    def got_far():
        wait("far", gath.at[0, 0])
        wait("mfar", meta.at[0, 0:2])

    def got_passes(d):
        wait(f"pass{d}", gath.at[0, 0:2])
        if d:
            wait(f"mpass{d}", meta.at[0, 0:2])

    def got_relays(d):
        wait(f"relay{d}", gath.at[0, 0])
        if d:
            wait(f"mrelay{d}", meta.at[0, 0])

    place_row = lax.broadcasted_iota(jnp.int32, (2 * most, tok), 0)
    wanted = jnp.where(place_row < most, ep * most + place_row, (other - 1) * most + place_row).astype(F32)

    def build(dx, dy):
        place = PLACE[dx, dy]
        one, scaled = jnp.zeros((2 * most, tok), F32), jnp.zeros((2 * most, tok), F32)
        for k in range(8):
            hit = meta[dx, dy, k:k + 1, 0:tok] == wanted
            one = one + jnp.where(hit, 1.0, 0.0)
            scaled = scaled + jnp.where(hit, meta[dx, dy, 8 + k:9 + k, 0:tok], 0.0)
        comb[place] = scaled.T.astype(BF16)
        picks[place] = one.astype(BF16)

    def select(dx, dy, side):
        place = PLACE[dx, dy]

        @pl.loop(0, 2)
        def _(q):
            cols = pl.ds(pl.multiple_of(side * half + q * quarter, quarter), quarter)
            rows = jnp.dot(picks[place], gath[dx, dy, :, cols], preferred_element_type=F32).astype(BF16)
            xown[place, :, cols] = rows[:most]
            zsend[place, :, cols] = rows[most:]

        cols = (first, second)[side]
        way = "zm" if place % 2 else "zp"
        send(way, zsend.at[place, :, cols], zrecv.at[place, :, cols], "rows", f"rows{place // 4}")

    def select_all(*slots):
        for slot in slots:
            build(*slot)
            select(*slot, 0)
            select(*slot, 1)

    def got_rows(group):
        wait(f"rows{group}", zrecv.at[pl.ds(4 * group, 4)])

    tile = 256

    def gate_up(rows_ref, hidden, place, places, start=0, stop=hid // tile):
        rows = places * most

        @pl.loop(start, stop)
        def _(n):
            cols = pl.ds(pl.multiple_of(n * tile, tile), tile)
            block = rows_ref[place:place + places].reshape(rows, width)
            gate = jnp.dot(block, wg[:, cols], preferred_element_type=F32)
            up = jnp.dot(block, wu[:, cols], preferred_element_type=F32)
            hidden[place * most:place * most + rows, cols] = (gate / (1.0 + jnp.exp(-gate)) * up).astype(BF16)

    own_first()
    own_second()
    select_all((0, 0))
    got_own()
    own_relay()
    passes(1)
    passes(3)
    for slot in ORDER[1:5]:
        build(*slot)
        select(*slot, 0 if slot[1] == 0 else 1)
    got_passes(0)
    relays(0)
    for slot in ORDER[1:5]:
        select(*slot, 1 if slot[1] == 0 else 0)
    got_far()
    passes(2)
    got_passes(1)
    relays(1)
    select_all((1, 1))
    got_passes(3)
    relays(3)
    select_all((1, 3), (3, 1), (3, 3))
    got_relays(0)
    select_all((0, 2), (2, 0))
    loads[0].wait()
    loads[1].wait()
    gate_up(xown, hown, 0, 8, 0, 1)
    got_passes(2)
    relays(2)
    gate_up(xown, hown, 0, 8, 1, 2)
    got_relays(1)
    select_all((1, 2), (2, 1))
    got_relays(3)
    select_all((3, 2), (2, 3))
    gate_up(xown, hown, 0, 8, 2, 3)
    got_relays(2)
    select_all((2, 2))

    starts = [sum(PARTS[:c]) * width // sum(PARTS) for c in range(len(PARTS) + 1)]

    def chunk_cols(c):
        return pl.ds(starts[c], starts[c + 1] - starts[c])

    def sides(c):
        middle = (starts[c] + starts[c + 1]) // 2
        return pl.ds(starts[c], middle - starts[c]), pl.ds(middle, starts[c + 1] - middle)

    top, low = pl.ds(0, tok // 2), pl.ds(tok // 2, tok // 2)

    def down_z(group, c):
        rows = 8 * most
        out = jnp.dot(hz[rows * group:rows * (group + 1), :], wd[:, chunk_cols(c)], preferred_element_type=F32)
        zout[4 * group:4 * group + 4, :, :, chunk_cols(c)] = out.astype(BF16).reshape(4, 2, most, chunk_cols(c).size)
        for side, way in ((0, "zm"), (1, "zp")):
            send(
                way,
                zout.at[pl.ds(4 * group, 4), side, :, chunk_cols(c)],
                both.at[pl.ds(4 * group, 4), side, pl.ds(most, most), chunk_cols(c)],
                "back", f"back{c}",
            )

    def down_own(c):
        out = jnp.dot(hown[...], wd[:, chunk_cols(c)], preferred_element_type=F32)
        both[:, :, 0:most, chunk_cols(c)] = out.astype(BF16).reshape(8, 2, most, chunk_cols(c).size)

    got_rows(0)
    got_rows(1)
    gate_up(zrecv, hz, 0, 8)
    loads[2].wait()
    down_z(0, 0)
    down_z(0, 1)
    gate_up(xown, hown, 8, 8)
    got_rows(2)
    gate_up(zrecv, hz, 8, 4)
    down_own(0)
    down_own(1)
    got_rows(3)
    gate_up(zrecv, hz, 12, 4)
    down_z(1, 0)
    down_z(1, 1)
    for c in range(2, len(PARTS)):
        down_z(0, c)
        down_z(1, c)

    def expand(c):
        cols = chunk_cols(c)
        left, right = sides(c)
        if c >= 2:
            down_own(c)
        wait(f"back{c}", zout.at[:, :, :, cols])

        def fill(dx, dy):
            place = PLACE[dx, dy]
            part[dx, dy, :, cols] = jnp.dot(
                comb[place], both[place // 2, place % 2, :, cols], preferred_element_type=F32
            ).astype(BF16)

        far = [slot for slot in ORDER if 2 in slot]
        for slot in far:
            fill(*slot)
        send("yp", part.at[:, 2, top, left], r1p.at[:, :, left], "1p", f"1{c}")
        send("ym", part.at[:, 2, low, left], r1m.at[:, :, left], "1m", f"1{c}")
        send("xp", part.at[2, :, top, right], r1p.at[:, :, right], "1p", f"1{c}")
        send("xm", part.at[2, :, low, right], r1m.at[:, :, right], "1m", f"1{c}")
        for slot in ORDER:
            if slot not in far:
                fill(*slot)
        halves_two(c, low, top)

    def halves_two(c, plus, minus):
        left, right = sides(c)
        send("yp", part.at[:, 1, plus, left], r2p.at[:, plus, left], "2p", f"2{c}")
        send("ym", part.at[:, 3, minus, left], r2m.at[:, minus, left], "2m", f"2{c}")
        send("xp", part.at[1, :, plus, right], r2p.at[:, plus, right], "2p", f"2{c}")
        send("xm", part.at[3, :, minus, right], r2m.at[:, minus, right], "2m", f"2{c}")

    def halves_five(c, plus, minus):
        left, right = sides(c)
        send("xp", part.at[1, 0, plus, left], r5p.at[plus, left], "5p", f"5{c}")
        send("xm", part.at[3, 0, minus, left], r5m.at[minus, left], "5m", f"5{c}")
        send("yp", part.at[0, 1, plus, right], r5p.at[plus, right], "5p", f"5{c}")
        send("ym", part.at[0, 3, minus, right], r5m.at[minus, right], "5m", f"5{c}")

    def double(c):
        return pl.ds(0, 2 * chunk_cols(c).size)

    def add(dx, dy, rows, cols, *refs):
        total = part[dx, dy, rows, cols].astype(F32)
        for ref in refs:
            total = total + ref[...].astype(F32)
        part[dx, dy, rows, cols] = total.astype(BF16)

    every = pl.ds(0, tok)

    def step_two(c):
        left, right = sides(c)
        wait(f"1{c}", r1p.at[:, :, double(c)])
        for d in range(4):
            add(d, 1, top, left, r1p.at[d, :, left])
            add(d, 3, low, left, r1m.at[d, :, left])
            add(1, d, top, right, r1p.at[d, :, right])
            add(3, d, low, right, r1m.at[d, :, right])
        halves_two(c, top, low)

    def step_three(c):
        left, right = sides(c)
        wait(f"2{c}", r2p.at[:, :, double(c)])
        for d in (2, 1, 3, 0):
            add(d, 0, every, left, r2p.at[d, :, left], r2m.at[d, :, left])
            add(0, d, every, right, r2p.at[d, :, right], r2m.at[d, :, right])
            if d == 2:
                send("xp", part.at[2, 0, top, left], r4p.at[:, left], "4p", f"4{c}")
                send("xm", part.at[2, 0, low, left], r4m.at[:, left], "4m", f"4{c}")
                send("yp", part.at[0, 2, top, right], r4p.at[:, right], "4p", f"4{c}")
                send("ym", part.at[0, 2, low, right], r4m.at[:, right], "4m", f"4{c}")
            if d == 3:
                halves_five(c, low, top)

    def step_four(c):
        left, right = sides(c)
        wait(f"4{c}", r4p.at[:, double(c)])
        add(1, 0, top, left, r4p.at[:, left])
        add(3, 0, low, left, r4m.at[:, left])
        add(0, 1, top, right, r4p.at[:, right])
        add(0, 3, low, right, r4m.at[:, right])
        halves_five(c, top, low)

    stores = []

    def step_five(c):
        wait(f"5{c}", r5p.at[:, double(c)])
        for cols in sides(c):
            total = part[0, 0, :, cols].astype(F32) + r5p[:, cols].astype(F32) + r5m[:, cols].astype(F32)
            outv[:, cols] = total.astype(BF16)
        cols = chunk_cols(c)
        store = pltpu.make_async_copy(outv.at[:, cols], out_hbm.at[:, cols], local_sem.at[4 + c])
        store.start()
        stores.append(store)

    run = {"E": expand, "A": step_two, "B": step_three, "C": step_four, "D": step_five}
    for step in STEPS:
        run[step[0]](int(step[1]))
    drain("own", gath.at[0])
    drain("pass", gath.at[0])
    drain("second", gath.at[0, 0:3])
    drain("relay", gath.at[0])
    drain("m12", meta.at[0:3])
    drain("m3", meta.at[0, 0:3])
    drain("rows", zsend)
    drain("back", zout)
    for kind, like in (("1p", r1p), ("1m", r1m), ("2p", r2p), ("2m", r2m), ("4p", r4p), ("4m", r4m), ("5p", r5p), ("5m", r5m)):
        drain(kind, like)
    for store in stores:
        store.wait()


def shards(n_hi, tokens, expert_ids, gate_probs, w_gate, w_up, w_down):
    tok, width = tokens.shape
    hid = w_gate.shape[2]
    most = 32
    vmem = pl.BlockSpec(memory_space=pltpu.VMEM)
    hbm = pl.BlockSpec(memory_space=pl.ANY)
    return pl.pallas_call(
        functools.partial(kernel, (n_hi, tok, width, hid, most)),
        out_shape=jax.ShapeDtypeStruct((tok, width), BF16),
        in_specs=[hbm, vmem, vmem, hbm, hbm, hbm],
        out_specs=hbm,
        scratch_shapes=[
            pltpu.VMEM((4, 4, tok, width), BF16),
            pltpu.VMEM((4, 4, 16, 128), F32),
            pltpu.VMEM((16, tok, 2 * most), BF16),
            pltpu.VMEM((16, most, width), BF16),
            pltpu.VMEM((16, most, width), BF16),
            pltpu.VMEM((16, most, width), BF16),
            pltpu.VMEM((16 * most, hid), BF16),
            pltpu.VMEM((16 * most, hid), BF16),
            pltpu.VMEM((width, hid), BF16),
            pltpu.VMEM((width, hid), BF16),
            pltpu.VMEM((hid, width), BF16),
            pltpu.VMEM((8, 2, most, width), BF16),
            pltpu.VMEM((8, 2, 2 * most, width), BF16),
            pltpu.VMEM((4, 4, tok, width), BF16),
            pltpu.VMEM((16, 2 * most, tok), BF16),
            pltpu.VMEM((4, tok // 2, width), BF16),
            pltpu.VMEM((4, tok // 2, width), BF16),
            pltpu.VMEM((4, tok, width), BF16),
            pltpu.VMEM((4, tok, width), BF16),
            pltpu.VMEM((tok // 2, width), BF16),
            pltpu.VMEM((tok // 2, width), BF16),
            pltpu.VMEM((tok, width), BF16),
            pltpu.VMEM((tok, width), BF16),
            pltpu.VMEM((tok, width), BF16),
            pltpu.SemaphoreType.DMA((MAX_SEMS,)),
            pltpu.SemaphoreType.DMA((MAX_SEMS,)),
            pltpu.SemaphoreType.DMA((4 + len(PARTS),)),
        ],
        compiler_params=pltpu.CompilerParams(
            collective_id=0, has_side_effects=True, vmem_limit_bytes=60 * 1024 * 1024
        ),
        name="routed_experts",
    )(tokens, expert_ids.T, gate_probs.T, w_gate, w_up, w_down)


def solution(mesh):
    placed = (
        P(("dp", "ep"), None),
        P(("dp", "ep"), None),
        P(("dp", "ep"), None),
        P("ep", None, None),
        P("ep", None, None),
        P("ep", None, None),
    )
    return jax.shard_map(
        functools.partial(shards, mesh.shape["dp"] // 2), mesh=mesh, in_specs=placed,
        out_specs=P(("dp", "ep"), None), check_vma=False,
    )
```

```python
import functools

import jax
import jax.numpy as jnp
from jax import lax
from jax.experimental import pallas as pl
from jax.experimental.pallas import tpu as pltpu
from jax.sharding import PartitionSpec as P

MESH = pl.DeviceIdType.MESH
F32, BF16 = jnp.float32, jnp.bfloat16
OPPOSITE = {"xp": "xm", "xm": "xp", "yp": "ym", "ym": "yp", "zp": "zm", "zm": "zp"}

CLUSTER = [(0, 0), (1, 0), (3, 0), (0, 1), (0, 3)]
OTHERS = [(1, 1), (3, 3), (1, 3), (3, 1), (0, 2), (2, 0), (1, 2), (2, 1), (3, 2), (2, 3), (2, 2)]
PLACE = {slot: place for place, slot in enumerate(CLUSTER + [None] + OTHERS) if slot}
PLACES = 18
NEAR = {1: "xp", 2: "xm", 3: "yp", 4: "ym"}
PARTS = (1, 1, 2, 2, 1, 1)
STEPS = (
    "E0", "E1", "A0", "F0", "A1", "E2", "B0", "B1", "A2", "E3", "C0", "C1", "E4", "B2", "E5", "A3", "D0", "D1", "A4", "C2", "A5",
    "B3", "B4", "D2", "B5", "C3", "C4", "C5", "D3", "D4", "D5",
)
MAX_SEMS = 96


def kernel(
    sizes, tok_hbm, ids_ref, probs_ref, wg_hbm, wu_hbm, wd_hbm, out_hbm,
    gath, meta, comb, xown, zsend, zrecv, hown, hz, wg, wu, wd, zout, both, part, picks,
    fgath, fmeta, fcomb, fpick, fsend, frecv, fsum, zsum,
    r1p, r1m, r2p, r2m, r4p, r4m, r5p, r5m, outv,
    send_sem, recv_sem, local_sem,
):
    n_hi, tok, width, hid, most = sizes
    half, quarter = width // 2, width // 4
    ep, dp = lax.axis_index("ep"), lax.axis_index("dp")
    x, y, z_lo = lax.rem(ep, 4), lax.rem(ep // 4, 4), ep // 16
    z_hi, core = dp // 2, lax.rem(dp, 2)

    def at(xx, yy, zz):
        return zz * 16 + yy * 4 + xx

    cross = 1 - core
    here = z_hi * 2 + cross
    z_up = lax.rem(z_hi + z_lo, n_hi) * 2 + cross
    z_down = lax.rem(z_hi + z_lo + n_hi - 1, n_hi) * 2 + cross
    target = {
        "xp": {"ep": at(lax.rem(x + 1, 4), y, z_lo), "dp": here},
        "xm": {"ep": at(lax.rem(x + 3, 4), y, z_lo), "dp": here},
        "yp": {"ep": at(x, lax.rem(y + 1, 4), z_lo), "dp": here},
        "ym": {"ep": at(x, lax.rem(y + 3, 4), z_lo), "dp": here},
        "zp": {"ep": at(x, y, 1 - z_lo), "dp": z_up},
        "zm": {"ep": at(x, y, 1 - z_lo), "dp": z_down},
    }
    other = at(x, y, 1 - z_lo)

    sems = {}

    def sem(array, kind):
        return array.at[sems.setdefault(kind, len(sems))]

    def send(way, src, dst, leaves, lands):
        pltpu.make_async_remote_copy(
            src_ref=src, dst_ref=dst, send_sem=sem(send_sem, leaves), recv_sem=sem(recv_sem, lands),
            device_id=target[way], device_id_type=MESH,
        ).start()

    def wait(lands, *like):
        pltpu.make_async_copy(*like, *like, sem(recv_sem, lands)).wait()

    def drain(leaves, like):
        pltpu.make_async_copy(like, like, sem(send_sem, leaves)).wait()

    load_tok = pltpu.make_async_copy(tok_hbm, gath.at[0, 0], local_sem.at[0])
    load_tok.start()
    loads = [
        pltpu.make_async_copy(src.at[0], dst, local_sem.at[1 + i])
        for i, (src, dst) in enumerate(((wg_hbm, wg), (wu_hbm, wu), (wd_hbm, wd)))
    ]
    for load in loads:
        load.start()

    barrier = pltpu.get_barrier_semaphore()
    for way in target:
        pl.semaphore_signal(barrier, inc=1, device_id=target[way], device_id_type=MESH)

    ids = ids_ref[...].astype(F32)
    probs = probs_ref[...]
    weights = probs / jnp.sum(probs, axis=0, keepdims=True)
    experts = lax.broadcasted_iota(jnp.int32, (32, tok), 0).astype(F32)
    named = jnp.zeros((32, tok), F32)
    for k in range(8):
        named = named + jnp.where(ids[k:k + 1, :] == experts, 1.0, 0.0)
    before = lax.broadcasted_iota(jnp.int32, (tok, tok), 0) < lax.broadcasted_iota(jnp.int32, (tok, tok), 1)
    ranks = jnp.dot(named.astype(BF16), before.astype(F32).astype(BF16), preferred_element_type=F32)
    for k in range(8):
        rank = jnp.sum(jnp.where(ids[k:k + 1, :] == experts, ranks, 0.0), axis=0, keepdims=True)
        meta[0, 0, k:k + 1, 0:tok] = ids[k:k + 1, :] * float(most) + rank
    meta[0, 0, 8:16, 0:tok] = weights

    pl.semaphore_wait(barrier, 6)
    load_tok.wait()

    first, second = pl.ds(0, half), pl.ds(half, half)
    quarters = [pl.ds(q * quarter, quarter) for q in range(4)]

    def move(kind, leaves, way, slot, cols, with_meta=None):
        dx, dy = slot
        shift = {"xp": (3, 0), "xm": (1, 0), "yp": (0, 3), "ym": (0, 1)}[way]
        to = ((dx + shift[0]) % 4, (dy + shift[1]) % 4)
        send(way, gath.at[dx, dy, :, cols], gath.at[to[0], to[1], :, cols], leaves, kind)
        if with_meta:
            send(way, meta.at[dx, dy], meta.at[to[0], to[1]], with_meta, "m" + kind)

    def own_first():
        for way in ("xp", "xm"):
            move("own", "own", way, (0, 0), first, "m12")
        for way in ("yp", "ym"):
            move("own", "own", way, (0, 0), second, "m3")

    def own_second():
        for way in ("yp", "ym"):
            move("pass0", "own", way, (0, 0), first)
        for way in ("xp", "xm"):
            move("pass0", "own", way, (0, 0), second)

    def own_relay():
        move("far", "pass", "xp", (3, 0), quarters[0], "m12")
        move("far", "pass", "xm", (1, 0), quarters[1])
        move("far", "pass", "yp", (0, 3), quarters[2], "m3")
        move("far", "pass", "ym", (0, 1), quarters[3])

    def passes(d):
        e = (4 - d) % 4
        move(f"pass{d}", "pass", "ym", (d, 0), first, "m12")
        move(f"pass{d}", "second", "xm", (0, d), second)
        move(f"pass{d}", "pass", "yp", (e, 0), first, "m12")
        move(f"pass{d}", "second", "xp", (0, e), second)

    def relays(d):
        move(f"relay{d}", "relay", "yp", (d, 3), quarters[0], "m12" if d else None)
        move(f"relay{d}", "relay", "ym", (d, 1), quarters[1])
        move(f"relay{d}", "relay", "xp", (3, d), quarters[2])
        move(f"relay{d}", "relay", "xm", (1, d), quarters[3])

    def got_own():
        wait("own", gath.at[0, 0:2])
        wait("mown", meta.at[0])

    def got_far():
        wait("far", gath.at[0, 0])
        wait("mfar", meta.at[0, 0:2])

    def got_passes(d):
        wait(f"pass{d}", gath.at[0, 0:2])
        if d:
            wait(f"mpass{d}", meta.at[0, 0:2])

    def got_relays(d):
        wait(f"relay{d}", gath.at[0, 0])
        if d:
            wait(f"mrelay{d}", meta.at[0, 0])

    place_row = lax.broadcasted_iota(jnp.int32, (2 * most, tok), 0)
    wanted = jnp.where(place_row < most, ep * most + place_row, (other - 1) * most + place_row).astype(F32)

    def build(dx, dy):
        place = PLACE[dx, dy]
        one, scaled = jnp.zeros((2 * most, tok), F32), jnp.zeros((2 * most, tok), F32)
        for k in range(8):
            hit = meta[dx, dy, k:k + 1, 0:tok] == wanted
            one = one + jnp.where(hit, 1.0, 0.0)
            scaled = scaled + jnp.where(hit, meta[dx, dy, 8 + k:9 + k, 0:tok], 0.0)
        comb[place] = scaled.T.astype(BF16)
        picks[place] = one.astype(BF16)

    def select(dx, dy):
        place = PLACE[dx, dy]
        rows = most if place < 5 else 2 * most

        @pl.loop(0, 4)
        def _(q):
            cols = pl.ds(pl.multiple_of(q * quarter, quarter), quarter)
            chosen = jnp.dot(picks[place, :rows], gath[dx, dy, :, cols], preferred_element_type=F32).astype(BF16)
            xown[place, :, cols] = chosen[:most]
            if place >= 5:
                zsend[place, :, cols] = chosen[most:]

        if place >= 5:
            group = min((place - 6) // 4, 2)
            send("zm" if place % 2 else "zp", zsend.at[place], zrecv.at[place], "rows", f"rows{group}")

    def select_all(*slots):
        for slot in slots:
            build(*slot)
            select(*slot)

    def got_rows(group):
        wait(f"rows{group}", zrecv.at[pl.ds(0, (4, 4, 3)[group])])

    near_experts = (ep, at(lax.rem(x + 1, 4), y, z_lo), at(lax.rem(x + 3, 4), y, z_lo), at(x, lax.rem(y + 1, 4), z_lo), at(x, lax.rem(y + 3, 4), z_lo))

    def select_foreign():
        for i, expert in enumerate(near_experts):
            row = (expert * most + lax.broadcasted_iota(jnp.int32, (most, tok), 0)).astype(F32)
            one, scaled = jnp.zeros((most, tok), F32), jnp.zeros((most, tok), F32)
            for k in range(8):
                hit = fmeta[k:k + 1, 0:tok] == row
                one = one + jnp.where(hit, 1.0, 0.0)
                scaled = scaled + jnp.where(hit, fmeta[8 + k:9 + k, 0:tok], 0.0)
            fcomb[i] = scaled.T.astype(BF16)
            fpick[i * most:(i + 1) * most, :] = one.astype(BF16)

        @pl.loop(0, 4)
        def _(q):
            cols = pl.ds(pl.multiple_of(q * quarter, quarter), quarter)
            chosen = jnp.dot(fpick[...], fgath[:, cols], preferred_element_type=F32).astype(BF16)
            zrecv[0, :, cols] = chosen[:most]
            for i in range(4):
                fsend[i, :, cols] = chosen[(i + 1) * most:(i + 2) * most]

    def send_near():
        for i, (way, slot) in enumerate((("xp", (3, 0)), ("xm", (1, 0)), ("yp", (0, 3)), ("ym", (0, 1)))):
            send(way, fsend.at[i], zrecv.at[PLACE[slot]], "near", "near")

    def back_near():
        for place, way in NEAR.items():
            index = ("xm", "xp", "ym", "yp").index(way)
            send(way, zout.at[place // 2, place % 2], frecv.at[index], "nearback", "nearback")

    def sum_near():
        wait("nearback", frecv)

        @pl.loop(0, 4)
        def _(q):
            cols = pl.ds(pl.multiple_of(q * quarter, quarter), quarter)
            total = jnp.dot(fcomb[0], zout[0, 0, :, cols], preferred_element_type=F32)
            for i in range(4):
                total = total + jnp.dot(fcomb[i + 1], frecv[i, :, cols], preferred_element_type=F32)
            fsum[:, cols] = total.astype(BF16)

        send("zp", fsum, zsum, "sum", "sum")

    tile = 256

    def gate_up(rows_ref, hidden, place, places, start=0, stop=hid // tile):
        rows = places * most

        @pl.loop(start, stop)
        def _(n):
            cols = pl.ds(pl.multiple_of(n * tile, tile), tile)
            block = rows_ref[place:place + places].reshape(rows, width)
            gate = jnp.dot(block, wg[:, cols], preferred_element_type=F32)
            up = jnp.dot(block, wu[:, cols], preferred_element_type=F32)
            hidden[place * most:place * most + rows, cols] = (gate / (1.0 + jnp.exp(-gate)) * up).astype(BF16)

    own_first()
    own_second()
    send("zm", gath.at[0, 0], fgath, "whole", "whole")
    send("zm", meta.at[0, 0], fmeta, "mwhole", "mwhole")
    select_all((0, 0))
    got_own()
    passes(1)
    own_relay()
    passes(3)
    for slot in CLUSTER[1:]:
        build(*slot)
    got_passes(0)
    relays(0)
    for slot in CLUSTER[1:]:
        select(*slot)
    wait("whole", fgath)
    wait("mwhole", fmeta)
    select_foreign()
    loads[0].wait()
    loads[1].wait()
    gate_up(xown, hown, 0, 5, 0, 2)
    got_passes(1)
    select_all((1, 1), (3, 3))
    got_far()
    passes(2)
    gate_up(xown, hown, 0, 5, 2, 3)
    got_passes(3)
    relays(1)
    relays(3)
    select_all((1, 3), (3, 1))
    got_relays(0)
    select_all((0, 2), (2, 0))
    gate_up(xown, hown, 6, 6, 0, 1)
    got_passes(2)
    relays(2)
    send_near()
    gate_up(xown, hown, 6, 6, 1, 2)
    got_relays(1)
    select_all((1, 2), (2, 1))
    got_relays(3)
    select_all((3, 2), (2, 3))
    got_relays(2)
    select_all((2, 2))

    starts = [sum(PARTS[:c]) * width // sum(PARTS) for c in range(len(PARTS) + 1)]

    def chunk_cols(c):
        return pl.ds(starts[c], starts[c + 1] - starts[c])

    def sides(c):
        middle = (starts[c] + starts[c + 1]) // 2
        return pl.ds(starts[c], middle - starts[c]), pl.ds(middle, starts[c + 1] - middle)

    top, low = pl.ds(0, tok // 2), pl.ds(tok // 2, tok // 2)

    def down_z(part_of, c):
        place, places = ((6, 8), (14, 3))[part_of]
        cols = chunk_cols(c)
        out = jnp.dot(hz[most * place:most * (place + places), :], wd[:, cols], preferred_element_type=F32).astype(BF16)
        for i in range(places):
            zout[(place + i) // 2, (place + i) % 2, :, cols] = out[most * i:most * (i + 1)]
        for side, way in ((0, "zm"), (1, "zp")):
            pairs = pl.ds(place // 2, (places + 1 - side) // 2)
            send(
                way,
                zout.at[pairs, side, :, cols],
                both.at[pairs, side, pl.ds(most, most), cols],
                "back", f"back{c}",
            )

    def down_near():
        @pl.loop(0, 4)
        def _(q):
            cols = pl.ds(pl.multiple_of(q * quarter, quarter), quarter)
            out = jnp.dot(hz[0:5 * most, :], wd[:, cols], preferred_element_type=F32).astype(BF16)
            for i in range(5):
                zout[i // 2, i % 2, :, cols] = out[most * i:most * (i + 1)]

        back_near()

    def down_own(c):
        cols = chunk_cols(c)
        out = jnp.dot(hown[...], wd[:, cols], preferred_element_type=F32).astype(BF16)
        for slot, place in PLACE.items():
            both[place // 2, place % 2, 0:most, cols] = out[most * place:most * (place + 1)]

    gate_up(xown, hown, 6, 6, 2, 3)
    gate_up(xown, hown, 12, 5)
    got_rows(0)
    got_rows(1)
    gate_up(zrecv, hz, 6, 8)
    loads[2].wait()
    down_z(0, 0)
    down_z(0, 1)
    wait("near", zrecv.at[pl.ds(0, 4)])
    gate_up(zrecv, hz, 0, 5)
    got_rows(2)
    gate_up(zrecv, hz, 14, 3)
    down_z(1, 0)
    down_z(1, 1)
    for c in range(2, len(PARTS)):
        down_z(0, c)
        down_z(1, c)
    down_near()
    down_own(0)
    down_own(1)

    def expand(c):
        cols = chunk_cols(c)
        left, right = sides(c)
        if c >= 2:
            down_own(c)
        wait(f"back{c}", zrecv.at[pl.ds(0, 11), :, cols])

        def fill(dx, dy):
            place = PLACE[dx, dy]
            rows = most if place < 5 else 2 * most
            part[dx, dy, :, cols] = jnp.dot(
                comb[place, :, :rows], both[place // 2, place % 2, :rows, cols], preferred_element_type=F32
            ).astype(BF16)

        far = [slot for slot in PLACE if 2 in slot]
        for slot in far:
            fill(*slot)
        send("yp", part.at[:, 2, top, left], r1p.at[:, :, left], "1p", f"1{c}")
        send("ym", part.at[:, 2, low, left], r1m.at[:, :, left], "1m", f"1{c}")
        send("xp", part.at[2, :, top, right], r1p.at[:, :, right], "1p", f"1{c}")
        send("xm", part.at[2, :, low, right], r1m.at[:, :, right], "1m", f"1{c}")
        for slot in PLACE:
            if slot not in far:
                fill(*slot)
        halves_two(c, low, top)

    def halves_two(c, plus, minus):
        left, right = sides(c)
        send("yp", part.at[:, 1, plus, left], r2p.at[:, plus, left], "2p", f"2{c}")
        send("ym", part.at[:, 3, minus, left], r2m.at[:, minus, left], "2m", f"2{c}")
        send("xp", part.at[1, :, plus, right], r2p.at[:, plus, right], "2p", f"2{c}")
        send("xm", part.at[3, :, minus, right], r2m.at[:, minus, right], "2m", f"2{c}")

    def halves_five(c, plus, minus):
        left, right = sides(c)
        send("xp", part.at[1, 0, plus, left], r5p.at[plus, left], "5p", f"5{c}")
        send("xm", part.at[3, 0, minus, left], r5m.at[minus, left], "5m", f"5{c}")
        send("yp", part.at[0, 1, plus, right], r5p.at[plus, right], "5p", f"5{c}")
        send("ym", part.at[0, 3, minus, right], r5m.at[minus, right], "5m", f"5{c}")

    def double(c):
        return pl.ds(0, 2 * chunk_cols(c).size)

    def add(dx, dy, rows, cols, *refs):
        total = part[dx, dy, rows, cols].astype(F32)
        for ref in refs:
            total = total + ref[...].astype(F32)
        part[dx, dy, rows, cols] = total.astype(BF16)

    every = pl.ds(0, tok)

    def step_two(c):
        left, right = sides(c)
        wait(f"1{c}", r1p.at[:, :, double(c)])
        for d in range(4):
            add(d, 1, top, left, r1p.at[d, :, left])
            add(d, 3, low, left, r1m.at[d, :, left])
            add(1, d, top, right, r1p.at[d, :, right])
            add(3, d, low, right, r1m.at[d, :, right])
        halves_two(c, top, low)

    def step_three(c):
        left, right = sides(c)
        wait(f"2{c}", r2p.at[:, :, double(c)])
        for d in (2, 1, 3, 0):
            add(d, 0, every, left, r2p.at[d, :, left], r2m.at[d, :, left])
            add(0, d, every, right, r2p.at[d, :, right], r2m.at[d, :, right])
            if d == 2:
                send("xp", part.at[2, 0, top, left], r4p.at[:, left], "4p", f"4{c}")
                send("xm", part.at[2, 0, low, left], r4m.at[:, left], "4m", f"4{c}")
                send("yp", part.at[0, 2, top, right], r4p.at[:, right], "4p", f"4{c}")
                send("ym", part.at[0, 2, low, right], r4m.at[:, right], "4m", f"4{c}")
            if d == 3:
                halves_five(c, low, top)

    def step_four(c):
        left, right = sides(c)
        wait(f"4{c}", r4p.at[:, double(c)])
        add(1, 0, top, left, r4p.at[:, left])
        add(3, 0, low, left, r4m.at[:, left])
        add(0, 1, top, right, r4p.at[:, right])
        add(0, 3, low, right, r4m.at[:, right])
        halves_five(c, top, low)

    stores = []

    def step_five(c):
        wait(f"5{c}", r5p.at[:, double(c)])
        if c == 0:
            wait("sum", zsum)
        for cols in sides(c):
            total = part[0, 0, :, cols].astype(F32) + zsum[:, cols].astype(F32) + r5p[:, cols].astype(F32) + r5m[:, cols].astype(F32)
            outv[:, cols] = total.astype(BF16)
        cols = chunk_cols(c)
        store = pltpu.make_async_copy(outv.at[:, cols], out_hbm.at[:, cols], local_sem.at[4 + c])
        store.start()
        stores.append(store)

    run = {"E": expand, "A": step_two, "B": step_three, "C": step_four, "D": step_five, "F": lambda c: sum_near()}
    for step in STEPS:
        run[step[0]](int(step[1]))
    assert len(sems) <= MAX_SEMS
    drain("own", gath.at[0])
    drain("pass", gath.at[0])
    drain("second", gath.at[0, 0:3])
    drain("relay", gath.at[0])
    drain("m12", meta.at[0:3])
    drain("m3", meta.at[0, 0:3])
    drain("rows", zsend.at[pl.ds(0, 11)])
    drain("back", zsend.at[pl.ds(0, 11)])
    drain("near", frecv)
    drain("nearback", frecv)
    drain("whole", fgath)
    drain("mwhole", fmeta)
    drain("sum", fsum)
    for kind, like in (("1p", r1p), ("1m", r1m), ("2p", r2p), ("2m", r2m), ("4p", r4p), ("4m", r4m), ("5p", r5p), ("5m", r5m)):
        drain(kind, like)
    for store in stores:
        store.wait()


def shards(n_hi, tokens, expert_ids, gate_probs, w_gate, w_up, w_down):
    tok, width = tokens.shape
    hid = w_gate.shape[2]
    most = 32
    vmem = pl.BlockSpec(memory_space=pltpu.VMEM)
    hbm = pl.BlockSpec(memory_space=pl.ANY)
    return pl.pallas_call(
        functools.partial(kernel, (n_hi, tok, width, hid, most)),
        out_shape=jax.ShapeDtypeStruct((tok, width), BF16),
        in_specs=[hbm, vmem, vmem, hbm, hbm, hbm],
        out_specs=hbm,
        scratch_shapes=[
            pltpu.VMEM((4, 4, tok, width), BF16),
            pltpu.VMEM((4, 4, 16, 128), F32),
            pltpu.VMEM((PLACES, tok, 2 * most), BF16),
            pltpu.VMEM((PLACES, most, width), BF16),
            pltpu.VMEM((PLACES, most, width), BF16),
            pltpu.VMEM((PLACES, most, width), BF16),
            pltpu.VMEM((PLACES * most, hid), BF16),
            pltpu.VMEM((PLACES * most, hid), BF16),
            pltpu.VMEM((width, hid), BF16),
            pltpu.VMEM((width, hid), BF16),
            pltpu.VMEM((hid, width), BF16),
            pltpu.VMEM((PLACES // 2, 2, most, width), BF16),
            pltpu.VMEM((PLACES // 2, 2, 2 * most, width), BF16),
            pltpu.VMEM((4, 4, tok, width), BF16),
            pltpu.VMEM((PLACES, 2 * most, tok), BF16),
            pltpu.VMEM((tok, width), BF16),
            pltpu.VMEM((16, 128), F32),
            pltpu.VMEM((5, tok, most), BF16),
            pltpu.VMEM((5 * most, tok), BF16),
            pltpu.VMEM((4, most, width), BF16),
            pltpu.VMEM((4, most, width), BF16),
            pltpu.VMEM((tok, width), BF16),
            pltpu.VMEM((tok, width), BF16),
            pltpu.VMEM((4, tok // 2, width), BF16),
            pltpu.VMEM((4, tok // 2, width), BF16),
            pltpu.VMEM((4, tok, width), BF16),
            pltpu.VMEM((4, tok, width), BF16),
            pltpu.VMEM((tok // 2, width), BF16),
            pltpu.VMEM((tok // 2, width), BF16),
            pltpu.VMEM((tok, width), BF16),
            pltpu.VMEM((tok, width), BF16),
            pltpu.VMEM((tok, width), BF16),
            pltpu.SemaphoreType.DMA((MAX_SEMS,)),
            pltpu.SemaphoreType.DMA((MAX_SEMS,)),
            pltpu.SemaphoreType.DMA((4 + len(PARTS),)),
        ],
        compiler_params=pltpu.CompilerParams(
            collective_id=0, has_side_effects=True, vmem_limit_bytes=60 * 1024 * 1024
        ),
        name="routed_experts",
    )(tokens, expert_ids.T, gate_probs.T, w_gate, w_up, w_down)


def solution(mesh):
    placed = (
        P(("dp", "ep"), None),
        P(("dp", "ep"), None),
        P(("dp", "ep"), None),
        P("ep", None, None),
        P("ep", None, None),
        P("ep", None, None),
    )
    return jax.shard_map(
        functools.partial(shards, mesh.shape["dp"] // 2), mesh=mesh, in_specs=placed,
        out_specs=P(("dp", "ep"), None), check_vma=False,
    )
```

```python
import functools

import jax
import jax.numpy as jnp
from jax import lax
from jax.experimental import pallas as pl
from jax.experimental.pallas import tpu as pltpu
from jax.sharding import PartitionSpec as P

MESH = pl.DeviceIdType.MESH
F32, BF16 = jnp.float32, jnp.bfloat16
OPPOSITE = {"xp": "xm", "xm": "xp", "yp": "ym", "ym": "yp", "zp": "zm", "zm": "zp"}

CLUSTER = [(0, 0), (1, 0), (3, 0), (0, 1), (0, 3)]
OTHERS = [(1, 1), (3, 3), (1, 3), (3, 1), (0, 2), (2, 0), (1, 2), (2, 1), (3, 2), (2, 3), (2, 2)]
PLACE = {slot: place for place, slot in enumerate(CLUSTER + [None] + OTHERS) if slot}
PLACES = 18
NEAR = {1: "xp", 2: "xm", 3: "yp", 4: "ym"}
PARTS = (1, 1, 2, 2, 1, 1)
STEPS = (
    "G0", "G1", "Z0", "W1", "G2", "F0", "W2", "E0", "G3", "E1", "E2", "A0", "W3", "G4", "E3", "A1", "A2", "G5", "B0", "E4", "E5",
    "A3", "B1", "B2", "C0", "A4", "A5", "B3", "C1", "C2", "D0", "B4", "B5", "C3", "D1", "D2", "C4", "C5", "D3", "D4", "D5",
)
MAX_SEMS = 96


def kernel(
    sizes, tok_hbm, ids_ref, probs_ref, wg_hbm, wu_hbm, wd_hbm, out_hbm,
    gath, meta, comb, xown, zsend, zrecv, hown, hz, wg, wu, wd, zout, both, part, picks,
    fgath, fmeta, fcomb, fpick, fsend, frecv, fsum, zsum,
    r1p, r1m, r2p, r2m, r4p, r4m, r5p, r5m, outv,
    send_sem, recv_sem, local_sem,
):
    n_hi, tok, width, hid, most = sizes
    half, quarter = width // 2, width // 4
    ep, dp = lax.axis_index("ep"), lax.axis_index("dp")
    x, y, z_lo = lax.rem(ep, 4), lax.rem(ep // 4, 4), ep // 16
    z_hi, core = dp // 2, lax.rem(dp, 2)

    def at(xx, yy, zz):
        return zz * 16 + yy * 4 + xx

    cross = 1 - core
    here = z_hi * 2 + cross
    z_up = lax.rem(z_hi + z_lo, n_hi) * 2 + cross
    z_down = lax.rem(z_hi + z_lo + n_hi - 1, n_hi) * 2 + cross
    target = {
        "xp": {"ep": at(lax.rem(x + 1, 4), y, z_lo), "dp": here},
        "xm": {"ep": at(lax.rem(x + 3, 4), y, z_lo), "dp": here},
        "yp": {"ep": at(x, lax.rem(y + 1, 4), z_lo), "dp": here},
        "ym": {"ep": at(x, lax.rem(y + 3, 4), z_lo), "dp": here},
        "zp": {"ep": at(x, y, 1 - z_lo), "dp": z_up},
        "zm": {"ep": at(x, y, 1 - z_lo), "dp": z_down},
    }
    other = at(x, y, 1 - z_lo)

    sems = {}

    def sem(array, kind):
        return array.at[sems.setdefault(kind, len(sems))]

    def send(way, src, dst, leaves, lands):
        pltpu.make_async_remote_copy(
            src_ref=src, dst_ref=dst, send_sem=sem(send_sem, leaves), recv_sem=sem(recv_sem, lands),
            device_id=target[way], device_id_type=MESH,
        ).start()

    def wait(lands, *like):
        pltpu.make_async_copy(*like, *like, sem(recv_sem, lands)).wait()

    def drain(leaves, like):
        pltpu.make_async_copy(like, like, sem(send_sem, leaves)).wait()

    load_tok = pltpu.make_async_copy(tok_hbm, gath.at[0, 0], local_sem.at[0])
    load_tok.start()
    loads = [
        pltpu.make_async_copy(src.at[0], dst, local_sem.at[1 + i])
        for i, (src, dst) in enumerate(((wg_hbm, wg), (wu_hbm, wu), (wd_hbm, wd)))
    ]
    for load in loads:
        load.start()

    barrier = pltpu.get_barrier_semaphore()
    for way in target:
        pl.semaphore_signal(barrier, inc=1, device_id=target[way], device_id_type=MESH)

    ids = ids_ref[...].astype(F32)
    probs = probs_ref[...]
    weights = probs / jnp.sum(probs, axis=0, keepdims=True)
    experts = lax.broadcasted_iota(jnp.int32, (32, tok), 0).astype(F32)
    named = jnp.zeros((32, tok), F32)
    for k in range(8):
        named = named + jnp.where(ids[k:k + 1, :] == experts, 1.0, 0.0)
    before = lax.broadcasted_iota(jnp.int32, (tok, tok), 0) < lax.broadcasted_iota(jnp.int32, (tok, tok), 1)
    ranks = jnp.dot(named.astype(BF16), before.astype(F32).astype(BF16), preferred_element_type=F32)
    for k in range(8):
        rank = jnp.sum(jnp.where(ids[k:k + 1, :] == experts, ranks, 0.0), axis=0, keepdims=True)
        meta[0, 0, k:k + 1, 0:tok] = ids[k:k + 1, :] * float(most) + rank
    meta[0, 0, 8:16, 0:tok] = weights

    pl.semaphore_wait(barrier, 6)
    load_tok.wait()

    first, second = pl.ds(0, half), pl.ds(half, half)
    quarters = [pl.ds(q * quarter, quarter) for q in range(4)]

    def move(kind, leaves, way, slot, cols, with_meta=None):
        dx, dy = slot
        shift = {"xp": (3, 0), "xm": (1, 0), "yp": (0, 3), "ym": (0, 1)}[way]
        to = ((dx + shift[0]) % 4, (dy + shift[1]) % 4)
        send(way, gath.at[dx, dy, :, cols], gath.at[to[0], to[1], :, cols], leaves, kind)
        if with_meta:
            send(way, meta.at[dx, dy], meta.at[to[0], to[1]], with_meta, "m" + kind)

    def own_first():
        for way in ("xp", "xm"):
            move("own", "own", way, (0, 0), first, "m12")
        for way in ("yp", "ym"):
            move("own", "own", way, (0, 0), second, "m3")

    def own_second():
        for way in ("yp", "ym"):
            move("pass0", "own", way, (0, 0), first)
        for way in ("xp", "xm"):
            move("pass0", "own", way, (0, 0), second)

    def own_relay():
        move("far", "pass", "xp", (3, 0), quarters[0], "m12")
        move("far", "pass", "xm", (1, 0), quarters[1])
        move("far", "pass", "yp", (0, 3), quarters[2], "m3")
        move("far", "pass", "ym", (0, 1), quarters[3])

    def passes(d):
        e = (4 - d) % 4
        move(f"pass{d}", "pass", "ym", (d, 0), first, "m12")
        move(f"pass{d}", "second", "xm", (0, d), second)
        move(f"pass{d}", "pass", "yp", (e, 0), first, "m12")
        move(f"pass{d}", "second", "xp", (0, e), second)

    def relays(d):
        move(f"relay{d}", "relay", "yp", (d, 3), quarters[0], "m12" if d else None)
        move(f"relay{d}", "relay", "ym", (d, 1), quarters[1])
        move(f"relay{d}", "relay", "xp", (3, d), quarters[2])
        move(f"relay{d}", "relay", "xm", (1, d), quarters[3])

    def got_own():
        wait("own", gath.at[0, 0:2])
        wait("mown", meta.at[0])

    def got_far():
        wait("far", gath.at[0, 0])
        wait("mfar", meta.at[0, 0:2])

    def got_passes(d):
        wait(f"pass{d}", gath.at[0, 0:2])
        if d:
            wait(f"mpass{d}", meta.at[0, 0:2])

    def got_relays(d):
        wait(f"relay{d}", gath.at[0, 0])
        if d:
            wait(f"mrelay{d}", meta.at[0, 0])

    place_row = lax.broadcasted_iota(jnp.int32, (2 * most, tok), 0)
    wanted = jnp.where(place_row < most, ep * most + place_row, (other - 1) * most + place_row).astype(F32)

    def build(dx, dy):
        place = PLACE[dx, dy]
        one, scaled = jnp.zeros((2 * most, tok), F32), jnp.zeros((2 * most, tok), F32)
        for k in range(8):
            hit = meta[dx, dy, k:k + 1, 0:tok] == wanted
            one = one + jnp.where(hit, 1.0, 0.0)
            scaled = scaled + jnp.where(hit, meta[dx, dy, 8 + k:9 + k, 0:tok], 0.0)
        comb[place] = scaled.T.astype(BF16)
        picks[place] = one.astype(BF16)

    def select(dx, dy):
        place = PLACE[dx, dy]
        rows = most if place < 5 else 2 * most

        @pl.loop(0, 4)
        def _(q):
            cols = pl.ds(pl.multiple_of(q * quarter, quarter), quarter)
            chosen = jnp.dot(picks[place, :rows], gath[dx, dy, :, cols], preferred_element_type=F32).astype(BF16)
            xown[place, :, cols] = chosen[:most]
            if place >= 5:
                zsend[place, :, cols] = chosen[most:]

        if place >= 5:
            group = min((place - 6) // 4, 2)
            send("zm" if place % 2 else "zp", zsend.at[place], zrecv.at[place], "rows", f"rows{group}")

    def select_all(*slots):
        for slot in slots:
            build(*slot)
            select(*slot)

    def got_rows(group):
        wait(f"rows{group}", zrecv.at[pl.ds(0, (4, 4, 3)[group])])

    near_experts = (ep, at(lax.rem(x + 1, 4), y, z_lo), at(lax.rem(x + 3, 4), y, z_lo), at(x, lax.rem(y + 1, 4), z_lo), at(x, lax.rem(y + 3, 4), z_lo))

    def select_foreign():
        for i, expert in enumerate(near_experts):
            row = (expert * most + lax.broadcasted_iota(jnp.int32, (most, tok), 0)).astype(F32)
            one, scaled = jnp.zeros((most, tok), F32), jnp.zeros((most, tok), F32)
            for k in range(8):
                hit = fmeta[k:k + 1, 0:tok] == row
                one = one + jnp.where(hit, 1.0, 0.0)
                scaled = scaled + jnp.where(hit, fmeta[8 + k:9 + k, 0:tok], 0.0)
            fcomb[i] = scaled.T.astype(BF16)
            fpick[i * most:(i + 1) * most, :] = one.astype(BF16)

        @pl.loop(0, 4)
        def _(q):
            cols = pl.ds(pl.multiple_of(q * quarter, quarter), quarter)
            chosen = jnp.dot(fpick[...], fgath[:, cols], preferred_element_type=F32).astype(BF16)
            zrecv[0, :, cols] = chosen[:most]
            for i in range(4):
                fsend[i, :, cols] = chosen[(i + 1) * most:(i + 2) * most]

    def send_near():
        for i, (way, slot) in enumerate((("xp", (3, 0)), ("xm", (1, 0)), ("yp", (0, 3)), ("ym", (0, 1)))):
            send(way, fsend.at[i], zrecv.at[PLACE[slot]], "near", "near")

    def back_near():
        for place, way in NEAR.items():
            index = ("xm", "xp", "ym", "yp").index(way)
            send(way, zout.at[place // 2, place % 2], frecv.at[index], "nearback", "nearback")

    def sum_near():
        wait("nearback", frecv)

        @pl.loop(0, 4)
        def _(q):
            cols = pl.ds(pl.multiple_of(q * quarter, quarter), quarter)
            total = jnp.dot(fcomb[0], zout[0, 0, :, cols], preferred_element_type=F32)
            for i in range(4):
                total = total + jnp.dot(fcomb[i + 1], frecv[i, :, cols], preferred_element_type=F32)
            fsum[:, cols] = total.astype(BF16)

        send("zp", fsum, zsum, "sum", "sum")

    tile = 256

    def gate_up(rows_ref, hidden, place, places, start=0, stop=hid // tile):
        rows = places * most

        @pl.loop(start, stop)
        def _(n):
            cols = pl.ds(pl.multiple_of(n * tile, tile), tile)
            block = rows_ref[place:place + places].reshape(rows, width)
            gate = jnp.dot(block, wg[:, cols], preferred_element_type=F32)
            up = jnp.dot(block, wu[:, cols], preferred_element_type=F32)
            hidden[place * most:place * most + rows, cols] = (gate / (1.0 + jnp.exp(-gate)) * up).astype(BF16)

    own_first()
    own_second()
    send("zm", gath.at[0, 0], fgath, "whole", "whole")
    send("zm", meta.at[0, 0], fmeta, "mwhole", "mwhole")
    select_all((0, 0))
    got_own()
    passes(1)
    own_relay()
    passes(3)
    for slot in CLUSTER[1:]:
        build(*slot)
    got_passes(0)
    relays(0)
    for slot in CLUSTER[1:]:
        select(*slot)
    wait("whole", fgath)
    wait("mwhole", fmeta)
    select_foreign()
    loads[0].wait()
    loads[1].wait()
    gate_up(xown, hown, 0, 5, 0, 2)
    got_passes(1)
    select_all((1, 1), (3, 3))
    got_far()
    passes(2)
    gate_up(xown, hown, 0, 5, 2, 3)
    got_passes(3)
    relays(1)
    relays(3)
    select_all((1, 3), (3, 1))
    got_relays(0)
    select_all((0, 2), (2, 0))
    gate_up(xown, hown, 6, 6, 0, 1)
    got_passes(2)
    relays(2)
    send_near()
    gate_up(xown, hown, 6, 6, 1, 3)
    got_relays(1)
    select_all((1, 2), (2, 1))
    got_relays(3)
    select_all((3, 2), (2, 3))
    got_relays(2)
    select_all((2, 2))

    starts = [sum(PARTS[:c]) * width // sum(PARTS) for c in range(len(PARTS) + 1)]

    def chunk_cols(c):
        return pl.ds(starts[c], starts[c + 1] - starts[c])

    def sides(c):
        middle = (starts[c] + starts[c + 1]) // 2
        return pl.ds(starts[c], middle - starts[c]), pl.ds(middle, starts[c + 1] - middle)

    top, low = pl.ds(0, tok // 2), pl.ds(tok // 2, tok // 2)

    def quarter_chunks(q):
        return [c for c in range(len(PARTS)) if q * quarter <= starts[c] < (q + 1) * quarter]

    def down_z(part_of, q):
        place, places = ((6, 8), (14, 3))[part_of]
        rows = hz[most * place:most * (place + places), :]
        out = jnp.dot(rows, wd[:, quarters[q]], preferred_element_type=F32).astype(BF16)
        for i in range(places):
            zout[(place + i) // 2, (place + i) % 2, :, quarters[q]] = out[most * i:most * (i + 1)]
        for c in quarter_chunks(q):
            for side, way in ((0, "zm"), (1, "zp")):
                pairs = pl.ds(place // 2, (places + 1 - side) // 2)
                send(
                    way,
                    zout.at[pairs, side, :, chunk_cols(c)],
                    both.at[pairs, side, pl.ds(most, most), chunk_cols(c)],
                    "back", f"back{part_of}{c}",
                )

    def down_near():
        @pl.loop(0, 4)
        def _(q):
            cols = pl.ds(pl.multiple_of(q * quarter, quarter), quarter)
            out = jnp.dot(hz[0:5 * most, :], wd[:, cols], preferred_element_type=F32).astype(BF16)
            for i in range(5):
                zout[i // 2, i % 2, :, cols] = out[most * i:most * (i + 1)]

        back_near()

    def down_own(q):
        out = jnp.dot(hown[...], wd[:, quarters[q]], preferred_element_type=F32).astype(BF16)
        for place in PLACE.values():
            both[place // 2, place % 2, 0:most, quarters[q]] = out[most * place:most * (place + 1)]

    gate_up(xown, hown, 12, 5)
    got_rows(0)
    got_rows(1)
    gate_up(zrecv, hz, 6, 8)
    loads[2].wait()
    down_z(0, 0)
    down_z(0, 1)
    down_z(0, 2)
    wait("near", zrecv.at[pl.ds(0, 4)])
    gate_up(zrecv, hz, 0, 5)
    down_near()
    got_rows(2)
    gate_up(zrecv, hz, 14, 3)
    down_z(1, 0)
    down_z(1, 1)
    down_own(0)

    def down_rest(c):
        down_z(0, 3)
        down_z(1, 2)
        down_z(1, 3)

    def fill(c, *slots):
        cols = chunk_cols(c)
        for dx, dy in slots:
            place = PLACE[dx, dy]
            rows = most if place < 5 else 2 * most
            part[dx, dy, :, cols] = jnp.dot(
                comb[place, :, :rows], both[place // 2, place % 2, :rows, cols], preferred_element_type=F32
            ).astype(BF16)

    late = ((3, 2), (2, 3), (2, 2))

    def halves_one(c, pair):
        left, right = sides(c)
        send("yp", part.at[pair, 2, top, left], r1p.at[pair, :, left], "1p", f"1{c}")
        send("ym", part.at[pair, 2, low, left], r1m.at[pair, :, left], "1m", f"1{c}")
        send("xp", part.at[2, pair, top, right], r1p.at[pair, :, right], "1p", f"1{c}")
        send("xm", part.at[2, pair, low, right], r1m.at[pair, :, right], "1m", f"1{c}")

    def expand(c):
        left, right = sides(c)
        wait(f"back0{c}", zrecv.at[pl.ds(0, 8), :, chunk_cols(c)])
        fill(c, (0, 2), (1, 2), (2, 0), (2, 1))
        halves_one(c, pl.ds(0, 2))
        fill(c, *[slot for slot in PLACE if 2 not in slot])
        send("yp", part.at[:, 1, low, left], r2p.at[:, low, left], "2p", f"2{c}")
        send("xp", part.at[1, :, low, right], r2p.at[:, low, right], "2p", f"2{c}")
        send("ym", part.at[pl.ds(0, 2), 3, top, left], r2m.at[pl.ds(0, 2), top, left], "2m", f"2{c}")
        send("xm", part.at[3, pl.ds(0, 2), top, right], r2m.at[pl.ds(0, 2), top, right], "2m", f"2{c}")

    def expand_late(c):
        left, right = sides(c)
        wait(f"back1{c}", zrecv.at[pl.ds(0, 3), :, chunk_cols(c)])
        fill(c, *late)
        halves_one(c, pl.ds(2, 2))
        send("ym", part.at[pl.ds(2, 2), 3, top, left], r2m.at[pl.ds(2, 2), top, left], "2m", f"2{c}")
        send("xm", part.at[3, pl.ds(2, 2), top, right], r2m.at[pl.ds(2, 2), top, right], "2m", f"2{c}")

    def halves_two(c, plus, minus):
        left, right = sides(c)
        send("yp", part.at[:, 1, plus, left], r2p.at[:, plus, left], "2p", f"2{c}")
        send("ym", part.at[:, 3, minus, left], r2m.at[:, minus, left], "2m", f"2{c}")
        send("xp", part.at[1, :, plus, right], r2p.at[:, plus, right], "2p", f"2{c}")
        send("xm", part.at[3, :, minus, right], r2m.at[:, minus, right], "2m", f"2{c}")

    def halves_five(c, plus, minus):
        left, right = sides(c)
        send("xp", part.at[1, 0, plus, left], r5p.at[plus, left], "5p", f"5{c}")
        send("xm", part.at[3, 0, minus, left], r5m.at[minus, left], "5m", f"5{c}")
        send("yp", part.at[0, 1, plus, right], r5p.at[plus, right], "5p", f"5{c}")
        send("ym", part.at[0, 3, minus, right], r5m.at[minus, right], "5m", f"5{c}")

    def double(c):
        return pl.ds(0, 2 * chunk_cols(c).size)

    def add(dx, dy, rows, cols, *refs):
        total = part[dx, dy, rows, cols].astype(F32)
        for ref in refs:
            total = total + ref[...].astype(F32)
        part[dx, dy, rows, cols] = total.astype(BF16)

    every = pl.ds(0, tok)

    def step_two(c):
        left, right = sides(c)
        wait(f"1{c}", r1p.at[:, :, double(c)])
        for d in range(4):
            add(d, 1, top, left, r1p.at[d, :, left])
            add(d, 3, low, left, r1m.at[d, :, left])
            add(1, d, top, right, r1p.at[d, :, right])
            add(3, d, low, right, r1m.at[d, :, right])
        halves_two(c, top, low)

    def step_three(c):
        left, right = sides(c)
        wait(f"2{c}", r2p.at[:, :, double(c)])
        for d in (2, 1, 3, 0):
            add(d, 0, every, left, r2p.at[d, :, left], r2m.at[d, :, left])
            add(0, d, every, right, r2p.at[d, :, right], r2m.at[d, :, right])
            if d == 2:
                send("xp", part.at[2, 0, top, left], r4p.at[:, left], "4p", f"4{c}")
                send("xm", part.at[2, 0, low, left], r4m.at[:, left], "4m", f"4{c}")
                send("yp", part.at[0, 2, top, right], r4p.at[:, right], "4p", f"4{c}")
                send("ym", part.at[0, 2, low, right], r4m.at[:, right], "4m", f"4{c}")
            if d == 3:
                halves_five(c, low, top)

    def step_four(c):
        left, right = sides(c)
        wait(f"4{c}", r4p.at[:, double(c)])
        add(1, 0, top, left, r4p.at[:, left])
        add(3, 0, low, left, r4m.at[:, left])
        add(0, 1, top, right, r4p.at[:, right])
        add(0, 3, low, right, r4m.at[:, right])
        halves_five(c, top, low)

    stores = []

    def step_five(c):
        wait(f"5{c}", r5p.at[:, double(c)])
        if c == 0:
            wait("sum", zsum)
        for cols in sides(c):
            total = part[0, 0, :, cols].astype(F32) + zsum[:, cols].astype(F32) + r5p[:, cols].astype(F32) + r5m[:, cols].astype(F32)
            outv[:, cols] = total.astype(BF16)
        cols = chunk_cols(c)
        store = pltpu.make_async_copy(outv.at[:, cols], out_hbm.at[:, cols], local_sem.at[4 + c])
        store.start()
        stores.append(store)

    run = {"G": expand, "E": expand_late, "Z": down_rest, "W": down_own, "A": step_two, "B": step_three, "C": step_four, "D": step_five, "F": lambda c: sum_near()}
    for step in STEPS:
        run[step[0]](int(step[1]))
    assert len(sems) <= MAX_SEMS
    drain("own", gath.at[0])
    drain("pass", gath.at[0])
    drain("second", gath.at[0, 0:3])
    drain("relay", gath.at[0])
    drain("m12", meta.at[0:3])
    drain("m3", meta.at[0, 0:3])
    drain("rows", zsend.at[pl.ds(0, 11)])
    drain("back", zsend.at[pl.ds(0, 11)])
    drain("near", frecv)
    drain("nearback", frecv)
    drain("whole", fgath)
    drain("mwhole", fmeta)
    drain("sum", fsum)
    for kind, like in (("1p", r1p), ("1m", r1m), ("2p", r2p), ("2m", r2m), ("4p", r4p), ("4m", r4m), ("5p", r5p), ("5m", r5m)):
        drain(kind, like)
    for store in stores:
        store.wait()


def shards(n_hi, tokens, expert_ids, gate_probs, w_gate, w_up, w_down):
    tok, width = tokens.shape
    hid = w_gate.shape[2]
    most = 32
    vmem = pl.BlockSpec(memory_space=pltpu.VMEM)
    hbm = pl.BlockSpec(memory_space=pl.ANY)
    return pl.pallas_call(
        functools.partial(kernel, (n_hi, tok, width, hid, most)),
        out_shape=jax.ShapeDtypeStruct((tok, width), BF16),
        in_specs=[hbm, vmem, vmem, hbm, hbm, hbm],
        out_specs=hbm,
        scratch_shapes=[
            pltpu.VMEM((4, 4, tok, width), BF16),
            pltpu.VMEM((4, 4, 16, 128), F32),
            pltpu.VMEM((PLACES, tok, 2 * most), BF16),
            pltpu.VMEM((PLACES, most, width), BF16),
            pltpu.VMEM((PLACES, most, width), BF16),
            pltpu.VMEM((PLACES, most, width), BF16),
            pltpu.VMEM((PLACES * most, hid), BF16),
            pltpu.VMEM((PLACES * most, hid), BF16),
            pltpu.VMEM((width, hid), BF16),
            pltpu.VMEM((width, hid), BF16),
            pltpu.VMEM((hid, width), BF16),
            pltpu.VMEM((PLACES // 2, 2, most, width), BF16),
            pltpu.VMEM((PLACES // 2, 2, 2 * most, width), BF16),
            pltpu.VMEM((4, 4, tok, width), BF16),
            pltpu.VMEM((PLACES, 2 * most, tok), BF16),
            pltpu.VMEM((tok, width), BF16),
            pltpu.VMEM((16, 128), F32),
            pltpu.VMEM((5, tok, most), BF16),
            pltpu.VMEM((5 * most, tok), BF16),
            pltpu.VMEM((4, most, width), BF16),
            pltpu.VMEM((4, most, width), BF16),
            pltpu.VMEM((tok, width), BF16),
            pltpu.VMEM((tok, width), BF16),
            pltpu.VMEM((4, tok // 2, width), BF16),
            pltpu.VMEM((4, tok // 2, width), BF16),
            pltpu.VMEM((4, tok, width), BF16),
            pltpu.VMEM((4, tok, width), BF16),
            pltpu.VMEM((tok // 2, width), BF16),
            pltpu.VMEM((tok // 2, width), BF16),
            pltpu.VMEM((tok, width), BF16),
            pltpu.VMEM((tok, width), BF16),
            pltpu.VMEM((tok, width), BF16),
            pltpu.SemaphoreType.DMA((MAX_SEMS,)),
            pltpu.SemaphoreType.DMA((MAX_SEMS,)),
            pltpu.SemaphoreType.DMA((4 + len(PARTS),)),
        ],
        compiler_params=pltpu.CompilerParams(
            collective_id=0, has_side_effects=True, vmem_limit_bytes=60 * 1024 * 1024
        ),
        name="routed_experts",
    )(tokens, expert_ids.T, gate_probs.T, w_gate, w_up, w_down)


def solution(mesh):
    placed = (
        P(("dp", "ep"), None),
        P(("dp", "ep"), None),
        P(("dp", "ep"), None),
        P("ep", None, None),
        P("ep", None, None),
        P("ep", None, None),
    )
    return jax.shard_map(
        functools.partial(shards, mesh.shape["dp"] // 2), mesh=mesh, in_specs=placed,
        out_specs=P(("dp", "ep"), None), check_vma=False,
    )
```

```python
import functools

import jax
import jax.numpy as jnp
from jax import lax
from jax.experimental import pallas as pl
from jax.experimental.pallas import tpu as pltpu
from jax.sharding import PartitionSpec as P

MESH = pl.DeviceIdType.MESH
F32, BF16 = jnp.float32, jnp.bfloat16
OPPOSITE = {"xp": "xm", "xm": "xp", "yp": "ym", "ym": "yp", "zp": "zm", "zm": "zp"}

CLUSTER = [(0, 0), (1, 0), (3, 0), (0, 1), (0, 3)]
OTHERS = [(1, 1), (3, 3), (1, 3), (3, 1), (0, 2), (2, 0), (1, 2), (2, 1), (3, 2), (2, 3), (2, 2)]
PLACE = {slot: place for place, slot in enumerate(CLUSTER + [None] + OTHERS) if slot}
PLACES = 18
NEAR = {1: "xp", 2: "xm", 3: "yp", 4: "ym"}
PARTS = (1,) * 8
STEPS = (
    "O3", "W2", "Z", "a2", "a3", "N", "L", "DN", "b2", "G4", "b3", "W3", "G5", "W0", "a0", "b0", "W1", "G6", "E4",
    "E5", "a1", "G7", "E7", "b1", "E6", "G0", "A4", "A5", "E0", "G1", "F", "E1", "B4", "G2", "G3", "E2", "E3", "A7",
    "A0", "A6", "A2", "A3", "A1", "C4", "B7", "B5", "B6", "B2", "B0", "B3", "B1", "D4", "C5", "C6", "C7", "C2", "C0",
    "C3", "C1", "D5", "D7", "D3", "D6", "D2", "D0", "D1",
)
MAX_SEMS = 128


def kernel(
    sizes, tok_hbm, ids_ref, probs_ref, wg_hbm, wu_hbm, wd_hbm, out_hbm,
    gath, meta, comb, xown, zsend, zrecv, hown, hz, wg, wu, wd, zout, both, part, picks,
    fgath, fmeta, fcomb, fpick, fsend, frecv, fsum, zsum,
    r1p, r1m, r2p, r2m, r4p, r4m, r5p, r5m, outv,
    send_sem, recv_sem, local_sem,
):
    n_hi, tok, width, hid, most = sizes
    half, quarter = width // 2, width // 4
    ep, dp = lax.axis_index("ep"), lax.axis_index("dp")
    x, y, z_lo = lax.rem(ep, 4), lax.rem(ep // 4, 4), ep // 16
    z_hi, core = dp // 2, lax.rem(dp, 2)

    def at(xx, yy, zz):
        return zz * 16 + yy * 4 + xx

    cross = 1 - core
    here = z_hi * 2 + cross
    z_up = lax.rem(z_hi + z_lo, n_hi) * 2 + cross
    z_down = lax.rem(z_hi + z_lo + n_hi - 1, n_hi) * 2 + cross
    target = {
        "xp": {"ep": at(lax.rem(x + 1, 4), y, z_lo), "dp": here},
        "xm": {"ep": at(lax.rem(x + 3, 4), y, z_lo), "dp": here},
        "yp": {"ep": at(x, lax.rem(y + 1, 4), z_lo), "dp": here},
        "ym": {"ep": at(x, lax.rem(y + 3, 4), z_lo), "dp": here},
        "zp": {"ep": at(x, y, 1 - z_lo), "dp": z_up},
        "zm": {"ep": at(x, y, 1 - z_lo), "dp": z_down},
    }
    other = at(x, y, 1 - z_lo)

    sems = {}

    def sem(array, kind):
        return array.at[sems.setdefault(kind, len(sems))]

    def send(way, src, dst, leaves, lands):
        pltpu.make_async_remote_copy(
            src_ref=src, dst_ref=dst, send_sem=sem(send_sem, leaves), recv_sem=sem(recv_sem, lands),
            device_id=target[way], device_id_type=MESH,
        ).start()

    def wait(lands, *like):
        pltpu.make_async_copy(*like, *like, sem(recv_sem, lands)).wait()

    def drain(leaves, like):
        pltpu.make_async_copy(like, like, sem(send_sem, leaves)).wait()

    load_tok = pltpu.make_async_copy(tok_hbm, gath.at[0, 0], local_sem.at[0])
    load_tok.start()
    loads = [
        pltpu.make_async_copy(src.at[0], dst, local_sem.at[1 + i])
        for i, (src, dst) in enumerate(((wg_hbm, wg), (wu_hbm, wu), (wd_hbm, wd)))
    ]
    for load in loads:
        load.start()

    barrier = pltpu.get_barrier_semaphore()
    for way in target:
        pl.semaphore_signal(barrier, inc=1, device_id=target[way], device_id_type=MESH)

    ids = ids_ref[...].astype(F32)
    probs = probs_ref[...]
    weights = probs / jnp.sum(probs, axis=0, keepdims=True)
    experts = lax.broadcasted_iota(jnp.int32, (32, tok), 0).astype(F32)
    named = jnp.zeros((32, tok), F32)
    for k in range(8):
        named = named + jnp.where(ids[k:k + 1, :] == experts, 1.0, 0.0)
    before = lax.broadcasted_iota(jnp.int32, (tok, tok), 0) < lax.broadcasted_iota(jnp.int32, (tok, tok), 1)
    ranks = jnp.dot(named.astype(BF16), before.astype(F32).astype(BF16), preferred_element_type=F32)
    for k in range(8):
        rank = jnp.sum(jnp.where(ids[k:k + 1, :] == experts, ranks, 0.0), axis=0, keepdims=True)
        meta[0, 0, k:k + 1, 0:tok] = ids[k:k + 1, :] * float(most) + rank
    meta[0, 0, 8:16, 0:tok] = weights

    pl.semaphore_wait(barrier, 6)
    load_tok.wait()

    first, second = pl.ds(0, half), pl.ds(half, half)
    quarters = [pl.ds(q * quarter, quarter) for q in range(4)]

    def move(kind, leaves, way, slot, cols, with_meta=None):
        dx, dy = slot
        shift = {"xp": (3, 0), "xm": (1, 0), "yp": (0, 3), "ym": (0, 1)}[way]
        to = ((dx + shift[0]) % 4, (dy + shift[1]) % 4)
        send(way, gath.at[dx, dy, :, cols], gath.at[to[0], to[1], :, cols], leaves, kind)
        if with_meta:
            send(way, meta.at[dx, dy], meta.at[to[0], to[1]], with_meta, "m" + kind)

    def own_first():
        for way in ("xp", "xm"):
            move("own", "own", way, (0, 0), first, "m12")
        for way in ("yp", "ym"):
            move("own", "own", way, (0, 0), second, "m3")

    def own_second():
        for way in ("yp", "ym"):
            move("pass0", "own", way, (0, 0), first)
        for way in ("xp", "xm"):
            move("pass0", "own", way, (0, 0), second)

    def own_relay():
        move("far", "pass", "xp", (3, 0), quarters[0], "m12")
        move("far", "pass", "xm", (1, 0), quarters[1])
        move("far", "pass", "yp", (0, 3), quarters[2], "m3")
        move("far", "pass", "ym", (0, 1), quarters[3])

    def passes(d):
        e = (4 - d) % 4
        move(f"pass{d}", "pass", "ym", (d, 0), first, "m12")
        move(f"pass{d}", "second", "xm", (0, d), second)
        move(f"pass{d}", "pass", "yp", (e, 0), first, "m12")
        move(f"pass{d}", "second", "xp", (0, e), second)

    def relays(d):
        move(f"relay{d}", "relay", "yp", (d, 3), quarters[0], "m12" if d else None)
        move(f"relay{d}", "relay", "ym", (d, 1), quarters[1])
        move(f"relay{d}", "relay", "xp", (3, d), quarters[2])
        move(f"relay{d}", "relay", "xm", (1, d), quarters[3])

    def got_own():
        wait("own", gath.at[0, 0:2])
        wait("mown", meta.at[0])

    def got_far():
        wait("far", gath.at[0, 0])
        wait("mfar", meta.at[0, 0:2])

    def got_passes(d):
        wait(f"pass{d}", gath.at[0, 0:2])
        if d:
            wait(f"mpass{d}", meta.at[0, 0:2])

    def got_relays(d):
        wait(f"relay{d}", gath.at[0, 0])
        if d:
            wait(f"mrelay{d}", meta.at[0, 0])

    place_row = lax.broadcasted_iota(jnp.int32, (2 * most, tok), 0)
    wanted = jnp.where(place_row < most, ep * most + place_row, (other - 1) * most + place_row).astype(F32)

    def build(dx, dy):
        place = PLACE[dx, dy]
        one, scaled = jnp.zeros((2 * most, tok), F32), jnp.zeros((2 * most, tok), F32)
        for k in range(8):
            hit = meta[dx, dy, k:k + 1, 0:tok] == wanted
            one = one + jnp.where(hit, 1.0, 0.0)
            scaled = scaled + jnp.where(hit, meta[dx, dy, 8 + k:9 + k, 0:tok], 0.0)
        comb[place] = scaled.T.astype(BF16)
        picks[place] = one.astype(BF16)

    def select(dx, dy):
        place = PLACE[dx, dy]
        rows = most if place < 5 else 2 * most

        @pl.loop(0, 4, unroll=4)
        def _(q):
            cols = pl.ds(pl.multiple_of(q * quarter, quarter), quarter)
            chosen = jnp.dot(picks[place, :rows], gath[dx, dy, :, cols], preferred_element_type=F32).astype(BF16)
            xown[place, :, cols] = chosen[:most]
            if place >= 5:
                zsend[place, :, cols] = chosen[most:]

        if place >= 5:
            group = min((place - 6) // 4, 2)
            send("zm" if place % 2 else "zp", zsend.at[place], zrecv.at[place], "rows", f"rows{group}")

    def select_all(*slots):
        for slot in slots:
            build(*slot)
            select(*slot)

    def got_rows(group):
        wait(f"rows{group}", zrecv.at[pl.ds(0, (4, 4, 3)[group])])

    near_experts = (ep, at(lax.rem(x + 1, 4), y, z_lo), at(lax.rem(x + 3, 4), y, z_lo), at(x, lax.rem(y + 1, 4), z_lo), at(x, lax.rem(y + 3, 4), z_lo))

    def select_foreign():
        for i, expert in enumerate(near_experts):
            row = (expert * most + lax.broadcasted_iota(jnp.int32, (most, tok), 0)).astype(F32)
            one, scaled = jnp.zeros((most, tok), F32), jnp.zeros((most, tok), F32)
            for k in range(8):
                hit = fmeta[k:k + 1, 0:tok] == row
                one = one + jnp.where(hit, 1.0, 0.0)
                scaled = scaled + jnp.where(hit, fmeta[8 + k:9 + k, 0:tok], 0.0)
            fcomb[i] = scaled.T.astype(BF16)
            fpick[i * most:(i + 1) * most, :] = one.astype(BF16)

        @pl.loop(0, 4, unroll=4)
        def _(q):
            cols = pl.ds(pl.multiple_of(q * quarter, quarter), quarter)
            chosen = jnp.dot(fpick[...], fgath[:, cols], preferred_element_type=F32).astype(BF16)
            zrecv[0, :, cols] = chosen[:most]
            for i in range(4):
                fsend[i, :, cols] = chosen[(i + 1) * most:(i + 2) * most]

    def send_near():
        for i, (way, slot) in enumerate((("xp", (3, 0)), ("xm", (1, 0)), ("yp", (0, 3)), ("ym", (0, 1)))):
            send(way, fsend.at[i], zrecv.at[PLACE[slot]], "near", "near")

    def back_near():
        for place, way in NEAR.items():
            index = ("xm", "xp", "ym", "yp").index(way)
            send(way, zout.at[place // 2, place % 2], frecv.at[index], "nearback", "nearback")

    def sum_near():
        wait("nearback", frecv)

        @pl.loop(0, 4, unroll=4)
        def _(q):
            cols = pl.ds(pl.multiple_of(q * quarter, quarter), quarter)
            total = jnp.dot(fcomb[0], zout[0, 0, :, cols], preferred_element_type=F32)
            for i in range(4):
                total = total + jnp.dot(fcomb[i + 1], frecv[i, :, cols], preferred_element_type=F32)
            fsum[:, cols] = total.astype(BF16)

        send("zp", fsum, zsum, "sum", "sum")

    tile = 256

    def gate_up(rows_ref, hidden, place, places, start=0, stop=hid // tile):
        rows = places * most

        @pl.loop(start, stop, unroll=stop - start)
        def _(n):
            cols = pl.ds(pl.multiple_of(n * tile, tile), tile)
            block = rows_ref[place:place + places].reshape(rows, width)
            gate = jnp.dot(block, wg[:, cols], preferred_element_type=F32)
            up = jnp.dot(block, wu[:, cols], preferred_element_type=F32)
            hidden[place * most:place * most + rows, cols] = (gate / (1.0 + jnp.exp(-gate)) * up).astype(BF16)

    own_first()
    own_second()
    send("zm", gath.at[0, 0], fgath, "whole", "whole")
    send("zm", meta.at[0, 0], fmeta, "mwhole", "mwhole")
    select_all((0, 0))
    got_own()
    passes(1)
    own_relay()
    passes(3)
    for slot in CLUSTER[1:]:
        build(*slot)
    got_passes(0)
    relays(0)
    for slot in CLUSTER[1:]:
        select(*slot)
    wait("whole", fgath)
    wait("mwhole", fmeta)
    select_foreign()
    for load in loads:
        load.wait()
    gate_up(xown, hown, 0, 5, 0, 2)
    got_passes(1)
    select_all((1, 1), (3, 3))
    got_far()
    passes(2)
    gate_up(xown, hown, 0, 5, 2, 3)
    got_passes(3)
    relays(1)
    relays(3)
    select_all((1, 3), (3, 1))
    got_relays(0)
    select_all((0, 2), (2, 0))
    gate_up(xown, hown, 6, 6, 0, 1)
    got_passes(2)
    relays(2)
    send_near()
    gate_up(xown, hown, 6, 6, 1, 3)
    got_relays(1)
    select_all((1, 2), (2, 1))
    got_relays(3)
    select_all((3, 2), (2, 3))
    got_relays(2)
    select_all((2, 2))

    starts = [sum(PARTS[:c]) * width // sum(PARTS) for c in range(len(PARTS) + 1)]

    def chunk_cols(c):
        return pl.ds(starts[c], starts[c + 1] - starts[c])

    def sides(c):
        middle = (starts[c] + starts[c + 1]) // 2
        return pl.ds(starts[c], middle - starts[c]), pl.ds(middle, starts[c + 1] - middle)

    top, low = pl.ds(0, tok // 2), pl.ds(tok // 2, tok // 2)

    def quarter_chunks(q):
        return [c for c in range(len(PARTS)) if q * quarter <= starts[c] < (q + 1) * quarter]

    def down_z(part_of, q):
        place, places = ((6, 8), (14, 3))[part_of]
        rows = hz[most * place:most * (place + places), :]
        out = jnp.dot(rows, wd[:, quarters[q]], preferred_element_type=F32).astype(BF16)
        for i in range(places):
            zout[(place + i) // 2, (place + i) % 2, :, quarters[q]] = out[most * i:most * (i + 1)]
        for c in quarter_chunks(q):
            for side, way in ((0, "zm"), (1, "zp")):
                pairs = pl.ds(place // 2, (places + 1 - side) // 2)
                send(
                    way,
                    zout.at[pairs, side, :, chunk_cols(c)],
                    both.at[pairs, side, pl.ds(most, most), chunk_cols(c)],
                    "back", f"back{part_of}{c}",
                )

    def down_near():
        @pl.loop(0, 4, unroll=4)
        def _(q):
            cols = pl.ds(pl.multiple_of(q * quarter, quarter), quarter)
            out = jnp.dot(hz[0:5 * most, :], wd[:, cols], preferred_element_type=F32).astype(BF16)
            for i in range(5):
                zout[i // 2, i % 2, :, cols] = out[most * i:most * (i + 1)]

        back_near()

    def down_own(q):
        out = jnp.dot(hown[...], wd[:, quarters[q]], preferred_element_type=F32).astype(BF16)
        for place in PLACE.values():
            both[place // 2, place % 2, 0:most, quarters[q]] = out[most * place:most * (place + 1)]

    def serve_own():
        gate_up(xown, hown, 12, 5)

    def serve_near():
        wait("near", zrecv.at[pl.ds(0, 4)])
        gate_up(zrecv, hz, 0, 5)

    def serve_early():
        got_rows(0)
        got_rows(1)
        gate_up(zrecv, hz, 6, 8)

    def serve_late():
        got_rows(2)
        gate_up(zrecv, hz, 14, 3)

    def fill(c, *slots):
        cols = chunk_cols(c)
        for dx, dy in slots:
            place = PLACE[dx, dy]
            rows = most if place < 5 else 2 * most
            part[dx, dy, :, cols] = jnp.dot(
                comb[place, :, :rows], both[place // 2, place % 2, :rows, cols], preferred_element_type=F32
            ).astype(BF16)

    late = ((3, 2), (2, 3), (2, 2))

    def halves_one(c, pair):
        left, right = sides(c)
        send("yp", part.at[pair, 2, top, left], r1p.at[pair, :, left], "1p", f"1{c}")
        send("ym", part.at[pair, 2, low, left], r1m.at[pair, :, left], "1m", f"1{c}")
        send("xp", part.at[2, pair, top, right], r1p.at[pair, :, right], "1p", f"1{c}")
        send("xm", part.at[2, pair, low, right], r1m.at[pair, :, right], "1m", f"1{c}")

    def expand(c):
        left, right = sides(c)
        wait(f"back0{c}", zrecv.at[pl.ds(0, 8), :, chunk_cols(c)])
        fill(c, (0, 2), (1, 2), (2, 0), (2, 1))
        halves_one(c, pl.ds(0, 2))
        fill(c, *[slot for slot in PLACE if 2 not in slot])
        send("yp", part.at[:, 1, low, left], r2p.at[:, low, left], "2p", f"2{c}")
        send("xp", part.at[1, :, low, right], r2p.at[:, low, right], "2p", f"2{c}")
        send("ym", part.at[pl.ds(0, 2), 3, top, left], r2m.at[pl.ds(0, 2), top, left], "2m", f"2{c}")
        send("xm", part.at[3, pl.ds(0, 2), top, right], r2m.at[pl.ds(0, 2), top, right], "2m", f"2{c}")

    def expand_late(c):
        left, right = sides(c)
        wait(f"back1{c}", zrecv.at[pl.ds(0, 3), :, chunk_cols(c)])
        fill(c, *late)
        halves_one(c, pl.ds(2, 2))
        send("ym", part.at[pl.ds(2, 2), 3, top, left], r2m.at[pl.ds(2, 2), top, left], "2m", f"2{c}")
        send("xm", part.at[3, pl.ds(2, 2), top, right], r2m.at[pl.ds(2, 2), top, right], "2m", f"2{c}")

    def halves_two(c, plus, minus):
        left, right = sides(c)
        send("yp", part.at[:, 1, plus, left], r2p.at[:, plus, left], "2p", f"2{c}")
        send("ym", part.at[:, 3, minus, left], r2m.at[:, minus, left], "2m", f"2{c}")
        send("xp", part.at[1, :, plus, right], r2p.at[:, plus, right], "2p", f"2{c}")
        send("xm", part.at[3, :, minus, right], r2m.at[:, minus, right], "2m", f"2{c}")

    def halves_five(c, plus, minus):
        left, right = sides(c)
        send("xp", part.at[1, 0, plus, left], r5p.at[plus, left], "5p", f"5{c}")
        send("xm", part.at[3, 0, minus, left], r5m.at[minus, left], "5m", f"5{c}")
        send("yp", part.at[0, 1, plus, right], r5p.at[plus, right], "5p", f"5{c}")
        send("ym", part.at[0, 3, minus, right], r5m.at[minus, right], "5m", f"5{c}")

    def double(c):
        return pl.ds(0, 2 * chunk_cols(c).size)

    def add(dx, dy, rows, cols, *refs):
        total = part[dx, dy, rows, cols].astype(F32)
        for ref in refs:
            total = total + ref[...].astype(F32)
        part[dx, dy, rows, cols] = total.astype(BF16)

    every = pl.ds(0, tok)

    def step_two(c):
        left, right = sides(c)
        wait(f"1{c}", r1p.at[:, :, double(c)])
        for d in range(4):
            add(d, 1, top, left, r1p.at[d, :, left])
            add(d, 3, low, left, r1m.at[d, :, left])
            add(1, d, top, right, r1p.at[d, :, right])
            add(3, d, low, right, r1m.at[d, :, right])
        halves_two(c, top, low)

    def step_three(c):
        left, right = sides(c)
        wait(f"2{c}", r2p.at[:, :, double(c)])
        for d in (2, 1, 3, 0):
            add(d, 0, every, left, r2p.at[d, :, left], r2m.at[d, :, left])
            add(0, d, every, right, r2p.at[d, :, right], r2m.at[d, :, right])
            if d == 2:
                send("xp", part.at[2, 0, top, left], r4p.at[:, left], "4p", f"4{c}")
                send("xm", part.at[2, 0, low, left], r4m.at[:, left], "4m", f"4{c}")
                send("yp", part.at[0, 2, top, right], r4p.at[:, right], "4p", f"4{c}")
                send("ym", part.at[0, 2, low, right], r4m.at[:, right], "4m", f"4{c}")
            if d == 3:
                halves_five(c, low, top)

    def step_four(c):
        left, right = sides(c)
        wait(f"4{c}", r4p.at[:, double(c)])
        add(1, 0, top, left, r4p.at[:, left])
        add(3, 0, low, left, r4m.at[:, left])
        add(0, 1, top, right, r4p.at[:, right])
        add(0, 3, low, right, r4m.at[:, right])
        halves_five(c, top, low)

    stores = []

    def step_five(c):
        wait(f"5{c}", r5p.at[:, double(c)])
        if not stores:
            wait("sum", zsum)
        for cols in sides(c):
            total = part[0, 0, :, cols].astype(F32) + zsum[:, cols].astype(F32) + r5p[:, cols].astype(F32) + r5m[:, cols].astype(F32)
            outv[:, cols] = total.astype(BF16)
        cols = chunk_cols(c)
        store = pltpu.make_async_copy(outv.at[:, cols], out_hbm.at[:, cols], local_sem.at[4 + c])
        store.start()
        stores.append(store)

    whole = {"O3": serve_own, "N": serve_near, "Z": serve_early, "L": serve_late, "DN": down_near, "F": sum_near}
    chunked = {
        "a": functools.partial(down_z, 0), "b": functools.partial(down_z, 1), "W": down_own, "G": expand, "E": expand_late,
        "A": step_two, "B": step_three, "C": step_four, "D": step_five,
    }
    for step in STEPS:
        if step in whole:
            whole[step]()
        else:
            chunked[step[0]](int(step[1]))
    assert len(sems) <= MAX_SEMS
    drain("own", gath.at[0])
    drain("pass", gath.at[0])
    drain("second", gath.at[0, 0:3])
    drain("relay", gath.at[0])
    drain("m12", meta.at[0:3])
    drain("m3", meta.at[0, 0:3])
    drain("rows", zsend.at[pl.ds(0, 11)])
    drain("back", zsend.at[pl.ds(0, 11)])
    drain("near", frecv)
    drain("nearback", frecv)
    drain("whole", fgath)
    drain("mwhole", fmeta)
    drain("sum", fsum)
    for kind, like in (("1p", r1p), ("1m", r1m), ("2p", r2p), ("2m", r2m), ("4p", r4p), ("4m", r4m), ("5p", r5p), ("5m", r5m)):
        drain(kind, like)
    for store in stores:
        store.wait()


def shards(n_hi, tokens, expert_ids, gate_probs, w_gate, w_up, w_down):
    tok, width = tokens.shape
    hid = w_gate.shape[2]
    most = 32
    vmem = pl.BlockSpec(memory_space=pltpu.VMEM)
    hbm = pl.BlockSpec(memory_space=pl.ANY)
    return pl.pallas_call(
        functools.partial(kernel, (n_hi, tok, width, hid, most)),
        out_shape=jax.ShapeDtypeStruct((tok, width), BF16),
        in_specs=[hbm, vmem, vmem, hbm, hbm, hbm],
        out_specs=hbm,
        scratch_shapes=[
            pltpu.VMEM((4, 4, tok, width), BF16),
            pltpu.VMEM((4, 4, 16, 128), F32),
            pltpu.VMEM((PLACES, tok, 2 * most), BF16),
            pltpu.VMEM((PLACES, most, width), BF16),
            pltpu.VMEM((PLACES, most, width), BF16),
            pltpu.VMEM((PLACES, most, width), BF16),
            pltpu.VMEM((PLACES * most, hid), BF16),
            pltpu.VMEM((PLACES * most, hid), BF16),
            pltpu.VMEM((width, hid), BF16),
            pltpu.VMEM((width, hid), BF16),
            pltpu.VMEM((hid, width), BF16),
            pltpu.VMEM((PLACES // 2, 2, most, width), BF16),
            pltpu.VMEM((PLACES // 2, 2, 2 * most, width), BF16),
            pltpu.VMEM((4, 4, tok, width), BF16),
            pltpu.VMEM((PLACES, 2 * most, tok), BF16),
            pltpu.VMEM((tok, width), BF16),
            pltpu.VMEM((16, 128), F32),
            pltpu.VMEM((5, tok, most), BF16),
            pltpu.VMEM((5 * most, tok), BF16),
            pltpu.VMEM((4, most, width), BF16),
            pltpu.VMEM((4, most, width), BF16),
            pltpu.VMEM((tok, width), BF16),
            pltpu.VMEM((tok, width), BF16),
            pltpu.VMEM((4, tok // 2, width), BF16),
            pltpu.VMEM((4, tok // 2, width), BF16),
            pltpu.VMEM((4, tok, width), BF16),
            pltpu.VMEM((4, tok, width), BF16),
            pltpu.VMEM((tok // 2, width), BF16),
            pltpu.VMEM((tok // 2, width), BF16),
            pltpu.VMEM((tok, width), BF16),
            pltpu.VMEM((tok, width), BF16),
            pltpu.VMEM((tok, width), BF16),
            pltpu.SemaphoreType.DMA((MAX_SEMS,)),
            pltpu.SemaphoreType.DMA((MAX_SEMS,)),
            pltpu.SemaphoreType.DMA((4 + len(PARTS),)),
        ],
        compiler_params=pltpu.CompilerParams(
            collective_id=0, has_side_effects=True, vmem_limit_bytes=60 * 1024 * 1024
        ),
        name="routed_experts",
    )(tokens, expert_ids.T, gate_probs.T, w_gate, w_up, w_down)


def solution(mesh):
    placed = (
        P(("dp", "ep"), None),
        P(("dp", "ep"), None),
        P(("dp", "ep"), None),
        P("ep", None, None),
        P("ep", None, None),
        P("ep", None, None),
    )
    return jax.shard_map(
        functools.partial(shards, mesh.shape["dp"] // 2), mesh=mesh, in_specs=placed,
        out_specs=P(("dp", "ep"), None), check_vma=False,
    )
```

```python
import functools

import jax
import jax.numpy as jnp
from jax import lax
from jax.experimental import pallas as pl
from jax.experimental.pallas import tpu as pltpu
from jax.sharding import PartitionSpec as P

MESH = pl.DeviceIdType.MESH
F32, BF16 = jnp.float32, jnp.bfloat16
OPPOSITE = {"xp": "xm", "xm": "xp", "yp": "ym", "ym": "yp", "zp": "zm", "zm": "zp"}

CLUSTER = [(0, 0), (1, 0), (3, 0), (0, 1), (0, 3)]
OTHERS = [(1, 1), (3, 3), (1, 3), (3, 1), (0, 2), (2, 0), (1, 2), (2, 1), (3, 2), (2, 3), (2, 2)]
PLACE = {slot: place for place, slot in enumerate(CLUSTER + [None] + OTHERS) if slot}
PLACES = 18
NEAR = {1: "xp", 2: "xm", 3: "yp", 4: "ym"}
PARTS = (1,) * 8
STEPS = (
    "O3", "N", "Z", "a1", "W3", "W1", "L", "b1", "DN", "a2", "b2", "G2", "W2", "E2", "G3", "a3", "E3", "G4", "b3",
    "G5", "E4", "E5", "A2", "A3", "a0", "G6", "W0", "b0", "G7", "A4", "E7", "E6", "G0", "B2", "G1", "E0", "E1", "A5",
    "A6", "F", "A7", "A1", "A0", "B5", "B6", "B3", "B7", "B4", "B1", "B0", "C5", "C3", "C6", "C2", "C7", "C1", "C4",
    "C0", "X", "D7", "D1", "D5", "D4", "D2", "D6", "D3", "D0",
)
LEAVING, LANDING = 22, 75


def kernel(
    sizes, tok_hbm, ids_ref, probs_ref, wg_hbm, wu_hbm, wd_hbm, out_hbm,
    gath, meta, comb, xown, zsend, zrecv, hown, hz, wg, wu, wd, zout, both, part, picks,
    fgath, fmeta, fcomb, fpick, fsend, frecv, fsum, zsum, esend, erecv,
    r1p, r1m, r2p, r2m, r4p, r4m, r5p, r5m, outv,
    send_sem, recv_sem, local_sem,
):
    n_hi, tok, width, hid, most = sizes
    half, quarter = width // 2, width // 4
    ep, dp = lax.axis_index("ep"), lax.axis_index("dp")
    x, y, z_lo = lax.rem(ep, 4), lax.rem(ep // 4, 4), ep // 16
    z_hi, core = dp // 2, lax.rem(dp, 2)

    def at(xx, yy, zz):
        return zz * 16 + yy * 4 + xx

    cross = 1 - core
    here = z_hi * 2 + cross
    z_up = lax.rem(z_hi + z_lo, n_hi) * 2 + cross
    z_down = lax.rem(z_hi + z_lo + n_hi - 1, n_hi) * 2 + cross
    target = {
        "xp": {"ep": at(lax.rem(x + 1, 4), y, z_lo), "dp": here},
        "xm": {"ep": at(lax.rem(x + 3, 4), y, z_lo), "dp": here},
        "yp": {"ep": at(x, lax.rem(y + 1, 4), z_lo), "dp": here},
        "ym": {"ep": at(x, lax.rem(y + 3, 4), z_lo), "dp": here},
        "zp": {"ep": at(x, y, 1 - z_lo), "dp": z_up},
        "zm": {"ep": at(x, y, 1 - z_lo), "dp": z_down},
    }
    other = at(x, y, 1 - z_lo)

    leaving, landing = {}, {}

    def sem(array, kinds, kind):
        return array.at[kinds.setdefault(kind, len(kinds))]

    def send(way, src, dst, leaves, lands):
        pltpu.make_async_remote_copy(
            src_ref=src, dst_ref=dst, send_sem=sem(send_sem, leaving, leaves), recv_sem=sem(recv_sem, landing, lands),
            device_id=target[way], device_id_type=MESH,
        ).start()

    def wait(lands, *like):
        pltpu.make_async_copy(*like, *like, sem(recv_sem, landing, lands)).wait()

    def drain(leaves, like):
        pltpu.make_async_copy(like, like, sem(send_sem, leaving, leaves)).wait()

    barrier = pltpu.get_barrier_semaphore()
    for way in target:
        pl.semaphore_signal(barrier, inc=1, device_id=target[way], device_id_type=MESH)

    load_tok = pltpu.make_async_copy(tok_hbm, gath.at[0, 0], local_sem.at[0])
    load_tok.start()
    loads = [
        pltpu.make_async_copy(src.at[0], dst, local_sem.at[1 + i])
        for i, (src, dst) in enumerate(((wg_hbm, wg), (wu_hbm, wu), (wd_hbm, wd)))
    ]
    for load in loads:
        load.start()

    ids = ids_ref[...].astype(F32)
    probs = probs_ref[...]
    weights = probs / jnp.sum(probs, axis=0, keepdims=True)
    experts = lax.broadcasted_iota(jnp.int32, (32, tok), 0).astype(F32)
    named = jnp.zeros((32, tok), F32)
    for k in range(8):
        named = named + jnp.where(ids[k:k + 1, :] == experts, 1.0, 0.0)
    before = lax.broadcasted_iota(jnp.int32, (tok, tok), 0) < lax.broadcasted_iota(jnp.int32, (tok, tok), 1)
    ranks = jnp.dot(named.astype(BF16), before.astype(F32).astype(BF16), preferred_element_type=F32)
    for k in range(8):
        rank = jnp.sum(jnp.where(ids[k:k + 1, :] == experts, ranks, 0.0), axis=0, keepdims=True)
        meta[0, 0, k:k + 1, 0:tok] = ids[k:k + 1, :] * float(most) + rank
    meta[0, 0, 8:16, 0:tok] = weights

    pl.semaphore_wait(barrier, 6)
    load_tok.wait()

    first, second = pl.ds(0, half), pl.ds(half, half)
    quarters = [pl.ds(q * quarter, quarter) for q in range(4)]

    def move(kind, leaves, way, slot, cols, with_meta=None):
        dx, dy = slot
        shift = {"xp": (3, 0), "xm": (1, 0), "yp": (0, 3), "ym": (0, 1)}[way]
        to = ((dx + shift[0]) % 4, (dy + shift[1]) % 4)
        send(way, gath.at[dx, dy, :, cols], gath.at[to[0], to[1], :, cols], leaves, kind)
        if with_meta:
            send(way, meta.at[dx, dy], meta.at[to[0], to[1]], with_meta, "m" + kind)

    def own_first():
        for way in ("xp", "xm"):
            move("own", "own", way, (0, 0), first, "m12")
        for way in ("yp", "ym"):
            move("own", "own", way, (0, 0), second, "m3")

    def own_second():
        for way in ("yp", "ym"):
            move("pass0", "own", way, (0, 0), first)
        for way in ("xp", "xm"):
            move("pass0", "own", way, (0, 0), second)

    def own_relay():
        move("far", "pass", "xp", (3, 0), quarters[0], "m12")
        move("far", "pass", "xm", (1, 0), quarters[1])
        move("far", "pass", "yp", (0, 3), quarters[2], "m3")
        move("far", "pass", "ym", (0, 1), quarters[3])

    def passes(d):
        e = (4 - d) % 4
        move(f"pass{d}", "pass", "ym", (d, 0), first, "m12")
        move(f"pass{d}", "second", "xm", (0, d), second)
        move(f"pass{d}", "pass", "yp", (e, 0), first, "m12")
        move(f"pass{d}", "second", "xp", (0, e), second)

    def relays(d):
        move(f"relay{d}", "relay", "yp", (d, 3), quarters[0], "m12" if d else None)
        move(f"relay{d}", "relay", "ym", (d, 1), quarters[1])
        move(f"relay{d}", "relay", "xp", (3, d), quarters[2])
        move(f"relay{d}", "relay", "xm", (1, d), quarters[3])

    def got_own():
        wait("own", gath.at[0, 0:2])
        wait("mown", meta.at[0])

    def got_far():
        wait("far", gath.at[0, 0])
        wait("mfar", meta.at[0, 0:2])

    def got_passes(d):
        wait(f"pass{d}", gath.at[0, 0:2])
        if d:
            wait(f"mpass{d}", meta.at[0, 0:2])

    def got_relays(d):
        wait(f"relay{d}", gath.at[0, 0])
        if d:
            wait(f"mrelay{d}", meta.at[0, 0])

    place_row = lax.broadcasted_iota(jnp.int32, (2 * most, tok), 0)
    wanted = jnp.where(place_row < most, ep * most + place_row, (other - 1) * most + place_row).astype(F32)

    def build(dx, dy):
        place = PLACE[dx, dy]
        one, scaled = jnp.zeros((2 * most, tok), F32), jnp.zeros((2 * most, tok), F32)
        for k in range(8):
            hit = meta[dx, dy, k:k + 1, 0:tok] == wanted
            one = one + jnp.where(hit, 1.0, 0.0)
            scaled = scaled + jnp.where(hit, meta[dx, dy, 8 + k:9 + k, 0:tok], 0.0)
        comb[place] = scaled.T.astype(BF16)
        picks[place] = one.astype(BF16)

    def ways_out(place):
        if place == 16:
            return (("zp", pl.ds(0, most // 2)), ("zm", pl.ds(most // 2, most // 2)))
        return (("zm" if place % 2 else "zp", pl.ds(0, most)),)

    def select(dx, dy):
        place = PLACE[dx, dy]
        rows = most if place < 5 else 2 * most

        @pl.loop(0, 4, unroll=4)
        def _(q):
            cols = pl.ds(pl.multiple_of(q * quarter, quarter), quarter)
            chosen = jnp.dot(picks[place, :rows], gath[dx, dy, :, cols], preferred_element_type=F32).astype(BF16)
            xown[place, :, cols] = chosen[:most]
            if place >= 5:
                zsend[place, :, cols] = chosen[most:]

        if place >= 5:
            group = min((place - 6) // 4, 2)
            for way, rows in ways_out(place):
                send(way, zsend.at[place, rows], zrecv.at[place, rows], "rows", f"rows{group}")

    def select_all(*slots):
        for slot in slots:
            build(*slot)
            select(*slot)

    def got_rows(group):
        wait(f"rows{group}", zrecv.at[pl.ds(0, (4, 4, 3)[group])])

    near_experts = (ep, at(lax.rem(x + 1, 4), y, z_lo), at(lax.rem(x + 3, 4), y, z_lo), at(x, lax.rem(y + 1, 4), z_lo), at(x, lax.rem(y + 3, 4), z_lo))

    def select_foreign():
        for i, expert in enumerate(near_experts):
            row = (expert * most + lax.broadcasted_iota(jnp.int32, (most, tok), 0)).astype(F32)
            one, scaled = jnp.zeros((most, tok), F32), jnp.zeros((most, tok), F32)
            for k in range(8):
                hit = fmeta[k:k + 1, 0:tok] == row
                one = one + jnp.where(hit, 1.0, 0.0)
                scaled = scaled + jnp.where(hit, fmeta[8 + k:9 + k, 0:tok], 0.0)
            fcomb[i] = scaled.T.astype(BF16)
            fpick[i * most:(i + 1) * most, :] = one.astype(BF16)

        @pl.loop(0, 4, unroll=4)
        def _(q):
            cols = pl.ds(pl.multiple_of(q * quarter, quarter), quarter)
            chosen = jnp.dot(fpick[...], fgath[:, cols], preferred_element_type=F32).astype(BF16)
            zrecv[0, :, cols] = chosen[:most]
            for i in range(4):
                fsend[i, :, cols] = chosen[(i + 1) * most:(i + 2) * most]

    def send_near():
        for i, (way, slot) in enumerate((("xp", (3, 0)), ("xm", (1, 0)), ("yp", (0, 3)), ("ym", (0, 1)))):
            send(way, fsend.at[i], zrecv.at[PLACE[slot]], "near", "near")

    def back_near():
        for place, way in NEAR.items():
            index = ("xm", "xp", "ym", "yp").index(way)
            send(way, zout.at[place // 2, place % 2], frecv.at[index], "nearback", "nearback")

    def sum_near():
        wait("nearback", frecv)

        @pl.loop(0, 4, unroll=4)
        def _(q):
            cols = pl.ds(pl.multiple_of(q * quarter, quarter), quarter)
            total = jnp.dot(fcomb[0], zout[0, 0, :, cols], preferred_element_type=F32)
            for i in range(4):
                total = total + jnp.dot(fcomb[i + 1], frecv[i, :, cols], preferred_element_type=F32)
            fsum[:, cols] = total.astype(BF16)

        send("zp", fsum, zsum, "sum", "sum")

    tile = 256

    def gate_up(rows_ref, hidden, place, places, start=0, stop=hid // tile):
        rows = places * most

        @pl.loop(start, stop, unroll=stop - start)
        def _(n):
            cols = pl.ds(pl.multiple_of(n * tile, tile), tile)
            block = rows_ref[place:place + places].reshape(rows, width)
            gate = jnp.dot(block, wg[:, cols], preferred_element_type=F32)
            up = jnp.dot(block, wu[:, cols], preferred_element_type=F32)
            hidden[place * most:place * most + rows, cols] = (gate / (1.0 + jnp.exp(-gate)) * up).astype(BF16)

    starts = [sum(PARTS[:c]) * width // sum(PARTS) for c in range(len(PARTS) + 1)]

    def chunk_cols(c):
        return pl.ds(starts[c], starts[c + 1] - starts[c])

    def sides(c):
        middle = (starts[c] + starts[c + 1]) // 2
        return pl.ds(starts[c], middle - starts[c]), pl.ds(middle, starts[c + 1] - middle)

    top, low = pl.ds(0, tok // 2), pl.ds(tok // 2, tok // 2)

    def early_own():
        for q in range(4):
            out = jnp.dot(hown[0:5 * most, :], wd[:, quarters[q]], preferred_element_type=F32).astype(BF16)
            for slot, place in PLACE.items():
                if place < 5:
                    part[slot[0], slot[1], :, quarters[q]] = jnp.dot(
                        comb[place, :, :most], out[most * place:most * (place + 1)], preferred_element_type=F32
                    ).astype(BF16)
        for c in range(len(PARTS)):
            left, right = sides(c)
            esend[0, :, early_cols(c)] = part[0, 1, low, left]
            esend[1, :, early_cols(c)] = part[0, 3, top, left]
            esend[2, :, early_cols(c)] = part[1, 0, low, right]
            esend[3, :, early_cols(c)] = part[3, 0, top, right]

    def early_cols(c):
        return pl.ds(starts[c] // 2, (starts[c + 1] - starts[c]) // 2)

    def send_early():
        for i, way in enumerate(("yp", "ym", "xp", "xm")):
            send(way, esend.at[i], erecv.at[i], "early", "early")

    own_first()
    own_second()
    send("zm", gath.at[0, 0], fgath, "whole", "whole")
    send("zm", meta.at[0, 0], fmeta, "mwhole", "mwhole")
    select_all((0, 0))
    got_own()
    passes(1)
    own_relay()
    passes(3)
    for slot in CLUSTER[1:]:
        build(*slot)
    got_passes(0)
    relays(0)
    for slot in CLUSTER[1:]:
        select(*slot)
    wait("whole", fgath)
    wait("mwhole", fmeta)
    select_foreign()
    for load in loads:
        load.wait()
    gate_up(xown, hown, 0, 5, 0, 2)
    got_passes(1)
    select_all((1, 1), (3, 3))
    got_far()
    passes(2)
    gate_up(xown, hown, 0, 5, 2, 3)
    early_own()
    got_passes(3)
    relays(1)
    relays(3)
    select_all((1, 3), (3, 1))
    got_relays(0)
    select_all((0, 2), (2, 0))
    gate_up(xown, hown, 6, 6, 0, 1)
    got_passes(2)
    relays(2)
    send_near()
    send_early()
    gate_up(xown, hown, 6, 6, 1, 3)
    got_relays(1)
    select_all((1, 2), (2, 1))
    got_relays(3)
    select_all((3, 2), (2, 3))
    got_relays(2)
    select_all((2, 2))

    def quarter_chunks(q):
        return [c for c in range(len(PARTS)) if q * quarter <= starts[c] < (q + 1) * quarter]

    def down_z(part_of, q):
        place, places = ((6, 8), (14, 3))[part_of]
        rows = hz[most * place:most * (place + places), :]
        out = jnp.dot(rows, wd[:, quarters[q]], preferred_element_type=F32).astype(BF16)
        for i in range(places):
            zout[(place + i) // 2, (place + i) % 2, :, quarters[q]] = out[most * i:most * (i + 1)]
        for c in quarter_chunks(q):
            cols, kind = chunk_cols(c), f"back{part_of}{c}"
            if part_of == 0:
                for side, way in ((0, "zm"), (1, "zp")):
                    pairs = pl.ds(place // 2, places // 2)
                    send(way, zout.at[pairs, side, :, cols], both.at[pairs, side, pl.ds(most, most), cols], "back", kind)
            else:
                for i in range(places):
                    pair, side = (place + i) // 2, (place + i) % 2
                    for way, rows in ways_out(place + i):
                        to = pl.ds(most + rows.start, rows.size)
                        send(OPPOSITE[way], zout.at[pair, side, rows, cols], both.at[pair, side, to, cols], "back", kind)

    def down_near():
        @pl.loop(0, 4, unroll=4)
        def _(q):
            cols = pl.ds(pl.multiple_of(q * quarter, quarter), quarter)
            out = jnp.dot(hz[0:5 * most, :], wd[:, cols], preferred_element_type=F32).astype(BF16)
            for i in range(5):
                zout[i // 2, i % 2, :, cols] = out[most * i:most * (i + 1)]

        back_near()

    def down_own(q):
        rows = hown[6 * most:17 * most, :]
        out = jnp.dot(rows, wd[:, quarters[q]], preferred_element_type=F32).astype(BF16)
        for place in range(6, 17):
            both[place // 2, place % 2, 0:most, quarters[q]] = out[most * (place - 6):most * (place - 5)]

    def serve_own():
        gate_up(xown, hown, 12, 5)

    def serve_near():
        wait("near", zrecv.at[pl.ds(0, 4)])
        gate_up(zrecv, hz, 0, 5)

    def serve_early():
        got_rows(0)
        got_rows(1)
        gate_up(zrecv, hz, 6, 8)

    def serve_late():
        got_rows(2)
        gate_up(zrecv, hz, 14, 3)

    def fill(c, *slots):
        cols = chunk_cols(c)
        for dx, dy in slots:
            place = PLACE[dx, dy]
            part[dx, dy, :, cols] = jnp.dot(
                comb[place], both[place // 2, place % 2, :, cols], preferred_element_type=F32
            ).astype(BF16)

    late = ((3, 2), (2, 3), (2, 2))

    def halves_one(c, pair):
        left, right = sides(c)
        send("yp", part.at[pair, 2, top, left], r1p.at[pair, :, left], "1p", f"1{c}")
        send("ym", part.at[pair, 2, low, left], r1m.at[pair, :, left], "1m", f"1{c}")
        send("xp", part.at[2, pair, top, right], r1p.at[pair, :, right], "1p", f"1{c}")
        send("xm", part.at[2, pair, low, right], r1m.at[pair, :, right], "1m", f"1{c}")

    def expand(c):
        left, right = sides(c)
        wait(f"back0{c}", zrecv.at[pl.ds(0, 8), :, chunk_cols(c)])
        fill(c, (0, 2), (1, 2), (2, 0), (2, 1))
        halves_one(c, pl.ds(0, 2))
        fill(c, (1, 1), (3, 3), (1, 3), (3, 1))
        send("yp", part.at[pl.ds(1, 3), 1, low, left], r2p.at[pl.ds(1, 3), low, left], "2p", f"2{c}")
        send("xp", part.at[1, pl.ds(1, 3), low, right], r2p.at[pl.ds(1, 3), low, right], "2p", f"2{c}")
        send("ym", part.at[1, 3, top, left], r2m.at[1, top, left], "2m", f"2{c}")
        send("xm", part.at[3, 1, top, right], r2m.at[1, top, right], "2m", f"2{c}")

    def expand_late(c):
        left, right = sides(c)
        wait(f"back1{c}", zrecv.at[pl.ds(0, 3), :, chunk_cols(c)])
        fill(c, *late)
        halves_one(c, pl.ds(2, 2))
        send("ym", part.at[pl.ds(2, 2), 3, top, left], r2m.at[pl.ds(2, 2), top, left], "2m", f"2{c}")
        send("xm", part.at[3, pl.ds(2, 2), top, right], r2m.at[pl.ds(2, 2), top, right], "2m", f"2{c}")

    def halves_two(c, plus, minus):
        left, right = sides(c)
        send("yp", part.at[:, 1, plus, left], r2p.at[:, plus, left], "2p", f"2{c}")
        send("ym", part.at[:, 3, minus, left], r2m.at[:, minus, left], "2m", f"2{c}")
        send("xp", part.at[1, :, plus, right], r2p.at[:, plus, right], "2p", f"2{c}")
        send("xm", part.at[3, :, minus, right], r2m.at[:, minus, right], "2m", f"2{c}")

    def halves_five(c, plus, minus):
        left, right = sides(c)
        send("xp", part.at[1, 0, plus, left], r5p.at[plus, left], "5p", f"5{c}")
        send("xm", part.at[3, 0, minus, left], r5m.at[minus, left], "5m", f"5{c}")
        send("yp", part.at[0, 1, plus, right], r5p.at[plus, right], "5p", f"5{c}")
        send("ym", part.at[0, 3, minus, right], r5m.at[minus, right], "5m", f"5{c}")

    def double(c):
        return pl.ds(0, 2 * chunk_cols(c).size)

    def add(dx, dy, rows, cols, *refs):
        total = part[dx, dy, rows, cols].astype(F32)
        for ref in refs:
            total = total + ref[...].astype(F32)
        part[dx, dy, rows, cols] = total.astype(BF16)

    every = pl.ds(0, tok)

    def step_two(c):
        left, right = sides(c)
        wait(f"1{c}", r1p.at[:, :, double(c)])
        for d in range(4):
            add(d, 1, top, left, r1p.at[d, :, left])
            add(d, 3, low, left, r1m.at[d, :, left])
            add(1, d, top, right, r1p.at[d, :, right])
            add(3, d, low, right, r1m.at[d, :, right])
        halves_two(c, top, low)

    got = []

    def step_three(c):
        left, right = sides(c)
        wait(f"2{c}", both.at[pl.ds(0, 7), 0, :, chunk_cols(c)])
        if "early" not in got:
            got.append("early")
            wait("early", erecv)
        for d in (2, 1, 3, 0):
            if d == 0:
                for cols, plus, minus in ((left, 0, 1), (right, 2, 3)):
                    add(0, 0, top, cols, r2p.at[0, top, cols], erecv.at[minus, :, early_cols(c)])
                    add(0, 0, low, cols, erecv.at[plus, :, early_cols(c)], r2m.at[0, low, cols])
                continue
            add(d, 0, every, left, r2p.at[d, :, left], r2m.at[d, :, left])
            add(0, d, every, right, r2p.at[d, :, right], r2m.at[d, :, right])
            if d == 2:
                send("xp", part.at[2, 0, top, left], r4p.at[:, left], "4p", f"4{c}")
                send("xm", part.at[2, 0, low, left], r4m.at[:, left], "4m", f"4{c}")
                send("yp", part.at[0, 2, top, right], r4p.at[:, right], "4p", f"4{c}")
                send("ym", part.at[0, 2, low, right], r4m.at[:, right], "4m", f"4{c}")
            if d == 3:
                halves_five(c, low, top)

    def step_four(c):
        left, right = sides(c)
        wait(f"4{c}", r4p.at[:, double(c)])
        add(1, 0, top, left, r4p.at[:, left])
        add(3, 0, low, left, r4m.at[:, left])
        add(0, 1, top, right, r4p.at[:, right])
        add(0, 3, low, right, r4m.at[:, right])
        halves_five(c, top, low)

    stores = []


    def step_five(c):
        wait(f"5{c}", r5p.at[:, double(c)])
        if not stores:
            wait("sum", zsum)
        for cols in sides(c):
            total = part[0, 0, :, cols].astype(F32) + zsum[:, cols].astype(F32) + r5p[:, cols].astype(F32) + r5m[:, cols].astype(F32)
            outv[:, cols] = total.astype(BF16)
        cols = chunk_cols(c)
        store = pltpu.make_async_copy(outv.at[:, cols], out_hbm.at[:, cols], local_sem.at[4])
        store.start()
        stores.append(c)

    def drain_all(c=0):
        drain("own", gath.at[0])
        drain("pass", gath.at[0])
        drain("second", gath.at[0, 0:3])
        drain("relay", gath.at[0])
        drain("m12", meta.at[0:3])
        drain("m3", meta.at[0, 0:3])
        for kind in ("rows", "back"):
            drain(kind, zsend.at[pl.ds(0, 11)])
        for kind in ("near", "nearback"):
            drain(kind, frecv)
        drain("whole", fgath)
        drain("mwhole", fmeta)
        drain("sum", fsum)
        drain("early", esend)
        for kind, like in (("1p", r1p), ("1m", r1m), ("4p", r4p), ("4m", r4m)):
            drain(kind, like)
        for kind in ("2p", "2m"):
            drain(kind, both.at[pl.ds(0, 7), 0, :, first])

    whole = {"O3": serve_own, "N": serve_near, "Z": serve_early, "L": serve_late, "DN": down_near, "F": sum_near, "X": drain_all}
    chunked = {
        "a": functools.partial(down_z, 0), "b": functools.partial(down_z, 1), "W": down_own, "G": expand, "E": expand_late,
        "A": step_two, "B": step_three, "C": step_four, "D": step_five,
    }
    for step in STEPS:
        if step in whole:
            whole[step]()
        else:
            chunked[step[0]](int(step[1]))
    assert (len(leaving), len(landing)) == (LEAVING, LANDING), (len(leaving), len(landing))
    drain("5p", r5p)
    drain("5m", r5m)
    pltpu.make_async_copy(outv, out_hbm, local_sem.at[4]).wait()


def shards(n_hi, tokens, expert_ids, gate_probs, w_gate, w_up, w_down):
    tok, width = tokens.shape
    hid = w_gate.shape[2]
    most = 32
    vmem = pl.BlockSpec(memory_space=pltpu.VMEM)
    hbm = pl.BlockSpec(memory_space=pl.ANY)
    return pl.pallas_call(
        functools.partial(kernel, (n_hi, tok, width, hid, most)),
        out_shape=jax.ShapeDtypeStruct((tok, width), BF16),
        in_specs=[hbm, vmem, vmem, hbm, hbm, hbm],
        out_specs=hbm,
        scratch_shapes=[
            pltpu.VMEM((4, 4, tok, width), BF16),
            pltpu.VMEM((4, 4, 16, 128), F32),
            pltpu.VMEM((PLACES, tok, 2 * most), BF16),
            pltpu.VMEM((PLACES, most, width), BF16),
            pltpu.VMEM((PLACES, most, width), BF16),
            pltpu.VMEM((PLACES, most, width), BF16),
            pltpu.VMEM((PLACES * most, hid), BF16),
            pltpu.VMEM((PLACES * most, hid), BF16),
            pltpu.VMEM((width, hid), BF16),
            pltpu.VMEM((width, hid), BF16),
            pltpu.VMEM((hid, width), BF16),
            pltpu.VMEM((PLACES // 2, 2, most, width), BF16),
            pltpu.VMEM((PLACES // 2, 2, 2 * most, width), BF16),
            pltpu.VMEM((4, 4, tok, width), BF16),
            pltpu.VMEM((PLACES, 2 * most, tok), BF16),
            pltpu.VMEM((tok, width), BF16),
            pltpu.VMEM((16, 128), F32),
            pltpu.VMEM((5, tok, most), BF16),
            pltpu.VMEM((5 * most, tok), BF16),
            pltpu.VMEM((4, most, width), BF16),
            pltpu.VMEM((4, most, width), BF16),
            pltpu.VMEM((tok, width), BF16),
            pltpu.VMEM((tok, width), BF16),
            pltpu.VMEM((4, tok // 2, width // 2), BF16),
            pltpu.VMEM((4, tok // 2, width // 2), BF16),
            pltpu.VMEM((4, tok // 2, width), BF16),
            pltpu.VMEM((4, tok // 2, width), BF16),
            pltpu.VMEM((4, tok, width), BF16),
            pltpu.VMEM((4, tok, width), BF16),
            pltpu.VMEM((tok // 2, width), BF16),
            pltpu.VMEM((tok // 2, width), BF16),
            pltpu.VMEM((tok, width), BF16),
            pltpu.VMEM((tok, width), BF16),
            pltpu.VMEM((tok, width), BF16),
            pltpu.SemaphoreType.DMA((LEAVING,)),
            pltpu.SemaphoreType.DMA((LANDING,)),
            pltpu.SemaphoreType.DMA((5,)),
        ],
        compiler_params=pltpu.CompilerParams(
            collective_id=0, has_side_effects=True, vmem_limit_bytes=60 * 1024 * 1024
        ),
        name="routed_experts",
    )(tokens, expert_ids.T, gate_probs.T, w_gate, w_up, w_down)


def solution(mesh):
    placed = (
        P(("dp", "ep"), None),
        P(("dp", "ep"), None),
        P(("dp", "ep"), None),
        P("ep", None, None),
        P("ep", None, None),
        P("ep", None, None),
    )
    return jax.shard_map(
        functools.partial(shards, mesh.shape["dp"] // 2), mesh=mesh, in_specs=placed,
        out_specs=P(("dp", "ep"), None), check_vma=False,
    )
```

```python
import functools

import jax
import jax.numpy as jnp
from jax import lax
from jax.experimental import pallas as pl
from jax.experimental.pallas import tpu as pltpu
from jax.sharding import PartitionSpec as P

MESH = pl.DeviceIdType.MESH
F32, BF16 = jnp.float32, jnp.bfloat16
OPPOSITE = {"xp": "xm", "xm": "xp", "yp": "ym", "ym": "yp", "zp": "zm", "zm": "zp"}

CLUSTER = [(0, 0), (1, 0), (3, 0), (0, 1), (0, 3)]
OTHERS = [(1, 1), (3, 3), (1, 3), (3, 1), (0, 2), (2, 0), (1, 2), (2, 1), (3, 2), (2, 3), (2, 2)]
PLACE = {slot: place for place, slot in enumerate(CLUSTER + [None] + OTHERS) if slot}
PLACES = 18
NEAR = {1: "xp", 2: "xm", 3: "yp", 4: "ym"}
PARTS = (1,) * 8
STEPS = (
    "O3", "Z", "a3", "W3", "a1", "N", "DN", "L", "W2", "G6", "W1", "b1", "b3", "a0", "G7", "W0", "G2", "G3", "E2",
    "b0", "E3", "E6", "b2", "a2", "E7", "G0", "A2", "A3", "G1", "E0", "A7", "A6", "E1", "G4", "E4", "F", "G5", "E5",
    "A1", "A0", "A4", "B7", "A5", "B2", "B1", "B6", "B0", "B3", "B4", "B5", "C7", "C1", "C0", "C2", "C6", "C4", "C3",
    "C5", "X", "D4", "D0", "D3", "D1", "D6", "D7", "D2", "D5",
)
LEAVING, LANDING = 21, 73


def kernel(
    sizes, tok_hbm, ids_ref, probs_ref, wg_hbm, wu_hbm, wd_hbm, out_hbm,
    gath, meta, comb, xown, zsend, zrecv, hown, hz, wg, wu, wd, zout, both, part, picks,
    fgath, fmeta, fcomb, fpick, fsend, frecv, fsum, zsum, esend, erecv,
    r1p, r1m, r2p, r2m, r4p, r4m, r5p, r5m, outv,
    send_sem, recv_sem, local_sem,
):
    n_hi, tok, width, hid, most = sizes
    half, quarter = width // 2, width // 4
    ep, dp = lax.axis_index("ep"), lax.axis_index("dp")
    x, y, z_lo = lax.rem(ep, 4), lax.rem(ep // 4, 4), ep // 16
    z_hi, core = dp // 2, lax.rem(dp, 2)

    def at(xx, yy, zz):
        return zz * 16 + yy * 4 + xx

    cross = 1 - core
    here = z_hi * 2 + cross
    z_up = lax.rem(z_hi + z_lo, n_hi) * 2 + cross
    z_down = lax.rem(z_hi + z_lo + n_hi - 1, n_hi) * 2 + cross
    target = {
        "xp": {"ep": at(lax.rem(x + 1, 4), y, z_lo), "dp": here},
        "xm": {"ep": at(lax.rem(x + 3, 4), y, z_lo), "dp": here},
        "yp": {"ep": at(x, lax.rem(y + 1, 4), z_lo), "dp": here},
        "ym": {"ep": at(x, lax.rem(y + 3, 4), z_lo), "dp": here},
        "zp": {"ep": at(x, y, 1 - z_lo), "dp": z_up},
        "zm": {"ep": at(x, y, 1 - z_lo), "dp": z_down},
    }
    other = at(x, y, 1 - z_lo)

    leaving, landing = {}, {}

    def sem(array, kinds, kind):
        return array.at[kinds.setdefault(kind, len(kinds))]

    def send(way, src, dst, leaves, lands):
        pltpu.make_async_remote_copy(
            src_ref=src, dst_ref=dst, send_sem=sem(send_sem, leaving, leaves), recv_sem=sem(recv_sem, landing, lands),
            device_id=target[way], device_id_type=MESH,
        ).start()

    def wait(lands, *like):
        pltpu.make_async_copy(*like, *like, sem(recv_sem, landing, lands)).wait()

    def drain(leaves, like):
        pltpu.make_async_copy(like, like, sem(send_sem, leaving, leaves)).wait()

    barrier = pltpu.get_barrier_semaphore()
    for way in target:
        pl.semaphore_signal(barrier, inc=1, device_id=target[way], device_id_type=MESH)

    load_tok = pltpu.make_async_copy(tok_hbm, gath.at[0, 0], local_sem.at[0])
    load_tok.start()
    loads = [
        pltpu.make_async_copy(src.at[0], dst, local_sem.at[1 + i])
        for i, (src, dst) in enumerate(((wg_hbm, wg), (wu_hbm, wu), (wd_hbm, wd)))
    ]
    for load in loads:
        load.start()

    ids = ids_ref[...].astype(F32)
    probs = probs_ref[...]
    weights = probs / jnp.sum(probs, axis=0, keepdims=True)
    experts = lax.broadcasted_iota(jnp.int32, (32, tok), 0).astype(F32)
    named = jnp.zeros((32, tok), F32)
    for k in range(8):
        named = named + jnp.where(ids[k:k + 1, :] == experts, 1.0, 0.0)
    before = lax.broadcasted_iota(jnp.int32, (tok, tok), 0) < lax.broadcasted_iota(jnp.int32, (tok, tok), 1)
    ranks = jnp.dot(named.astype(BF16), before.astype(F32).astype(BF16), preferred_element_type=F32)
    for k in range(8):
        rank = jnp.sum(jnp.where(ids[k:k + 1, :] == experts, ranks, 0.0), axis=0, keepdims=True)
        meta[0, k:k + 1, 0:tok] = ids[k:k + 1, :] * float(most) + rank
    meta[0, :, tok:2 * tok] = weights

    pl.semaphore_wait(barrier, 6)
    load_tok.wait()

    first, second = pl.ds(0, half), pl.ds(half, half)
    quarters = [pl.ds(q * quarter, quarter) for q in range(4)]

    def move(kind, leaves, way, slot, cols, with_meta=False):
        dx, dy = slot
        shift = {"xp": (3, 0), "xm": (1, 0), "yp": (0, 3), "ym": (0, 1)}[way]
        to = ((dx + shift[0]) % 4, (dy + shift[1]) % 4)
        send(way, gath.at[dx, dy, :, cols], gath.at[to[0], to[1], :, cols], leaves, kind)
        if with_meta:
            send(way, meta.at[4 * dx + dy], meta.at[4 * to[0] + to[1]], "meta", "m" + kind)

    def own_first():
        for way in ("xp", "xm"):
            move("own", "own", way, (0, 0), first, True)
        for way in ("yp", "ym"):
            move("own", "own", way, (0, 0), second, True)

    def own_second():
        for way in ("yp", "ym"):
            move("pass0", "own", way, (0, 0), first)
        for way in ("xp", "xm"):
            move("pass0", "own", way, (0, 0), second)

    def own_relay():
        move("far", "pass", "xp", (3, 0), quarters[0], True)
        move("far", "pass", "xm", (1, 0), quarters[1])
        move("far", "pass", "yp", (0, 3), quarters[2], True)
        move("far", "pass", "ym", (0, 1), quarters[3])

    def passes(d):
        e = (4 - d) % 4
        move(f"pass{d}", "pass", "ym", (d, 0), first, d > 1)
        move(f"pass{d}", "second", "xm", (0, d), second, d < 3)
        move(f"pass{d}", "pass", "yp", (e, 0), first, d > 1)
        move(f"pass{d}", "second", "xp", (0, e), second, d < 3)

    def relays(d):
        move(f"relay{d}", "relay", "yp", (d, 3), quarters[0])
        move(f"relay{d}", "relay", "ym", (d, 1), quarters[1], d == 2)
        move(f"relay{d}", "relay", "xp", (3, d), quarters[2])
        move(f"relay{d}", "relay", "xm", (1, d), quarters[3])

    def got_own():
        wait("own", gath.at[0, 0:2])
        wait("mown", meta.at[pl.ds(0, 4)])

    def got_far():
        wait("far", gath.at[0, 0])
        wait("mfar", meta.at[pl.ds(0, 2)])

    def got_passes(d):
        wait(f"pass{d}", gath.at[0, 0:2])
        if d:
            wait(f"mpass{d}", meta.at[pl.ds(0, 4 if d == 2 else 2)])

    def got_relays(d):
        wait(f"relay{d}", gath.at[0, 0])
        if d == 2:
            wait("mrelay2", meta.at[0])

    place_row = lax.broadcasted_iota(jnp.int32, (2 * most, tok), 0)
    wanted = jnp.where(place_row < most, ep * most + place_row, (other - 1) * most + place_row).astype(F32)

    def build(dx, dy):
        place = PLACE[dx, dy]
        one, scaled = jnp.zeros((2 * most, tok), F32), jnp.zeros((2 * most, tok), F32)
        routes = meta[4 * dx + dy]
        codes, shares_of = routes[:, 0:tok], routes[:, tok:2 * tok]
        for k in range(8):
            hit = codes[k:k + 1, :] == wanted
            one = one + jnp.where(hit, 1.0, 0.0)
            scaled = scaled + jnp.where(hit, shares_of[k:k + 1, :], 0.0)
        comb[place] = scaled.T.astype(BF16)
        picks[place] = one.astype(BF16)

    def ways_out(place):
        if place == 16:
            return (("zp", pl.ds(0, most // 2)), ("zm", pl.ds(most // 2, most // 2)))
        return (("zm" if place % 2 else "zp", pl.ds(0, most)),)

    def select(dx, dy):
        place = PLACE[dx, dy]
        rows = most if place < 5 else 2 * most

        @pl.loop(0, 4, unroll=4)
        def _(q):
            cols = pl.ds(pl.multiple_of(q * quarter, quarter), quarter)
            chosen = jnp.dot(picks[place, :rows], gath[dx, dy, :, cols], preferred_element_type=F32).astype(BF16)
            xown[place, :, cols] = chosen[:most]
            if place >= 5:
                zsend[place, :, cols] = chosen[most:]

        if place >= 5:
            group = min((place - 6) // 4, 2)
            for way, rows in ways_out(place):
                send(way, zsend.at[place, rows], zrecv.at[place, rows], "rows", f"rows{group}")

    def select_all(*slots):
        for slot in slots:
            build(*slot)
            select(*slot)

    def got_rows(group):
        wait(f"rows{group}", zrecv.at[pl.ds(0, (4, 4, 3)[group])])

    near_experts = (ep, at(lax.rem(x + 1, 4), y, z_lo), at(lax.rem(x + 3, 4), y, z_lo), at(x, lax.rem(y + 1, 4), z_lo), at(x, lax.rem(y + 3, 4), z_lo))

    def select_foreign():
        routes = fmeta[...]
        codes, shares_of = routes[:, 0:tok], routes[:, tok:2 * tok]
        for i, expert in enumerate(near_experts):
            row = (expert * most + lax.broadcasted_iota(jnp.int32, (most, tok), 0)).astype(F32)
            one, scaled = jnp.zeros((most, tok), F32), jnp.zeros((most, tok), F32)
            for k in range(8):
                hit = codes[k:k + 1, :] == row
                one = one + jnp.where(hit, 1.0, 0.0)
                scaled = scaled + jnp.where(hit, shares_of[k:k + 1, :], 0.0)
            fcomb[i] = scaled.T.astype(BF16)
            fpick[i * most:(i + 1) * most, :] = one.astype(BF16)

        @pl.loop(0, 4, unroll=4)
        def _(q):
            cols = pl.ds(pl.multiple_of(q * quarter, quarter), quarter)
            chosen = jnp.dot(fpick[...], fgath[:, cols], preferred_element_type=F32).astype(BF16)
            zrecv[0, :, cols] = chosen[:most]
            for i in range(4):
                fsend[i, :, cols] = chosen[(i + 1) * most:(i + 2) * most]

    def send_near():
        for i, (way, slot) in enumerate((("xp", (3, 0)), ("xm", (1, 0)), ("yp", (0, 3)), ("ym", (0, 1)))):
            send(way, fsend.at[i], zrecv.at[PLACE[slot]], "near", "near")

    def back_near():
        for place, way in NEAR.items():
            index = ("xm", "xp", "ym", "yp").index(way)
            send(way, zout.at[place // 2, place % 2], frecv.at[index], "nearback", "nearback")

    def sum_near():
        wait("nearback", frecv)

        @pl.loop(0, 4, unroll=4)
        def _(q):
            cols = pl.ds(pl.multiple_of(q * quarter, quarter), quarter)
            total = jnp.dot(fcomb[0], zout[0, 0, :, cols], preferred_element_type=F32)
            for i in range(4):
                total = total + jnp.dot(fcomb[i + 1], frecv[i, :, cols], preferred_element_type=F32)
            fsum[:, cols] = total.astype(BF16)

        send("zp", fsum, zsum, "sum", "sum")

    tile = 256

    def gate_up(rows_ref, hidden, place, places, start=0, stop=hid // tile):
        rows = places * most

        @pl.loop(start, stop, unroll=stop - start)
        def _(n):
            cols = pl.ds(pl.multiple_of(n * tile, tile), tile)
            block = rows_ref[place:place + places].reshape(rows, width)
            gate = jnp.dot(block, wg[:, cols], preferred_element_type=F32)
            up = jnp.dot(block, wu[:, cols], preferred_element_type=F32)
            hidden[place * most:place * most + rows, cols] = (gate / (1.0 + jnp.exp(-gate)) * up).astype(BF16)

    starts = [sum(PARTS[:c]) * width // sum(PARTS) for c in range(len(PARTS) + 1)]

    def chunk_cols(c):
        return pl.ds(starts[c], starts[c + 1] - starts[c])

    def sides(c):
        middle = (starts[c] + starts[c + 1]) // 2
        return pl.ds(starts[c], middle - starts[c]), pl.ds(middle, starts[c + 1] - middle)

    top, low = pl.ds(0, tok // 2), pl.ds(tok // 2, tok // 2)

    def early_own():
        for q in range(4):
            out = jnp.dot(hown[0:5 * most, :], wd[:, quarters[q]], preferred_element_type=F32).astype(BF16)
            for slot, place in PLACE.items():
                if place < 5:
                    part[slot[0], slot[1], :, quarters[q]] = jnp.dot(
                        comb[place, :, :most], out[most * place:most * (place + 1)], preferred_element_type=F32
                    ).astype(BF16)
        for c in range(len(PARTS)):
            left, right = sides(c)
            esend[0, :, early_cols(c)] = part[0, 1, low, left]
            esend[1, :, early_cols(c)] = part[0, 3, top, left]
            esend[2, :, early_cols(c)] = part[1, 0, low, right]
            esend[3, :, early_cols(c)] = part[3, 0, top, right]

    def early_cols(c):
        return pl.ds(starts[c] // 2, (starts[c + 1] - starts[c]) // 2)

    def send_early():
        for i, way in enumerate(("yp", "ym", "xp", "xm")):
            send(way, esend.at[i], erecv.at[i], "early", "early")

    own_first()
    own_second()
    send("zm", gath.at[0, 0], fgath, "whole", "whole")
    send("zm", meta.at[0], fmeta, "mwhole", "mwhole")
    select_all((0, 0))
    got_own()
    passes(1)
    own_relay()
    passes(3)
    for slot in CLUSTER[1:]:
        build(*slot)
    got_passes(0)
    relays(0)
    for slot in CLUSTER[1:]:
        select(*slot)
    wait("whole", fgath)
    wait("mwhole", fmeta)
    select_foreign()
    for load in loads:
        load.wait()
    gate_up(xown, hown, 0, 5, 0, 2)
    got_passes(1)
    select_all((1, 1), (3, 3))
    got_far()
    passes(2)
    gate_up(xown, hown, 0, 5, 2, 3)
    early_own()
    got_passes(3)
    relays(1)
    relays(3)
    select_all((1, 3), (3, 1))
    got_relays(0)
    select_all((0, 2), (2, 0))
    gate_up(xown, hown, 6, 6, 0, 1)
    got_passes(2)
    relays(2)
    send_near()
    send_early()
    gate_up(xown, hown, 6, 6, 1, 3)
    got_relays(1)
    select_all((1, 2), (2, 1))
    got_relays(3)
    select_all((3, 2), (2, 3))
    got_rows(0)
    gate_up(zrecv, hz, 6, 4)
    got_relays(2)
    select_all((2, 2))

    def quarter_chunks(q):
        return [c for c in range(len(PARTS)) if q * quarter <= starts[c] < (q + 1) * quarter]

    def down_z(part_of, q):
        place, places = ((6, 8), (14, 3))[part_of]
        rows = hz[most * place:most * (place + places), :]
        out = jnp.dot(rows, wd[:, quarters[q]], preferred_element_type=F32).astype(BF16)
        for i in range(places):
            zout[(place + i) // 2, (place + i) % 2, :, quarters[q]] = out[most * i:most * (i + 1)]
        for c in quarter_chunks(q):
            cols, kind = chunk_cols(c), f"back{part_of}{c}"
            if part_of == 0:
                for side, way in ((0, "zm"), (1, "zp")):
                    pairs = pl.ds(place // 2, places // 2)
                    send(way, zout.at[pairs, side, :, cols], both.at[pairs, side, pl.ds(most, most), cols], "back", kind)
            else:
                for i in range(places):
                    pair, side = (place + i) // 2, (place + i) % 2
                    for way, rows in ways_out(place + i):
                        to = pl.ds(most + rows.start, rows.size)
                        send(OPPOSITE[way], zout.at[pair, side, rows, cols], both.at[pair, side, to, cols], "back", kind)

    def down_near():
        @pl.loop(0, 4, unroll=4)
        def _(q):
            cols = pl.ds(pl.multiple_of(q * quarter, quarter), quarter)
            out = jnp.dot(hz[0:5 * most, :], wd[:, cols], preferred_element_type=F32).astype(BF16)
            for i in range(5):
                zout[i // 2, i % 2, :, cols] = out[most * i:most * (i + 1)]

        back_near()

    def down_own(q):
        rows = hown[6 * most:17 * most, :]
        out = jnp.dot(rows, wd[:, quarters[q]], preferred_element_type=F32).astype(BF16)
        for place in range(6, 17):
            both[place // 2, place % 2, 0:most, quarters[q]] = out[most * (place - 6):most * (place - 5)]

    def serve_own():
        gate_up(xown, hown, 12, 5)

    def serve_near():
        wait("near", zrecv.at[pl.ds(0, 4)])
        gate_up(zrecv, hz, 0, 5)

    def serve_early():
        got_rows(1)
        gate_up(zrecv, hz, 10, 4)

    def serve_late():
        got_rows(2)
        gate_up(zrecv, hz, 14, 3)

    def fill(c, *slots):
        cols = chunk_cols(c)
        for dx, dy in slots:
            place = PLACE[dx, dy]
            part[dx, dy, :, cols] = jnp.dot(
                comb[place], both[place // 2, place % 2, :, cols], preferred_element_type=F32
            ).astype(BF16)

    late = ((3, 2), (2, 3), (2, 2))

    def halves_one(c, pair):
        left, right = sides(c)
        send("yp", part.at[pair, 2, top, left], r1p.at[pair, :, left], "1p", f"1{c}")
        send("ym", part.at[pair, 2, low, left], r1m.at[pair, :, left], "1m", f"1{c}")
        send("xp", part.at[2, pair, top, right], r1p.at[pair, :, right], "1p", f"1{c}")
        send("xm", part.at[2, pair, low, right], r1m.at[pair, :, right], "1m", f"1{c}")

    def expand(c):
        left, right = sides(c)
        wait(f"back0{c}", zrecv.at[pl.ds(0, 8), :, chunk_cols(c)])
        fill(c, (0, 2), (1, 2), (2, 0), (2, 1))
        halves_one(c, pl.ds(0, 2))
        fill(c, (1, 1), (3, 3), (1, 3), (3, 1))
        send("yp", part.at[pl.ds(1, 3), 1, low, left], r2p.at[pl.ds(1, 3), low, left], "2p", f"2{c}")
        send("xp", part.at[1, pl.ds(1, 3), low, right], r2p.at[pl.ds(1, 3), low, right], "2p", f"2{c}")
        send("ym", part.at[1, 3, top, left], r2m.at[1, top, left], "2m", f"2{c}")
        send("xm", part.at[3, 1, top, right], r2m.at[1, top, right], "2m", f"2{c}")

    def expand_late(c):
        left, right = sides(c)
        wait(f"back1{c}", zrecv.at[pl.ds(0, 3), :, chunk_cols(c)])
        fill(c, *late)
        halves_one(c, pl.ds(2, 2))
        send("ym", part.at[pl.ds(2, 2), 3, top, left], r2m.at[pl.ds(2, 2), top, left], "2m", f"2{c}")
        send("xm", part.at[3, pl.ds(2, 2), top, right], r2m.at[pl.ds(2, 2), top, right], "2m", f"2{c}")

    def halves_two(c, plus, minus):
        left, right = sides(c)
        send("yp", part.at[:, 1, plus, left], r2p.at[:, plus, left], "2p", f"2{c}")
        send("ym", part.at[:, 3, minus, left], r2m.at[:, minus, left], "2m", f"2{c}")
        send("xp", part.at[1, :, plus, right], r2p.at[:, plus, right], "2p", f"2{c}")
        send("xm", part.at[3, :, minus, right], r2m.at[:, minus, right], "2m", f"2{c}")

    def halves_five(c, plus, minus):
        left, right = sides(c)
        send("xp", part.at[1, 0, plus, left], r5p.at[plus, left], "5p", f"5{c}")
        send("xm", part.at[3, 0, minus, left], r5m.at[minus, left], "5m", f"5{c}")
        send("yp", part.at[0, 1, plus, right], r5p.at[plus, right], "5p", f"5{c}")
        send("ym", part.at[0, 3, minus, right], r5m.at[minus, right], "5m", f"5{c}")

    def double(c):
        return pl.ds(0, 2 * chunk_cols(c).size)

    def add(dx, dy, rows, cols, *refs):
        total = part[dx, dy, rows, cols].astype(F32)
        for ref in refs:
            total = total + ref[...].astype(F32)
        part[dx, dy, rows, cols] = total.astype(BF16)

    every = pl.ds(0, tok)

    def step_two(c):
        left, right = sides(c)
        wait(f"1{c}", r1p.at[:, :, double(c)])
        for d in range(4):
            add(d, 1, top, left, r1p.at[d, :, left])
            add(d, 3, low, left, r1m.at[d, :, left])
            add(1, d, top, right, r1p.at[d, :, right])
            add(3, d, low, right, r1m.at[d, :, right])
        halves_two(c, top, low)

    got = []

    def step_three(c):
        left, right = sides(c)
        wait(f"2{c}", both.at[pl.ds(0, 7), 0, :, chunk_cols(c)])
        if "early" not in got:
            got.append("early")
            wait("early", erecv)
        for d in (2, 1, 3, 0):
            if d == 0:
                for cols, plus, minus in ((left, 0, 1), (right, 2, 3)):
                    add(0, 0, top, cols, r2p.at[0, top, cols], erecv.at[minus, :, early_cols(c)])
                    add(0, 0, low, cols, erecv.at[plus, :, early_cols(c)], r2m.at[0, low, cols])
                continue
            add(d, 0, every, left, r2p.at[d, :, left], r2m.at[d, :, left])
            add(0, d, every, right, r2p.at[d, :, right], r2m.at[d, :, right])
            if d == 2:
                send("xp", part.at[2, 0, top, left], r4p.at[:, left], "4p", f"4{c}")
                send("xm", part.at[2, 0, low, left], r4m.at[:, left], "4m", f"4{c}")
                send("yp", part.at[0, 2, top, right], r4p.at[:, right], "4p", f"4{c}")
                send("ym", part.at[0, 2, low, right], r4m.at[:, right], "4m", f"4{c}")
            if d == 3:
                halves_five(c, low, top)

    def step_four(c):
        left, right = sides(c)
        wait(f"4{c}", r4p.at[:, double(c)])
        add(1, 0, top, left, r4p.at[:, left])
        add(3, 0, low, left, r4m.at[:, left])
        add(0, 1, top, right, r4p.at[:, right])
        add(0, 3, low, right, r4m.at[:, right])
        halves_five(c, top, low)

    stores = []


    def step_five(c):
        wait(f"5{c}", r5p.at[:, double(c)])
        if not stores:
            wait("sum", zsum)
        for cols in sides(c):
            total = part[0, 0, :, cols].astype(F32) + zsum[:, cols].astype(F32) + r5p[:, cols].astype(F32) + r5m[:, cols].astype(F32)
            outv[:, cols] = total.astype(BF16)
        cols = chunk_cols(c)
        store = pltpu.make_async_copy(outv.at[:, cols], out_hbm.at[:, cols], local_sem.at[4])
        store.start()
        stores.append(c)

    def drain_all(c=0):
        drain("own", gath.at[0])
        drain("pass", gath.at[0])
        drain("second", gath.at[0, 0:3])
        drain("relay", gath.at[0])
        drain("meta", meta.at[pl.ds(0, 15)])
        for kind in ("rows", "back"):
            drain(kind, zsend.at[pl.ds(0, 11)])
        for kind in ("near", "nearback"):
            drain(kind, frecv)
        drain("whole", fgath)
        drain("mwhole", fmeta)
        drain("sum", fsum)
        drain("early", esend)
        for kind, like in (("1p", r1p), ("1m", r1m), ("4p", r4p), ("4m", r4m)):
            drain(kind, like)
        for kind in ("2p", "2m"):
            drain(kind, both.at[pl.ds(0, 7), 0, :, first])

    whole = {"O3": serve_own, "N": serve_near, "Z": serve_early, "L": serve_late, "DN": down_near, "F": sum_near, "X": drain_all}
    chunked = {
        "a": functools.partial(down_z, 0), "b": functools.partial(down_z, 1), "W": down_own, "G": expand, "E": expand_late,
        "A": step_two, "B": step_three, "C": step_four, "D": step_five,
    }
    for step in STEPS:
        if step in whole:
            whole[step]()
        else:
            chunked[step[0]](int(step[1]))
    assert (len(leaving), len(landing)) == (LEAVING, LANDING), (len(leaving), len(landing))
    drain("5p", r5p)
    drain("5m", r5m)
    pltpu.make_async_copy(outv, out_hbm, local_sem.at[4]).wait()


def shards(n_hi, tokens, expert_ids, gate_probs, w_gate, w_up, w_down):
    tok, width = tokens.shape
    hid = w_gate.shape[2]
    most = 32
    vmem = pl.BlockSpec(memory_space=pltpu.VMEM)
    hbm = pl.BlockSpec(memory_space=pl.ANY)
    return pl.pallas_call(
        functools.partial(kernel, (n_hi, tok, width, hid, most)),
        out_shape=jax.ShapeDtypeStruct((tok, width), BF16),
        in_specs=[hbm, vmem, vmem, hbm, hbm, hbm],
        out_specs=hbm,
        scratch_shapes=[
            pltpu.VMEM((4, 4, tok, width), BF16),
            pltpu.VMEM((16, 8, 128), F32),
            pltpu.VMEM((PLACES, tok, 2 * most), BF16),
            pltpu.VMEM((PLACES, most, width), BF16),
            pltpu.VMEM((PLACES, most, width), BF16),
            pltpu.VMEM((PLACES, most, width), BF16),
            pltpu.VMEM((PLACES * most, hid), BF16),
            pltpu.VMEM((PLACES * most, hid), BF16),
            pltpu.VMEM((width, hid), BF16),
            pltpu.VMEM((width, hid), BF16),
            pltpu.VMEM((hid, width), BF16),
            pltpu.VMEM((PLACES // 2, 2, most, width), BF16),
            pltpu.VMEM((PLACES // 2, 2, 2 * most, width), BF16),
            pltpu.VMEM((4, 4, tok, width), BF16),
            pltpu.VMEM((PLACES, 2 * most, tok), BF16),
            pltpu.VMEM((tok, width), BF16),
            pltpu.VMEM((8, 128), F32),
            pltpu.VMEM((5, tok, most), BF16),
            pltpu.VMEM((5 * most, tok), BF16),
            pltpu.VMEM((4, most, width), BF16),
            pltpu.VMEM((4, most, width), BF16),
            pltpu.VMEM((tok, width), BF16),
            pltpu.VMEM((tok, width), BF16),
            pltpu.VMEM((4, tok // 2, width // 2), BF16),
            pltpu.VMEM((4, tok // 2, width // 2), BF16),
            pltpu.VMEM((4, tok // 2, width), BF16),
            pltpu.VMEM((4, tok // 2, width), BF16),
            pltpu.VMEM((4, tok, width), BF16),
            pltpu.VMEM((4, tok, width), BF16),
            pltpu.VMEM((tok // 2, width), BF16),
            pltpu.VMEM((tok // 2, width), BF16),
            pltpu.VMEM((tok, width), BF16),
            pltpu.VMEM((tok, width), BF16),
            pltpu.VMEM((tok, width), BF16),
            pltpu.SemaphoreType.DMA((LEAVING,)),
            pltpu.SemaphoreType.DMA((LANDING,)),
            pltpu.SemaphoreType.DMA((5,)),
        ],
        compiler_params=pltpu.CompilerParams(
            collective_id=0, has_side_effects=True, vmem_limit_bytes=60 * 1024 * 1024
        ),
        name="routed_experts",
    )(tokens, expert_ids.T, gate_probs.T, w_gate, w_up, w_down)


def solution(mesh):
    placed = (
        P(("dp", "ep"), None),
        P(("dp", "ep"), None),
        P(("dp", "ep"), None),
        P("ep", None, None),
        P("ep", None, None),
        P("ep", None, None),
    )
    return jax.shard_map(
        functools.partial(shards, mesh.shape["dp"] // 2), mesh=mesh, in_specs=placed,
        out_specs=P(("dp", "ep"), None), check_vma=False,
    )
```

```python
import functools

import jax
import jax.numpy as jnp
from jax import lax
from jax.experimental import pallas as pl
from jax.experimental.pallas import tpu as pltpu
from jax.sharding import PartitionSpec as P

MESH = pl.DeviceIdType.MESH
F32, BF16 = jnp.float32, jnp.bfloat16
OPPOSITE = {"xp": "xm", "xm": "xp", "yp": "ym", "ym": "yp", "zp": "zm", "zm": "zp"}

CLUSTER = [(0, 0), (1, 0), (3, 0), (0, 1), (0, 3)]
OTHERS = [(1, 1), (3, 3), (1, 3), (3, 1), (0, 2), (2, 0), (1, 2), (2, 1), (3, 2), (2, 3), (2, 2)]
PLACE = {slot: place for place, slot in enumerate(CLUSTER + [None] + OTHERS) if slot}
PLACES = 18
NEAR = {1: "xp", 2: "xm", 3: "yp", 4: "ym"}
PARTS = (1,) * 8
STEPS = (
    "O3", "Z", "a3", "W3", "a1", "N", "DN", "L", "W2", "G6", "W1", "b1", "b3", "a0", "G7", "W0", "G2", "G3", "E2",
    "b0", "E3", "E6", "b2", "a2", "E7", "G0", "A2", "A3", "G1", "E0", "A7", "A6", "E1", "G4", "E4", "F", "G5", "E5",
    "A1", "A0", "A4", "B7", "A5", "B2", "B1", "B6", "B0", "B3", "B4", "B5", "C7", "C1", "C0", "C2", "C6", "C4", "C3",
    "C5", "X", "D4", "D0", "D3", "D1", "D6", "D7", "D2", "D5",
)
LEAVING, LANDING = 21, 73


def kernel(
    sizes, tok_hbm, routes_ref, wg_hbm, wu_hbm, wd_hbm, out_hbm,
    gath, meta, comb, xown, zsend, zrecv, hown, hz, wg, wu, wd, zout, both, part, picks,
    fgath, fmeta, fcomb, fpick, fsend, frecv, fsum, zsum, esend, erecv,
    r1p, r1m, r2p, r2m, r4p, r4m, r5p, r5m, outv,
    send_sem, recv_sem, local_sem,
):
    n_hi, tok, width, hid, most = sizes
    half, quarter = width // 2, width // 4
    ep, dp = lax.axis_index("ep"), lax.axis_index("dp")
    x, y, z_lo = lax.rem(ep, 4), lax.rem(ep // 4, 4), ep // 16
    z_hi, core = dp // 2, lax.rem(dp, 2)

    def at(xx, yy, zz):
        return zz * 16 + yy * 4 + xx

    cross = 1 - core
    here = z_hi * 2 + cross
    z_up = lax.rem(z_hi + z_lo, n_hi) * 2 + cross
    z_down = lax.rem(z_hi + z_lo + n_hi - 1, n_hi) * 2 + cross
    target = {
        "xp": {"ep": at(lax.rem(x + 1, 4), y, z_lo), "dp": here},
        "xm": {"ep": at(lax.rem(x + 3, 4), y, z_lo), "dp": here},
        "yp": {"ep": at(x, lax.rem(y + 1, 4), z_lo), "dp": here},
        "ym": {"ep": at(x, lax.rem(y + 3, 4), z_lo), "dp": here},
        "zp": {"ep": at(x, y, 1 - z_lo), "dp": z_up},
        "zm": {"ep": at(x, y, 1 - z_lo), "dp": z_down},
    }
    other = at(x, y, 1 - z_lo)

    leaving, landing = {}, {}

    def sem(array, kinds, kind):
        return array.at[kinds.setdefault(kind, len(kinds))]

    def send(way, src, dst, leaves, lands):
        pltpu.make_async_remote_copy(
            src_ref=src, dst_ref=dst, send_sem=sem(send_sem, leaving, leaves), recv_sem=sem(recv_sem, landing, lands),
            device_id=target[way], device_id_type=MESH,
        ).start()

    def wait(lands, *like):
        pltpu.make_async_copy(*like, *like, sem(recv_sem, landing, lands)).wait()

    def drain(leaves, like):
        pltpu.make_async_copy(like, like, sem(send_sem, leaving, leaves)).wait()

    barrier = pltpu.get_barrier_semaphore()
    for way in target:
        pl.semaphore_signal(barrier, inc=1, device_id=target[way], device_id_type=MESH)

    load_tok = pltpu.make_async_copy(tok_hbm, gath.at[0, 0], local_sem.at[0])
    load_tok.start()
    loads = [
        pltpu.make_async_copy(src.at[0], dst, local_sem.at[1 + i])
        for i, (src, dst) in enumerate(((wg_hbm, wg), (wu_hbm, wu), (wd_hbm, wd)))
    ]
    for load in loads:
        load.start()

    ids = jnp.floor(routes_ref[...] * 0.5)
    probs = routes_ref[...] - 2.0 * ids
    weights = probs / jnp.sum(probs, axis=0, keepdims=True)
    experts = lax.broadcasted_iota(jnp.int32, (32, tok), 0).astype(F32)
    named = jnp.zeros((32, tok), F32)
    for k in range(8):
        named = named + jnp.where(ids[k:k + 1, :] == experts, 1.0, 0.0)
    before = lax.broadcasted_iota(jnp.int32, (tok, tok), 0) < lax.broadcasted_iota(jnp.int32, (tok, tok), 1)
    ranks = jnp.dot(named.astype(BF16), before.astype(F32).astype(BF16), preferred_element_type=F32)
    for k in range(8):
        rank = jnp.sum(jnp.where(ids[k:k + 1, :] == experts, ranks, 0.0), axis=0, keepdims=True)
        meta[0, k:k + 1, 0:tok] = ids[k:k + 1, :] * float(most) + rank
    meta[0, :, tok:2 * tok] = weights

    pl.semaphore_wait(barrier, 6)
    load_tok.wait()

    first, second = pl.ds(0, half), pl.ds(half, half)
    quarters = [pl.ds(q * quarter, quarter) for q in range(4)]

    def move(kind, leaves, way, slot, cols, with_meta=False):
        dx, dy = slot
        shift = {"xp": (3, 0), "xm": (1, 0), "yp": (0, 3), "ym": (0, 1)}[way]
        to = ((dx + shift[0]) % 4, (dy + shift[1]) % 4)
        send(way, gath.at[dx, dy, :, cols], gath.at[to[0], to[1], :, cols], leaves, kind)
        if with_meta:
            send(way, meta.at[4 * dx + dy], meta.at[4 * to[0] + to[1]], "meta", "m" + kind)

    def own_first():
        for way in ("xp", "xm"):
            move("own", "own", way, (0, 0), first, True)
        for way in ("yp", "ym"):
            move("own", "own", way, (0, 0), second, True)

    def own_second():
        for way in ("yp", "ym"):
            move("pass0", "own", way, (0, 0), first)
        for way in ("xp", "xm"):
            move("pass0", "own", way, (0, 0), second)

    def own_relay():
        move("far", "pass", "xp", (3, 0), quarters[0], True)
        move("far", "pass", "xm", (1, 0), quarters[1])
        move("far", "pass", "yp", (0, 3), quarters[2], True)
        move("far", "pass", "ym", (0, 1), quarters[3])

    def passes(d):
        e = (4 - d) % 4
        move(f"pass{d}", "pass", "ym", (d, 0), first, d > 1)
        move(f"pass{d}", "second", "xm", (0, d), second, d < 3)
        move(f"pass{d}", "pass", "yp", (e, 0), first, d > 1)
        move(f"pass{d}", "second", "xp", (0, e), second, d < 3)

    def relays(d):
        move(f"relay{d}", "relay", "yp", (d, 3), quarters[0])
        move(f"relay{d}", "relay", "ym", (d, 1), quarters[1], d == 2)
        move(f"relay{d}", "relay", "xp", (3, d), quarters[2])
        move(f"relay{d}", "relay", "xm", (1, d), quarters[3])

    def got_own():
        wait("own", gath.at[0, 0:2])
        wait("mown", meta.at[pl.ds(0, 4)])

    def got_far():
        wait("far", gath.at[0, 0])
        wait("mfar", meta.at[pl.ds(0, 2)])

    def got_passes(d):
        wait(f"pass{d}", gath.at[0, 0:2])
        if d:
            wait(f"mpass{d}", meta.at[pl.ds(0, 4 if d == 2 else 2)])

    def got_relays(d):
        wait(f"relay{d}", gath.at[0, 0])
        if d == 2:
            wait("mrelay2", meta.at[0])

    place_row = lax.broadcasted_iota(jnp.int32, (2 * most, tok), 0)
    wanted = jnp.where(place_row < most, ep * most + place_row, (other - 1) * most + place_row).astype(F32)

    def build(dx, dy):
        place = PLACE[dx, dy]
        one, scaled = jnp.zeros((2 * most, tok), F32), jnp.zeros((2 * most, tok), F32)
        routes = meta[4 * dx + dy]
        codes, shares_of = routes[:, 0:tok], routes[:, tok:2 * tok]
        for k in range(8):
            hit = codes[k:k + 1, :] == wanted
            one = one + jnp.where(hit, 1.0, 0.0)
            scaled = scaled + jnp.where(hit, shares_of[k:k + 1, :], 0.0)
        comb[place] = scaled.T.astype(BF16)
        picks[place] = one.astype(BF16)

    def ways_out(place):
        if place == 16:
            return (("zp", pl.ds(0, most // 2)), ("zm", pl.ds(most // 2, most // 2)))
        return (("zm" if place % 2 else "zp", pl.ds(0, most)),)

    def select(dx, dy):
        place = PLACE[dx, dy]
        rows = most if place < 5 else 2 * most

        @pl.loop(0, 4, unroll=4)
        def _(q):
            cols = pl.ds(pl.multiple_of(q * quarter, quarter), quarter)
            chosen = jnp.dot(picks[place, :rows], gath[dx, dy, :, cols], preferred_element_type=F32).astype(BF16)
            xown[place, :, cols] = chosen[:most]
            if place >= 5:
                zsend[place, :, cols] = chosen[most:]

        if place >= 5:
            group = min((place - 6) // 4, 2)
            for way, rows in ways_out(place):
                send(way, zsend.at[place, rows], zrecv.at[place, rows], "rows", f"rows{group}")

    def select_all(*slots):
        for slot in slots:
            build(*slot)
            select(*slot)

    def got_rows(group):
        wait(f"rows{group}", zrecv.at[pl.ds(0, (4, 4, 3)[group])])

    near_experts = (ep, at(lax.rem(x + 1, 4), y, z_lo), at(lax.rem(x + 3, 4), y, z_lo), at(x, lax.rem(y + 1, 4), z_lo), at(x, lax.rem(y + 3, 4), z_lo))

    def select_foreign():
        routes = fmeta[...]
        codes, shares_of = routes[:, 0:tok], routes[:, tok:2 * tok]
        for i, expert in enumerate(near_experts):
            row = (expert * most + lax.broadcasted_iota(jnp.int32, (most, tok), 0)).astype(F32)
            one, scaled = jnp.zeros((most, tok), F32), jnp.zeros((most, tok), F32)
            for k in range(8):
                hit = codes[k:k + 1, :] == row
                one = one + jnp.where(hit, 1.0, 0.0)
                scaled = scaled + jnp.where(hit, shares_of[k:k + 1, :], 0.0)
            fcomb[i] = scaled.T.astype(BF16)
            fpick[i * most:(i + 1) * most, :] = one.astype(BF16)

        @pl.loop(0, 4, unroll=4)
        def _(q):
            cols = pl.ds(pl.multiple_of(q * quarter, quarter), quarter)
            chosen = jnp.dot(fpick[...], fgath[:, cols], preferred_element_type=F32).astype(BF16)
            zrecv[0, :, cols] = chosen[:most]
            for i in range(4):
                fsend[i, :, cols] = chosen[(i + 1) * most:(i + 2) * most]

    def send_near():
        for i, (way, slot) in enumerate((("xp", (3, 0)), ("xm", (1, 0)), ("yp", (0, 3)), ("ym", (0, 1)))):
            send(way, fsend.at[i], zrecv.at[PLACE[slot]], "near", "near")

    def back_near():
        for place, way in NEAR.items():
            index = ("xm", "xp", "ym", "yp").index(way)
            send(way, zout.at[place // 2, place % 2], frecv.at[index], "nearback", "nearback")

    def sum_near():
        wait("nearback", frecv)

        @pl.loop(0, 4, unroll=4)
        def _(q):
            cols = pl.ds(pl.multiple_of(q * quarter, quarter), quarter)
            total = jnp.dot(fcomb[0], zout[0, 0, :, cols], preferred_element_type=F32)
            for i in range(4):
                total = total + jnp.dot(fcomb[i + 1], frecv[i, :, cols], preferred_element_type=F32)
            fsum[:, cols] = total.astype(BF16)

        send("zp", fsum, zsum, "sum", "sum")

    tile = 256

    def gate_up(rows_ref, hidden, place, places, start=0, stop=hid // tile):
        rows = places * most

        @pl.loop(start, stop, unroll=stop - start)
        def _(n):
            cols = pl.ds(pl.multiple_of(n * tile, tile), tile)
            block = rows_ref[place:place + places].reshape(rows, width)
            gate = jnp.dot(block, wg[:, cols], preferred_element_type=F32)
            up = jnp.dot(block, wu[:, cols], preferred_element_type=F32)
            hidden[place * most:place * most + rows, cols] = (gate / (1.0 + jnp.exp(-gate)) * up).astype(BF16)

    starts = [sum(PARTS[:c]) * width // sum(PARTS) for c in range(len(PARTS) + 1)]

    def chunk_cols(c):
        return pl.ds(starts[c], starts[c + 1] - starts[c])

    def sides(c):
        middle = (starts[c] + starts[c + 1]) // 2
        return pl.ds(starts[c], middle - starts[c]), pl.ds(middle, starts[c + 1] - middle)

    top, low = pl.ds(0, tok // 2), pl.ds(tok // 2, tok // 2)

    def early_own():
        for q in range(4):
            out = jnp.dot(hown[0:5 * most, :], wd[:, quarters[q]], preferred_element_type=F32).astype(BF16)
            for slot, place in PLACE.items():
                if place < 5:
                    part[slot[0], slot[1], :, quarters[q]] = jnp.dot(
                        comb[place, :, :most], out[most * place:most * (place + 1)], preferred_element_type=F32
                    ).astype(BF16)
        for c in range(len(PARTS)):
            left, right = sides(c)
            esend[0, :, early_cols(c)] = part[0, 1, low, left]
            esend[1, :, early_cols(c)] = part[0, 3, top, left]
            esend[2, :, early_cols(c)] = part[1, 0, low, right]
            esend[3, :, early_cols(c)] = part[3, 0, top, right]

    def early_cols(c):
        return pl.ds(starts[c] // 2, (starts[c + 1] - starts[c]) // 2)

    def send_early():
        for i, way in enumerate(("yp", "ym", "xp", "xm")):
            send(way, esend.at[i], erecv.at[i], "early", "early")

    own_first()
    own_second()
    send("zm", gath.at[0, 0], fgath, "whole", "whole")
    send("zm", meta.at[0], fmeta, "mwhole", "mwhole")
    select_all((0, 0))
    got_own()
    passes(1)
    own_relay()
    passes(3)
    for slot in CLUSTER[1:]:
        build(*slot)
    got_passes(0)
    relays(0)
    for slot in CLUSTER[1:]:
        select(*slot)
    wait("whole", fgath)
    wait("mwhole", fmeta)
    select_foreign()
    for load in loads:
        load.wait()
    gate_up(xown, hown, 0, 5, 0, 2)
    got_passes(1)
    select_all((1, 1), (3, 3))
    got_far()
    passes(2)
    gate_up(xown, hown, 0, 5, 2, 3)
    early_own()
    got_passes(3)
    relays(1)
    relays(3)
    select_all((1, 3), (3, 1))
    got_relays(0)
    select_all((0, 2), (2, 0))
    gate_up(xown, hown, 6, 6, 0, 1)
    got_passes(2)
    relays(2)
    send_near()
    send_early()
    gate_up(xown, hown, 6, 6, 1, 3)
    got_relays(1)
    select_all((1, 2), (2, 1))
    got_relays(3)
    select_all((3, 2), (2, 3))
    got_rows(0)
    gate_up(zrecv, hz, 6, 4)
    got_relays(2)
    select_all((2, 2))

    def quarter_chunks(q):
        return [c for c in range(len(PARTS)) if q * quarter <= starts[c] < (q + 1) * quarter]

    def down_z(part_of, q):
        place, places = ((6, 8), (14, 3))[part_of]
        rows = hz[most * place:most * (place + places), :]
        out = jnp.dot(rows, wd[:, quarters[q]], preferred_element_type=F32).astype(BF16)
        for i in range(places):
            zout[(place + i) // 2, (place + i) % 2, :, quarters[q]] = out[most * i:most * (i + 1)]
        for c in quarter_chunks(q):
            cols, kind = chunk_cols(c), f"back{part_of}{c}"
            if part_of == 0:
                for side, way in ((0, "zm"), (1, "zp")):
                    pairs = pl.ds(place // 2, places // 2)
                    send(way, zout.at[pairs, side, :, cols], both.at[pairs, side, pl.ds(most, most), cols], "back", kind)
            else:
                for i in range(places):
                    pair, side = (place + i) // 2, (place + i) % 2
                    for way, rows in ways_out(place + i):
                        to = pl.ds(most + rows.start, rows.size)
                        send(OPPOSITE[way], zout.at[pair, side, rows, cols], both.at[pair, side, to, cols], "back", kind)

    def down_near():
        @pl.loop(0, 4, unroll=4)
        def _(q):
            cols = pl.ds(pl.multiple_of(q * quarter, quarter), quarter)
            out = jnp.dot(hz[0:5 * most, :], wd[:, cols], preferred_element_type=F32).astype(BF16)
            for i in range(5):
                zout[i // 2, i % 2, :, cols] = out[most * i:most * (i + 1)]

        back_near()

    def down_own(q):
        rows = hown[6 * most:17 * most, :]
        out = jnp.dot(rows, wd[:, quarters[q]], preferred_element_type=F32).astype(BF16)
        for place in range(6, 17):
            both[place // 2, place % 2, 0:most, quarters[q]] = out[most * (place - 6):most * (place - 5)]

    def serve_own():
        gate_up(xown, hown, 12, 5)

    def serve_near():
        wait("near", zrecv.at[pl.ds(0, 4)])
        gate_up(zrecv, hz, 0, 5)

    def serve_early():
        got_rows(1)
        gate_up(zrecv, hz, 10, 4)

    def serve_late():
        got_rows(2)
        gate_up(zrecv, hz, 14, 3)

    def fill(c, *slots):
        cols = chunk_cols(c)
        for dx, dy in slots:
            place = PLACE[dx, dy]
            part[dx, dy, :, cols] = jnp.dot(
                comb[place], both[place // 2, place % 2, :, cols], preferred_element_type=F32
            ).astype(BF16)

    late = ((3, 2), (2, 3), (2, 2))

    def halves_one(c, pair):
        left, right = sides(c)
        send("yp", part.at[pair, 2, top, left], r1p.at[pair, :, left], "1p", f"1{c}")
        send("ym", part.at[pair, 2, low, left], r1m.at[pair, :, left], "1m", f"1{c}")
        send("xp", part.at[2, pair, top, right], r1p.at[pair, :, right], "1p", f"1{c}")
        send("xm", part.at[2, pair, low, right], r1m.at[pair, :, right], "1m", f"1{c}")

    def expand(c):
        left, right = sides(c)
        wait(f"back0{c}", zrecv.at[pl.ds(0, 8), :, chunk_cols(c)])
        fill(c, (0, 2), (1, 2), (2, 0), (2, 1))
        halves_one(c, pl.ds(0, 2))
        fill(c, (1, 1), (3, 3), (1, 3), (3, 1))
        send("yp", part.at[pl.ds(1, 3), 1, low, left], r2p.at[pl.ds(1, 3), low, left], "2p", f"2{c}")
        send("xp", part.at[1, pl.ds(1, 3), low, right], r2p.at[pl.ds(1, 3), low, right], "2p", f"2{c}")
        send("ym", part.at[1, 3, top, left], r2m.at[1, top, left], "2m", f"2{c}")
        send("xm", part.at[3, 1, top, right], r2m.at[1, top, right], "2m", f"2{c}")

    def expand_late(c):
        left, right = sides(c)
        wait(f"back1{c}", zrecv.at[pl.ds(0, 3), :, chunk_cols(c)])
        fill(c, *late)
        halves_one(c, pl.ds(2, 2))
        send("ym", part.at[pl.ds(2, 2), 3, top, left], r2m.at[pl.ds(2, 2), top, left], "2m", f"2{c}")
        send("xm", part.at[3, pl.ds(2, 2), top, right], r2m.at[pl.ds(2, 2), top, right], "2m", f"2{c}")

    def halves_two(c, plus, minus):
        left, right = sides(c)
        send("yp", part.at[:, 1, plus, left], r2p.at[:, plus, left], "2p", f"2{c}")
        send("ym", part.at[:, 3, minus, left], r2m.at[:, minus, left], "2m", f"2{c}")
        send("xp", part.at[1, :, plus, right], r2p.at[:, plus, right], "2p", f"2{c}")
        send("xm", part.at[3, :, minus, right], r2m.at[:, minus, right], "2m", f"2{c}")

    def halves_five(c, plus, minus):
        left, right = sides(c)
        send("xp", part.at[1, 0, plus, left], r5p.at[plus, left], "5p", f"5{c}")
        send("xm", part.at[3, 0, minus, left], r5m.at[minus, left], "5m", f"5{c}")
        send("yp", part.at[0, 1, plus, right], r5p.at[plus, right], "5p", f"5{c}")
        send("ym", part.at[0, 3, minus, right], r5m.at[minus, right], "5m", f"5{c}")

    def double(c):
        return pl.ds(0, 2 * chunk_cols(c).size)

    def add(dx, dy, rows, cols, *refs):
        total = part[dx, dy, rows, cols].astype(F32)
        for ref in refs:
            total = total + ref[...].astype(F32)
        part[dx, dy, rows, cols] = total.astype(BF16)

    every = pl.ds(0, tok)

    def step_two(c):
        left, right = sides(c)
        wait(f"1{c}", r1p.at[:, :, double(c)])
        for d in range(4):
            add(d, 1, top, left, r1p.at[d, :, left])
            add(d, 3, low, left, r1m.at[d, :, left])
            add(1, d, top, right, r1p.at[d, :, right])
            add(3, d, low, right, r1m.at[d, :, right])
        halves_two(c, top, low)

    got = []

    def step_three(c):
        left, right = sides(c)
        wait(f"2{c}", both.at[pl.ds(0, 7), 0, :, chunk_cols(c)])
        if "early" not in got:
            got.append("early")
            wait("early", erecv)
        for d in (2, 1, 3, 0):
            if d == 0:
                for cols, plus, minus in ((left, 0, 1), (right, 2, 3)):
                    add(0, 0, top, cols, r2p.at[0, top, cols], erecv.at[minus, :, early_cols(c)])
                    add(0, 0, low, cols, erecv.at[plus, :, early_cols(c)], r2m.at[0, low, cols])
                continue
            add(d, 0, every, left, r2p.at[d, :, left], r2m.at[d, :, left])
            add(0, d, every, right, r2p.at[d, :, right], r2m.at[d, :, right])
            if d == 2:
                send("xp", part.at[2, 0, top, left], r4p.at[:, left], "4p", f"4{c}")
                send("xm", part.at[2, 0, low, left], r4m.at[:, left], "4m", f"4{c}")
                send("yp", part.at[0, 2, top, right], r4p.at[:, right], "4p", f"4{c}")
                send("ym", part.at[0, 2, low, right], r4m.at[:, right], "4m", f"4{c}")
            if d == 3:
                halves_five(c, low, top)

    def step_four(c):
        left, right = sides(c)
        wait(f"4{c}", r4p.at[:, double(c)])
        add(1, 0, top, left, r4p.at[:, left])
        add(3, 0, low, left, r4m.at[:, left])
        add(0, 1, top, right, r4p.at[:, right])
        add(0, 3, low, right, r4m.at[:, right])
        halves_five(c, top, low)

    stores = []


    def step_five(c):
        wait(f"5{c}", r5p.at[:, double(c)])
        if not stores:
            wait("sum", zsum)
        for cols in sides(c):
            total = part[0, 0, :, cols].astype(F32) + zsum[:, cols].astype(F32) + r5p[:, cols].astype(F32) + r5m[:, cols].astype(F32)
            outv[:, cols] = total.astype(BF16)
        cols = chunk_cols(c)
        store = pltpu.make_async_copy(outv.at[:, cols], out_hbm.at[:, cols], local_sem.at[4])
        store.start()
        stores.append(c)

    def drain_all(c=0):
        drain("own", gath.at[0])
        drain("pass", gath.at[0])
        drain("second", gath.at[0, 0:3])
        drain("relay", gath.at[0])
        drain("meta", meta.at[pl.ds(0, 15)])
        for kind in ("rows", "back"):
            drain(kind, zsend.at[pl.ds(0, 11)])
        for kind in ("near", "nearback"):
            drain(kind, frecv)
        drain("whole", fgath)
        drain("mwhole", fmeta)
        drain("sum", fsum)
        drain("early", esend)
        for kind, like in (("1p", r1p), ("1m", r1m), ("4p", r4p), ("4m", r4m)):
            drain(kind, like)
        for kind in ("2p", "2m"):
            drain(kind, both.at[pl.ds(0, 7), 0, :, first])

    whole = {"O3": serve_own, "N": serve_near, "Z": serve_early, "L": serve_late, "DN": down_near, "F": sum_near, "X": drain_all}
    chunked = {
        "a": functools.partial(down_z, 0), "b": functools.partial(down_z, 1), "W": down_own, "G": expand, "E": expand_late,
        "A": step_two, "B": step_three, "C": step_four, "D": step_five,
    }
    for step in STEPS:
        if step in whole:
            whole[step]()
        else:
            chunked[step[0]](int(step[1]))
    assert (len(leaving), len(landing)) == (LEAVING, LANDING), (len(leaving), len(landing))
    drain("5p", r5p)
    drain("5m", r5m)
    pltpu.make_async_copy(outv, out_hbm, local_sem.at[4]).wait()


def shards(n_hi, tokens, expert_ids, gate_probs, w_gate, w_up, w_down):
    tok, width = tokens.shape
    hid = w_gate.shape[2]
    most = 32
    vmem = pl.BlockSpec(memory_space=pltpu.VMEM)
    hbm = pl.BlockSpec(memory_space=pl.ANY)
    routes = (expert_ids.astype(F32) * 2.0 + gate_probs).T
    return pl.pallas_call(
        functools.partial(kernel, (n_hi, tok, width, hid, most)),
        out_shape=jax.ShapeDtypeStruct((tok, width), BF16),
        in_specs=[hbm, vmem, hbm, hbm, hbm],
        out_specs=hbm,
        scratch_shapes=[
            pltpu.VMEM((4, 4, tok, width), BF16),
            pltpu.VMEM((16, 8, 128), F32),
            pltpu.VMEM((PLACES, tok, 2 * most), BF16),
            pltpu.VMEM((PLACES, most, width), BF16),
            pltpu.VMEM((PLACES, most, width), BF16),
            pltpu.VMEM((PLACES, most, width), BF16),
            pltpu.VMEM((PLACES * most, hid), BF16),
            pltpu.VMEM((PLACES * most, hid), BF16),
            pltpu.VMEM((width, hid), BF16),
            pltpu.VMEM((width, hid), BF16),
            pltpu.VMEM((hid, width), BF16),
            pltpu.VMEM((PLACES // 2, 2, most, width), BF16),
            pltpu.VMEM((PLACES // 2, 2, 2 * most, width), BF16),
            pltpu.VMEM((4, 4, tok, width), BF16),
            pltpu.VMEM((PLACES, 2 * most, tok), BF16),
            pltpu.VMEM((tok, width), BF16),
            pltpu.VMEM((8, 128), F32),
            pltpu.VMEM((5, tok, most), BF16),
            pltpu.VMEM((5 * most, tok), BF16),
            pltpu.VMEM((4, most, width), BF16),
            pltpu.VMEM((4, most, width), BF16),
            pltpu.VMEM((tok, width), BF16),
            pltpu.VMEM((tok, width), BF16),
            pltpu.VMEM((4, tok // 2, width // 2), BF16),
            pltpu.VMEM((4, tok // 2, width // 2), BF16),
            pltpu.VMEM((4, tok // 2, width), BF16),
            pltpu.VMEM((4, tok // 2, width), BF16),
            pltpu.VMEM((4, tok, width), BF16),
            pltpu.VMEM((4, tok, width), BF16),
            pltpu.VMEM((tok // 2, width), BF16),
            pltpu.VMEM((tok // 2, width), BF16),
            pltpu.VMEM((tok, width), BF16),
            pltpu.VMEM((tok, width), BF16),
            pltpu.VMEM((tok, width), BF16),
            pltpu.SemaphoreType.DMA((LEAVING,)),
            pltpu.SemaphoreType.DMA((LANDING,)),
            pltpu.SemaphoreType.DMA((5,)),
        ],
        compiler_params=pltpu.CompilerParams(
            collective_id=0, has_side_effects=True, vmem_limit_bytes=54784 * 1024
        ),
        name="routed_experts",
    )(tokens, routes, w_gate, w_up, w_down)


def solution(mesh):
    placed = (
        P(("dp", "ep"), None),
        P(("dp", "ep"), None),
        P(("dp", "ep"), None),
        P("ep", None, None),
        P("ep", None, None),
        P("ep", None, None),
    )
    return jax.shard_map(
        functools.partial(shards, mesh.shape["dp"] // 2), mesh=mesh, in_specs=placed,
        out_specs=P(("dp", "ep"), None), check_vma=False,
    )
```

```python
import functools

import jax
import jax.numpy as jnp
from jax import lax
from jax.experimental import pallas as pl
from jax.experimental.pallas import tpu as pltpu
from jax.sharding import PartitionSpec as P

MESH = pl.DeviceIdType.MESH
F32, BF16 = jnp.float32, jnp.bfloat16
OPPOSITE = {"xp": "xm", "xm": "xp", "yp": "ym", "ym": "yp", "zp": "zm", "zm": "zp"}

CLUSTER = [(0, 0), (1, 0), (3, 0), (0, 1), (0, 3)]
OTHERS = [(1, 1), (3, 3), (1, 3), (3, 1), (0, 2), (2, 0), (1, 2), (2, 1), (3, 2), (2, 3), (2, 2)]
PLACE = {slot: place for place, slot in enumerate(CLUSTER + [None] + OTHERS) if slot}
PLACES = 18
NEAR = {1: "xp", 2: "xm", 3: "yp", 4: "ym"}
PARTS = (1,) * 8
STEPS = (
    "O3", "Z", "a3", "W3", "a1", "N", "DN", "L", "W2", "G6", "W1", "b1", "b3", "a0", "G7", "W0", "G2", "G3", "E2",
    "b0", "E3", "E6", "b2", "a2", "E7", "G0", "A2", "A3", "G1", "E0", "A7", "A6", "E1", "G4", "E4", "F", "G5", "E5",
    "A1", "A0", "A4", "B7", "A5", "B2", "B1", "B6", "B0", "B3", "B4", "B5", "C7", "C1", "C0", "C2", "C6", "C4", "C3",
    "C5", "X", "D4", "D0", "D3", "D1", "D6", "D7", "D2", "D5",
)
LEAVING, LANDING = 21, 57


def kernel(
    sizes, tok_hbm, routes_ref, wg_hbm, wu_hbm, wd_hbm, out_ref,
    gath, meta, comb, xown, zsend, zrecv, hown, hz, wg, wu, wd, zout, both, part, picks,
    fgath, fmeta, fcomb, fpick, fsend, frecv, fsum, zsum, esend, erecv,
    r1p, r1m, r2p, r2m, r4p, r4m, r5p, r5m,
    send_sem, recv_sem, local_sem,
):
    n_hi, tok, width, hid, most = sizes
    half, quarter = width // 2, width // 4
    ep, dp = lax.axis_index("ep"), lax.axis_index("dp")
    x, y, z_lo = lax.rem(ep, 4), lax.rem(ep // 4, 4), ep // 16
    z_hi, core = dp // 2, lax.rem(dp, 2)

    def at(xx, yy, zz):
        return zz * 16 + yy * 4 + xx

    cross = 1 - core
    here = z_hi * 2 + cross
    z_up = lax.rem(z_hi + z_lo, n_hi) * 2 + cross
    z_down = lax.rem(z_hi + z_lo + n_hi - 1, n_hi) * 2 + cross
    target = {
        "xp": {"ep": at(lax.rem(x + 1, 4), y, z_lo), "dp": here},
        "xm": {"ep": at(lax.rem(x + 3, 4), y, z_lo), "dp": here},
        "yp": {"ep": at(x, lax.rem(y + 1, 4), z_lo), "dp": here},
        "ym": {"ep": at(x, lax.rem(y + 3, 4), z_lo), "dp": here},
        "zp": {"ep": at(x, y, 1 - z_lo), "dp": z_up},
        "zm": {"ep": at(x, y, 1 - z_lo), "dp": z_down},
    }
    other = at(x, y, 1 - z_lo)

    leaving, landing = {}, {}

    def sem(array, kinds, kind):
        return array.at[kinds.setdefault(kind, len(kinds))]

    def send(way, src, dst, leaves, lands):
        pltpu.make_async_remote_copy(
            src_ref=src, dst_ref=dst, send_sem=sem(send_sem, leaving, leaves), recv_sem=sem(recv_sem, landing, lands),
            device_id=target[way], device_id_type=MESH,
        ).start()

    def wait(lands, *like):
        pltpu.make_async_copy(*like, *like, sem(recv_sem, landing, lands)).wait()

    def drain(leaves, like):
        pltpu.make_async_copy(like, like, sem(send_sem, leaving, leaves)).wait()

    barrier = pltpu.get_barrier_semaphore()
    for way in target:
        pl.semaphore_signal(barrier, inc=1, device_id=target[way], device_id_type=MESH)

    load_tok = pltpu.make_async_copy(tok_hbm, gath.at[0, 0], local_sem.at[0])
    load_tok.start()
    loads = [
        pltpu.make_async_copy(src.at[0], dst, local_sem.at[1 + i])
        for i, (src, dst) in enumerate(((wg_hbm, wg), (wu_hbm, wu), (wd_hbm, wd)))
    ]
    for load in loads:
        load.start()

    ids = jnp.floor(routes_ref[...] * 0.5)
    probs = routes_ref[...] - 2.0 * ids
    weights = probs / jnp.sum(probs, axis=0, keepdims=True)
    experts = lax.broadcasted_iota(jnp.int32, (32, tok), 0).astype(F32)
    named = jnp.zeros((32, tok), F32)
    for k in range(8):
        named = named + jnp.where(ids[k:k + 1, :] == experts, 1.0, 0.0)
    before = lax.broadcasted_iota(jnp.int32, (tok, tok), 0) < lax.broadcasted_iota(jnp.int32, (tok, tok), 1)
    ranks = jnp.dot(named.astype(BF16), before.astype(F32).astype(BF16), preferred_element_type=F32)
    for k in range(8):
        rank = jnp.sum(jnp.where(ids[k:k + 1, :] == experts, ranks, 0.0), axis=0, keepdims=True)
        meta[0, k:k + 1, 0:tok] = ids[k:k + 1, :] * float(most) + rank
    meta[0, :, tok:2 * tok] = weights

    pl.semaphore_wait(barrier, 6)
    load_tok.wait()

    first, second = pl.ds(0, half), pl.ds(half, half)
    quarters = [pl.ds(q * quarter, quarter) for q in range(4)]

    def move(kind, leaves, way, slot, cols, with_meta=False):
        dx, dy = slot
        shift = {"xp": (3, 0), "xm": (1, 0), "yp": (0, 3), "ym": (0, 1)}[way]
        to = ((dx + shift[0]) % 4, (dy + shift[1]) % 4)
        send(way, gath.at[dx, dy, :, cols], gath.at[to[0], to[1], :, cols], leaves, kind)
        if with_meta:
            send(way, meta.at[4 * dx + dy], meta.at[4 * to[0] + to[1]], "meta", "m" + kind)

    def own_first():
        for way in ("xp", "xm"):
            move("own", "own", way, (0, 0), first, True)
        for way in ("yp", "ym"):
            move("own", "own", way, (0, 0), second, True)

    def own_second():
        for way in ("yp", "ym"):
            move("pass0", "own", way, (0, 0), first)
        for way in ("xp", "xm"):
            move("pass0", "own", way, (0, 0), second)

    def own_relay():
        move("far", "pass", "xp", (3, 0), quarters[0], True)
        move("far", "pass", "xm", (1, 0), quarters[1])
        move("far", "pass", "yp", (0, 3), quarters[2], True)
        move("far", "pass", "ym", (0, 1), quarters[3])

    def passes(d):
        e = (4 - d) % 4
        move(f"pass{d}", "pass", "ym", (d, 0), first, d > 1)
        move(f"pass{d}", "second", "xm", (0, d), second, d < 3)
        move(f"pass{d}", "pass", "yp", (e, 0), first, d > 1)
        move(f"pass{d}", "second", "xp", (0, e), second, d < 3)

    def relays(d):
        move(f"relay{d}", "relay", "yp", (d, 3), quarters[0])
        move(f"relay{d}", "relay", "ym", (d, 1), quarters[1], d == 2)
        move(f"relay{d}", "relay", "xp", (3, d), quarters[2])
        move(f"relay{d}", "relay", "xm", (1, d), quarters[3])

    def got_own():
        wait("own", gath.at[0, 0:2])
        wait("mown", meta.at[pl.ds(0, 4)])

    def got_far():
        wait("far", gath.at[0, 0])
        wait("mfar", meta.at[pl.ds(0, 2)])

    def got_passes(d):
        wait(f"pass{d}", gath.at[0, 0:2])
        if d:
            wait(f"mpass{d}", meta.at[pl.ds(0, 4 if d == 2 else 2)])

    def got_relays(d):
        wait(f"relay{d}", gath.at[0, 0])
        if d == 2:
            wait("mrelay2", meta.at[0])

    place_row = lax.broadcasted_iota(jnp.int32, (2 * most, tok), 0)
    wanted = jnp.where(place_row < most, ep * most + place_row, (other - 1) * most + place_row).astype(F32)

    def build(dx, dy):
        place = PLACE[dx, dy]
        one, scaled = jnp.zeros((2 * most, tok), F32), jnp.zeros((2 * most, tok), F32)
        routes = meta[4 * dx + dy]
        codes, shares_of = routes[:, 0:tok], routes[:, tok:2 * tok]
        for k in range(8):
            hit = codes[k:k + 1, :] == wanted
            one = one + jnp.where(hit, 1.0, 0.0)
            scaled = scaled + jnp.where(hit, shares_of[k:k + 1, :], 0.0)
        comb[place] = scaled.T.astype(BF16)
        picks[place] = one.astype(BF16)

    def ways_out(place):
        if place == 16:
            return (("zp", pl.ds(0, most // 2)), ("zm", pl.ds(most // 2, most // 2)))
        return (("zm" if place % 2 else "zp", pl.ds(0, most)),)

    def select(dx, dy):
        place = PLACE[dx, dy]
        rows = most if place < 5 else 2 * most

        @pl.loop(0, 4, unroll=4)
        def _(q):
            cols = pl.ds(pl.multiple_of(q * quarter, quarter), quarter)
            chosen = jnp.dot(picks[place, :rows], gath[dx, dy, :, cols], preferred_element_type=F32).astype(BF16)
            xown[place, :, cols] = chosen[:most]
            if place >= 5:
                zsend[place, :, cols] = chosen[most:]

        if place >= 5:
            group = min((place - 6) // 4, 2)
            for way, rows in ways_out(place):
                send(way, zsend.at[place, rows], zrecv.at[place, rows], "rows", f"rows{group}")

    def select_all(*slots):
        for slot in slots:
            build(*slot)
            select(*slot)

    def got_rows(group):
        wait(f"rows{group}", zrecv.at[pl.ds(0, (4, 4, 3)[group])])

    near_experts = (ep, at(lax.rem(x + 1, 4), y, z_lo), at(lax.rem(x + 3, 4), y, z_lo), at(x, lax.rem(y + 1, 4), z_lo), at(x, lax.rem(y + 3, 4), z_lo))

    def select_foreign():
        routes = fmeta[...]
        codes, shares_of = routes[:, 0:tok], routes[:, tok:2 * tok]
        for i, expert in enumerate(near_experts):
            row = (expert * most + lax.broadcasted_iota(jnp.int32, (most, tok), 0)).astype(F32)
            one, scaled = jnp.zeros((most, tok), F32), jnp.zeros((most, tok), F32)
            for k in range(8):
                hit = codes[k:k + 1, :] == row
                one = one + jnp.where(hit, 1.0, 0.0)
                scaled = scaled + jnp.where(hit, shares_of[k:k + 1, :], 0.0)
            fcomb[i] = scaled.T.astype(BF16)
            fpick[i * most:(i + 1) * most, :] = one.astype(BF16)

        @pl.loop(0, 4, unroll=4)
        def _(q):
            cols = pl.ds(pl.multiple_of(q * quarter, quarter), quarter)
            chosen = jnp.dot(fpick[...], fgath[:, cols], preferred_element_type=F32).astype(BF16)
            zrecv[0, :, cols] = chosen[:most]
            for i in range(4):
                fsend[i, :, cols] = chosen[(i + 1) * most:(i + 2) * most]

    def send_near():
        for i, (way, slot) in enumerate((("xp", (3, 0)), ("xm", (1, 0)), ("yp", (0, 3)), ("ym", (0, 1)))):
            send(way, fsend.at[i], zrecv.at[PLACE[slot]], "near", "near")

    def back_near():
        for place, way in NEAR.items():
            index = ("xm", "xp", "ym", "yp").index(way)
            send(way, zout.at[place // 2, place % 2], frecv.at[index], "nb", "nb")

    def sum_near():
        wait("nb", frecv)

        @pl.loop(0, 4, unroll=4)
        def _(q):
            cols = pl.ds(pl.multiple_of(q * quarter, quarter), quarter)
            total = jnp.dot(fcomb[0], zout[0, 0, :, cols], preferred_element_type=F32)
            for i in range(4):
                total = total + jnp.dot(fcomb[i + 1], frecv[i, :, cols], preferred_element_type=F32)
            fsum[:, cols] = total.astype(BF16)

        send("zp", fsum, zsum, "sum", "sum")

    tile = 256

    def gate_up(rows_ref, hidden, place, places, start=0, stop=hid // tile):
        rows = places * most

        @pl.loop(start, stop, unroll=stop - start)
        def _(n):
            cols = pl.ds(pl.multiple_of(n * tile, tile), tile)
            block = rows_ref[place:place + places].reshape(rows, width)
            gate = jnp.dot(block, wg[:, cols], preferred_element_type=F32)
            up = jnp.dot(block, wu[:, cols], preferred_element_type=F32)
            hidden[place * most:place * most + rows, cols] = (gate / (1.0 + jnp.exp(-gate)) * up).astype(BF16)

    starts = [sum(PARTS[:c]) * width // sum(PARTS) for c in range(len(PARTS) + 1)]

    def chunk_cols(c):
        return pl.ds(starts[c], starts[c + 1] - starts[c])

    def sides(c):
        middle = (starts[c] + starts[c + 1]) // 2
        return pl.ds(starts[c], middle - starts[c]), pl.ds(middle, starts[c + 1] - middle)

    top, low = pl.ds(0, tok // 2), pl.ds(tok // 2, tok // 2)

    def early_own():
        for q in range(4):
            out = jnp.dot(hown[0:5 * most, :], wd[:, quarters[q]], preferred_element_type=F32).astype(BF16)
            for slot, place in PLACE.items():
                if place < 5:
                    part[slot[0], slot[1], :, quarters[q]] = jnp.dot(
                        comb[place, :, :most], out[most * place:most * (place + 1)], preferred_element_type=F32
                    ).astype(BF16)
        for c in range(len(PARTS)):
            left, right = sides(c)
            esend[0, :, early_cols(c)] = part[0, 1, low, left]
            esend[1, :, early_cols(c)] = part[0, 3, top, left]
            esend[2, :, early_cols(c)] = part[1, 0, low, right]
            esend[3, :, early_cols(c)] = part[3, 0, top, right]

    def early_cols(c):
        return pl.ds(starts[c] // 2, (starts[c + 1] - starts[c]) // 2)

    def send_early():
        for i, way in enumerate(("yp", "ym", "xp", "xm")):
            send(way, esend.at[i], erecv.at[i], "early", "early")

    own_first()
    own_second()
    send("zm", gath.at[0, 0], fgath, "whole", "whole")
    send("zm", meta.at[0], fmeta, "mw", "mw")
    select_all((0, 0))
    got_own()
    passes(1)
    own_relay()
    passes(3)
    for slot in CLUSTER[1:]:
        build(*slot)
    got_passes(0)
    relays(0)
    for slot in CLUSTER[1:]:
        select(*slot)
    wait("whole", fgath)
    wait("mw", fmeta)
    select_foreign()
    for load in loads:
        load.wait()
    gate_up(xown, hown, 0, 5, 0, 2)
    got_passes(1)
    select_all((1, 1), (3, 3))
    got_far()
    passes(2)
    gate_up(xown, hown, 0, 5, 2, 3)
    early_own()
    got_passes(3)
    relays(1)
    relays(3)
    select_all((1, 3), (3, 1))
    got_relays(0)
    select_all((0, 2), (2, 0))
    gate_up(xown, hown, 6, 6, 0, 1)
    got_passes(2)
    relays(2)
    send_near()
    send_early()
    gate_up(xown, hown, 6, 6, 1, 3)
    got_relays(1)
    select_all((1, 2), (2, 1))
    got_relays(3)
    select_all((3, 2), (2, 3))
    got_relays(2)
    select_all((2, 2))
    got_rows(0)
    gate_up(zrecv, hz, 6, 4)

    def quarter_chunks(q):
        return [c for c in range(len(PARTS)) if q * quarter <= starts[c] < (q + 1) * quarter]

    def down_z(part_of, q):
        place, places = ((6, 8), (14, 3))[part_of]
        rows = hz[most * place:most * (place + places), :]
        out = jnp.dot(rows, wd[:, quarters[q]], preferred_element_type=F32).astype(BF16)
        for i in range(places):
            zout[(place + i) // 2, (place + i) % 2, :, quarters[q]] = out[most * i:most * (i + 1)]
        for c in quarter_chunks(q):
            cols, kind = chunk_cols(c), "uv"[part_of] + str(c)
            if part_of == 0:
                for side, way in ((0, "zm"), (1, "zp")):
                    pairs = pl.ds(place // 2, places // 2)
                    send(way, zout.at[pairs, side, :, cols], both.at[pairs, side, pl.ds(most, most), cols], "back", kind)
            else:
                for i in range(places):
                    pair, side = (place + i) // 2, (place + i) % 2
                    for way, rows in ways_out(place + i):
                        to = pl.ds(most + rows.start, rows.size)
                        send(OPPOSITE[way], zout.at[pair, side, rows, cols], both.at[pair, side, to, cols], "back", kind)

    def down_near():
        @pl.loop(0, 4, unroll=4)
        def _(q):
            cols = pl.ds(pl.multiple_of(q * quarter, quarter), quarter)
            out = jnp.dot(hz[0:5 * most, :], wd[:, cols], preferred_element_type=F32).astype(BF16)
            for i in range(5):
                zout[i // 2, i % 2, :, cols] = out[most * i:most * (i + 1)]

        back_near()

    def down_own(q):
        rows = hown[6 * most:17 * most, :]
        out = jnp.dot(rows, wd[:, quarters[q]], preferred_element_type=F32).astype(BF16)
        for place in range(6, 17):
            both[place // 2, place % 2, 0:most, quarters[q]] = out[most * (place - 6):most * (place - 5)]

    def serve_own():
        gate_up(xown, hown, 12, 5)

    def serve_near():
        wait("near", zrecv.at[pl.ds(0, 4)])
        gate_up(zrecv, hz, 0, 5)

    def serve_early():
        got_rows(1)
        gate_up(zrecv, hz, 10, 4)

    def serve_late():
        got_rows(2)
        gate_up(zrecv, hz, 14, 3)

    def fill(c, *slots):
        cols = chunk_cols(c)
        for dx, dy in slots:
            place = PLACE[dx, dy]
            part[dx, dy, :, cols] = jnp.dot(
                comb[place], both[place // 2, place % 2, :, cols], preferred_element_type=F32
            ).astype(BF16)

    late = ((3, 2), (2, 3), (2, 2))

    def halves_one(c, pair):
        left, right = sides(c)
        send("yp", part.at[pair, 2, top, left], r1p.at[pair, :, left], "1p", f"1{c}")
        send("ym", part.at[pair, 2, low, left], r1m.at[pair, :, left], "1m", f"1{c}")
        send("xp", part.at[2, pair, top, right], r1p.at[pair, :, right], "1p", f"1{c}")
        send("xm", part.at[2, pair, low, right], r1m.at[pair, :, right], "1m", f"1{c}")

    def expand(c):
        left, right = sides(c)
        wait(f"u{c}", zrecv.at[pl.ds(0, 8), :, chunk_cols(c)])
        fill(c, (0, 2), (1, 2), (2, 0), (2, 1))
        halves_one(c, pl.ds(0, 2))
        fill(c, (1, 1), (3, 3), (1, 3), (3, 1))
        send("yp", part.at[pl.ds(1, 3), 1, low, left], r2p.at[pl.ds(1, 3), low, left], "2p", f"2{c}")
        send("xp", part.at[1, pl.ds(1, 3), low, right], r2p.at[pl.ds(1, 3), low, right], "2p", f"2{c}")
        send("ym", part.at[1, 3, top, left], r2m.at[1, top, left], "2m", f"2{c}")
        send("xm", part.at[3, 1, top, right], r2m.at[1, top, right], "2m", f"2{c}")

    def expand_late(c):
        left, right = sides(c)
        wait(f"v{c}", zrecv.at[pl.ds(0, 3), :, chunk_cols(c)])
        fill(c, *late)
        halves_one(c, pl.ds(2, 2))
        send("ym", part.at[pl.ds(2, 2), 3, top, left], r2m.at[pl.ds(2, 2), top, left], "2m", f"2{c}")
        send("xm", part.at[3, pl.ds(2, 2), top, right], r2m.at[pl.ds(2, 2), top, right], "2m", f"2{c}")

    def halves_two(c, plus, minus):
        left, right = sides(c)
        send("yp", part.at[:, 1, plus, left], r2p.at[:, plus, left], "2p", f"2{c}")
        send("ym", part.at[:, 3, minus, left], r2m.at[:, minus, left], "2m", f"2{c}")
        send("xp", part.at[1, :, plus, right], r2p.at[:, plus, right], "2p", f"2{c}")
        send("xm", part.at[3, :, minus, right], r2m.at[:, minus, right], "2m", f"2{c}")

    def halves_five(c, plus, minus):
        left, right = sides(c)
        send("xp", part.at[1, 0, plus, left], r5p.at[plus, left], "5p", f"v{c}")
        send("xm", part.at[3, 0, minus, left], r5m.at[minus, left], "5m", f"v{c}")
        send("yp", part.at[0, 1, plus, right], r5p.at[plus, right], "5p", f"v{c}")
        send("ym", part.at[0, 3, minus, right], r5m.at[minus, right], "5m", f"v{c}")

    def double(c):
        return pl.ds(0, 2 * chunk_cols(c).size)

    def add(dx, dy, rows, cols, *refs):
        total = part[dx, dy, rows, cols].astype(F32)
        for ref in refs:
            total = total + ref[...].astype(F32)
        part[dx, dy, rows, cols] = total.astype(BF16)

    every = pl.ds(0, tok)

    def step_two(c):
        left, right = sides(c)
        wait(f"1{c}", r1p.at[:, :, double(c)])
        for d in range(4):
            add(d, 1, top, left, r1p.at[d, :, left])
            add(d, 3, low, left, r1m.at[d, :, left])
            add(1, d, top, right, r1p.at[d, :, right])
            add(3, d, low, right, r1m.at[d, :, right])
        halves_two(c, top, low)

    got = []

    def step_three(c):
        left, right = sides(c)
        wait(f"2{c}", both.at[pl.ds(0, 7), 0, :, chunk_cols(c)])
        if "early" not in got:
            got.append("early")
            wait("early", erecv)
        for d in (2, 1, 3, 0):
            if d == 0:
                for cols, plus, minus in ((left, 0, 1), (right, 2, 3)):
                    add(0, 0, top, cols, r2p.at[0, top, cols], erecv.at[minus, :, early_cols(c)])
                    add(0, 0, low, cols, erecv.at[plus, :, early_cols(c)], r2m.at[0, low, cols])
                continue
            add(d, 0, every, left, r2p.at[d, :, left], r2m.at[d, :, left])
            add(0, d, every, right, r2p.at[d, :, right], r2m.at[d, :, right])
            if d == 2:
                send("xp", part.at[2, 0, top, left], r4p.at[:, left], "4p", f"u{c}")
                send("xm", part.at[2, 0, low, left], r4m.at[:, left], "4m", f"u{c}")
                send("yp", part.at[0, 2, top, right], r4p.at[:, right], "4p", f"u{c}")
                send("ym", part.at[0, 2, low, right], r4m.at[:, right], "4m", f"u{c}")
            if d == 3:
                halves_five(c, low, top)

    def step_four(c):
        left, right = sides(c)
        wait(f"u{c}", r4p.at[:, double(c)])
        add(1, 0, top, left, r4p.at[:, left])
        add(3, 0, low, left, r4m.at[:, left])
        add(0, 1, top, right, r4p.at[:, right])
        add(0, 3, low, right, r4m.at[:, right])
        halves_five(c, top, low)

    stores = []


    def step_five(c):
        wait(f"v{c}", r5p.at[:, double(c)])
        if not stores:
            wait("sum", zsum)
        for cols in sides(c):
            total = part[0, 0, :, cols].astype(F32) + zsum[:, cols].astype(F32) + r5p[:, cols].astype(F32) + r5m[:, cols].astype(F32)
            out_ref[:, cols] = total.astype(BF16)
        stores.append(c)

    def drain_all(c=0):
        drain("own", gath.at[0])
        drain("pass", gath.at[0])
        drain("second", gath.at[0, 0:3])
        drain("relay", gath.at[0])
        drain("meta", meta.at[pl.ds(0, 15)])
        for kind in ("rows", "back"):
            drain(kind, zsend.at[pl.ds(0, 11)])
        for kind in ("near", "nb"):
            drain(kind, frecv)
        drain("whole", fgath)
        drain("mw", fmeta)
        drain("sum", fsum)
        drain("early", esend)
        for kind, like in (("1p", r1p), ("1m", r1m), ("4p", r4p), ("4m", r4m)):
            drain(kind, like)
        for kind in ("2p", "2m"):
            drain(kind, both.at[pl.ds(0, 7), 0, :, first])

    whole = {"O3": serve_own, "N": serve_near, "Z": serve_early, "L": serve_late, "DN": down_near, "F": sum_near, "X": drain_all}
    chunked = {
        "a": functools.partial(down_z, 0), "b": functools.partial(down_z, 1), "W": down_own, "G": expand, "E": expand_late,
        "A": step_two, "B": step_three, "C": step_four, "D": step_five,
    }
    for step in STEPS:
        if step in whole:
            whole[step]()
        else:
            chunked[step[0]](int(step[1]))
    assert (len(leaving), len(landing)) == (LEAVING, LANDING), (len(leaving), len(landing))
    drain("5p", r5p)
    drain("5m", r5m)


def shards(n_hi, tokens, expert_ids, gate_probs, w_gate, w_up, w_down):
    tok, width = tokens.shape
    hid = w_gate.shape[2]
    most = 32
    vmem = pl.BlockSpec(memory_space=pltpu.VMEM)
    hbm = pl.BlockSpec(memory_space=pl.ANY)
    routes = (expert_ids.astype(F32) * 2.0 + gate_probs).T
    return pl.pallas_call(
        functools.partial(kernel, (n_hi, tok, width, hid, most)),
        out_shape=jax.ShapeDtypeStruct((tok, width), BF16),
        in_specs=[hbm, vmem, hbm, hbm, hbm],
        out_specs=vmem,
        scratch_shapes=[
            pltpu.VMEM((4, 4, tok, width), BF16),
            pltpu.VMEM((16, 8, 128), F32),
            pltpu.VMEM((PLACES, tok, 2 * most), BF16),
            pltpu.VMEM((PLACES, most, width), BF16),
            pltpu.VMEM((PLACES, most, width), BF16),
            pltpu.VMEM((PLACES, most, width), BF16),
            pltpu.VMEM((PLACES * most, hid), BF16),
            pltpu.VMEM((PLACES * most, hid), BF16),
            pltpu.VMEM((width, hid), BF16),
            pltpu.VMEM((width, hid), BF16),
            pltpu.VMEM((hid, width), BF16),
            pltpu.VMEM((PLACES // 2, 2, most, width), BF16),
            pltpu.VMEM((PLACES // 2, 2, 2 * most, width), BF16),
            pltpu.VMEM((4, 4, tok, width), BF16),
            pltpu.VMEM((PLACES, 2 * most, tok), BF16),
            pltpu.VMEM((tok, width), BF16),
            pltpu.VMEM((8, 128), F32),
            pltpu.VMEM((5, tok, most), BF16),
            pltpu.VMEM((5 * most, tok), BF16),
            pltpu.VMEM((4, most, width), BF16),
            pltpu.VMEM((4, most, width), BF16),
            pltpu.VMEM((tok, width), BF16),
            pltpu.VMEM((tok, width), BF16),
            pltpu.VMEM((4, tok // 2, width // 2), BF16),
            pltpu.VMEM((4, tok // 2, width // 2), BF16),
            pltpu.VMEM((4, tok // 2, width), BF16),
            pltpu.VMEM((4, tok // 2, width), BF16),
            pltpu.VMEM((4, tok, width), BF16),
            pltpu.VMEM((4, tok, width), BF16),
            pltpu.VMEM((tok // 2, width), BF16),
            pltpu.VMEM((tok // 2, width), BF16),
            pltpu.VMEM((tok, width), BF16),
            pltpu.VMEM((tok, width), BF16),
            pltpu.SemaphoreType.DMA((LEAVING,)),
            pltpu.SemaphoreType.DMA((LANDING,)),
            pltpu.SemaphoreType.DMA((4,)),
        ],
        compiler_params=pltpu.CompilerParams(
            collective_id=0, has_side_effects=True, vmem_limit_bytes=54784 * 1024
        ),
        name="routed_experts",
    )(tokens, routes, w_gate, w_up, w_down)


def solution(mesh):
    placed = (
        P(("dp", "ep"), None),
        P(("dp", "ep"), None),
        P(("dp", "ep"), None),
        P("ep", None, None),
        P("ep", None, None),
        P("ep", None, None),
    )
    return jax.shard_map(
        functools.partial(shards, mesh.shape["dp"] // 2), mesh=mesh, in_specs=placed,
        out_specs=P(("dp", "ep"), None), check_vma=False,
    )
```
